128 devices in a mesh: freq: 8 (over z_lo, y), band: 16 (over x, z_hi, core).
Axes of the slice: x: 4, y: 4, z: 4 (z_hi: 2, z_lo: 2; z = z_hi * 2 + z_lo), core: 2. Of those that a mesh axis runs over, the one named last changes fastest.
Arguments:
- pair_density: bfloat16 [4096, 2, 8192], P(('freq', 'band')), may hold values from -6 to 6
- trial_vectors: bfloat16 [32, 2, 64, 8192], P('freq', None, None, 'band'), may hold values from -6 to 6
- frequency: float32 [32], P('freq'), may hold values from 0.05 to 20
- val_energy: float32 [32], replicated, may hold values from -3 to -0.1
- cond_energy: float32 [128], replicated, may hold values from 0.1 to 4
- pair_index: int32 [4096], P(('freq', 'band')), may hold values from 0 to 4095, each once
Outputs:
- images: float32 [32, 2, 64, 8192], P('freq', None, None, 'band')
- subspace: float32 [32, 2, 64, 64], P('freq')
The draws below stay inside these ranges and needn't reach their ends.
Inputs may be any that keep to these rules, and one draw needn't show every extreme that they name: `pair_index`: every pair number 0 to 4095 appears exactly once.
All inputs are finite; a program needn't handle non-finite values.
Results may differ from the reference program's by a relative error of at most 0.0085.
Values may be sent and summed in bfloat16 or wider, within the bound.
A program may use at most 128 MiB of HBM per device.

```python
import math
import jax
import jax.numpy as jnp
from jax import lax

NG = 8192
NV = 32
K = 64
NFREQ = 32
PAIRS = 4096
NC = 128


def block_scale(own_key, dims, shards, smallest, top_value):
    gain = 1.0
    for position, shards_of in shards:
        draws = jax.random.uniform(jax.random.fold_in(jax.random.fold_in(own_key, 6), position), (shards_of,), jnp.float32, smallest / len(shards), top_value / len(shards))
        gain = gain * jnp.repeat(jnp.exp(draws), dims[position] // shards_of).reshape((-1,) + (1,) * (len(dims) - 1 - position))
    return gain


def bell_draw(rng, extent, spread, most, shards=(), kind=jnp.bfloat16):
    loudness = block_scale(rng, extent, shards, -0.22, 0.18) if shards else 1.0
    array = jax.random.normal(rng, extent, jnp.float32) * spread * loudness
    return jnp.minimum(jnp.maximum(array, -most), most).astype(kind)


def setup_inputs(seed: int = 0) -> dict:
    keys = jax.random.split(jax.random.key(seed), 7)
    pair_density = bell_draw(keys[0], (PAIRS, 2, NG), 1.0, 6.0, ((0, 128),))
    trial_vectors = bell_draw(keys[1], (NFREQ, 2, K, NG), 1.0, 6.0, ((0, 8), (3, 16)))
    frequency = jnp.clip(jnp.exp(math.log(20.0) - 5.9914645 * jax.random.uniform(keys[2], (NFREQ,), jnp.float32) ** block_scale(keys[2], (NFREQ,), ((0, 8),), -0.2, 0.2)), 0.05, 20.0)
    val_energy = jnp.clip(jax.random.uniform(keys[3], (NV,), jnp.float32, -3.0, -0.1), -3.0, -0.1)
    cond_energy = jnp.clip(jax.random.uniform(keys[4], (NC,), jnp.float32, 0.1, 4.0), 0.1, 4.0)
    pair_index = jax.random.permutation(keys[5], PAIRS).astype(jnp.int32)
    return dict(pair_density=pair_density, trial_vectors=trial_vectors, frequency=frequency, val_energy=val_energy, cond_energy=cond_energy, pair_index=pair_index)


def pair_weights(pair_index, frequency, val_energy, cond_energy):
    delta = cond_energy[pair_index % NC] - val_energy[pair_index // NC]
    prefactor = 1.0 / math.sqrt(2.0 * NG * PAIRS)
    ratio = delta[None, :] / (delta[None, :] * delta[None, :] + frequency[:, None] * frequency[:, None])
    return (-4.0 * prefactor * ratio).astype(jnp.bfloat16)

def reference(pair_density, trial_vectors, frequency, val_energy, cond_energy, pair_index):
    density = pair_density.astype(jnp.float32)
    vectors = trial_vectors.astype(jnp.float32)
    weight = pair_weights(pair_index, frequency, val_energy, cond_energy).astype(jnp.float32)
    products = jnp.einsum('pcg,fekg->fcekp', density, vectors)
    over_real = products[:, 0, 0] + products[:, 1, 1]
    over_imag = products[:, 0, 1] - products[:, 1, 0]
    scaled_real = (weight[:, None, :] * over_real).astype(jnp.bfloat16)
    scaled_imag = (weight[:, None, :] * over_imag).astype(jnp.bfloat16)
    mixed = jnp.stack([jnp.stack([scaled_real, -scaled_imag], 1), jnp.stack([scaled_imag, scaled_real], 1)], 1)
    images = jnp.einsum('pcg,fdckp->fdkg', density, mixed.astype(jnp.float32))
    hp = lax.Precision.HIGHEST
    real_part = jnp.einsum('fkg,flg->fkl', vectors[:, 0], images[:, 0], precision=hp) + jnp.einsum('fkg,flg->fkl', vectors[:, 1], images[:, 1], precision=hp)
    imag_part = jnp.einsum('fkg,flg->fkl', vectors[:, 0], images[:, 1], precision=hp) - jnp.einsum('fkg,flg->fkl', vectors[:, 1], images[:, 0], precision=hp)
    subspace = jnp.stack([real_part, imag_part], 1) / NG
    return (images, subspace)
```

```python
import functools
import math

import jax
import jax.numpy as jnp
from jax import lax
from jax.experimental import pallas as pl
from jax.experimental.pallas import tpu as pltpu
from jax.sharding import PartitionSpec as P

MESH = pl.DeviceIdType.MESH
ORDER = (0, 1, 3, 2)


def wrap(v, n=4):
    return lax.rem(v + n, n)


def dev(x, y, z, c):
    x, y, z, c = wrap(x), wrap(y), wrap(z), wrap(c, 2)
    return (lax.rem(z, 2) * 4 + y, x * 4 + (z // 2) * 2 + c)


def dot_nt(a, b):
    return lax.dot_general(a, b, (((1,), (1,)), ((), ())), preferred_element_type=jnp.float32)


def kernel(
    consts,
    rho, xin, idx, cond, val, freq,
    img, sub,
    R, XF, acc, C32, CB, CR, SF, L, SB, RI, D, SZ, SO, SA, FQ,
    x_s, x_r, y_s, y_r, f_s, f_r, p_s, p_r, v_s, v_r, c_s, c_r, g_s, g_r,
    i_s, i_r, d_s, d_r, u_s, u_r, w_s, w_r, q_s, q_r,
):
    prefactor, grid_count = consts
    fi, bi = lax.axis_index("freq"), lax.axis_index("band")
    zl, y = fi // 4, lax.rem(fi, 4)
    x, zh, c = bi // 4, lax.rem(bi // 2, 2), lax.rem(bi, 2)
    z = zh * 2 + zl
    me = (fi, bi)
    partner = dev(x, y, z, 1 - c)
    aligned = zl == c
    pending = []

    def send(src, dst, ss, rs, to):
        copy = pltpu.make_async_remote_copy(
            src_ref=src, dst_ref=dst, send_sem=ss, recv_sem=rs, device_id=to, device_id_type=MESH
        )
        copy.start()
        return copy

    def keep(copy):
        pending.append(copy)

    def arrived(dst, rs):
        pltpu.make_async_remote_copy(
            src_ref=dst, dst_ref=dst, send_sem=rs, recv_sem=rs, device_id=me, device_id_type=MESH
        ).wait_recv()

    def sent(src, ss):
        pltpu.make_async_remote_copy(
            src_ref=src, dst_ref=src, send_sem=ss, recv_sem=ss, device_id=me, device_id_type=MESH
        ).wait_send()

    plane = [
        (dy, dx, cc) for dy in range(4) for dx in range(4) for cc in range(2) if (dy, dx, cc) != (0, 0, 0)
    ]
    barrier = pltpu.get_barrier_semaphore()
    for dy, dx, cc in plane:
        pl.semaphore_signal(barrier, inc=1, device_id=dev(x + dx, y + dy, z, c + cc), device_id_type=MESH)
    for dz in (1, 2, 3):
        for cc in range(2):
            pl.semaphore_signal(barrier, inc=1, device_id=dev(x, y, z + dz, cc), device_id_type=MESH)

    lane = lax.broadcasted_iota(jnp.int32, (8, 128), 1)
    lane32 = jnp.bitwise_and(lane, 31)
    number = jnp.zeros((8, 128), jnp.int32)
    for i in range(32):
        number = jnp.where(lane32 == i, idx[i], number)
    cond_no = jnp.bitwise_and(number, 127)
    val_no = jnp.right_shift(number, 7)
    zero = jnp.zeros((8, 128), jnp.float32)
    cond_pick = lax.fori_loop(0, 128, lambda j, a: jnp.where(cond_no == j, cond[j], a), zero)
    val_pick = lax.fori_loop(0, 32, lambda j, a: jnp.where(val_no == j, val[j], a), zero)
    mine = jnp.right_shift(lane, 5) == lax.rem(x, 2) * 2 + c
    D[x * 2 + c] = jnp.where(mine, cond_pick - val_pick, 0.0)
    R[0, :, x, c] = rho[x]

    def lanes(block):
        return pl.ds(pl.multiple_of(block * 512, 512), 512)

    for f in range(4):
        FQ[0, f] = jnp.full((8, 128), freq[f], jnp.float32)

    @pl.when(aligned)
    def _():
        XF[:, :, :, lanes(zh * 2 + c)] = xin[...]
        FQ[1] = FQ[0]

    pl.semaphore_wait(barrier, len(plane) + 6)

    def at(e):
        return wrap(x - e)

    def spread(e):
        src = rho.at[x] if e == 0 else R.at[0, :, at(e), c]
        keep(send(src, R.at[1, :, at(e), c], y_s.at[0, e], y_r.at[0, e], dev(x, y + 1, z, c)))
        keep(send(src, R.at[3, :, at(e), c], y_s.at[1, e], y_r.at[1, e], dev(x, y - 1, z, c)))
        keep(send(src, R.at[0, :, at(e), c], p_s.at[0, e], p_r.at[0, e], partner))

    def pass_on(e):
        arrived(R.at[1, :, at(e), c], y_r.at[0, e])
        keep(send(R.at[1, 0, at(e), c], R.at[2, 0, at(e), c], f_s.at[0, e], f_r.at[0, e], dev(x, y + 1, z, c)))
        keep(send(R.at[1, :, at(e), c], R.at[1, :, at(e), c], p_s.at[1, e], p_r.at[1, e], partner))
        arrived(R.at[3, :, at(e), c], y_r.at[1, e])
        keep(send(R.at[3, 1, at(e), c], R.at[2, 1, at(e), c], f_s.at[1, e], f_r.at[1, e], dev(x, y - 1, z, c)))
        keep(send(R.at[3, :, at(e), c], R.at[3, :, at(e), c], p_s.at[3, e], p_r.at[3, e], partner))

    def pass_far(e):
        arrived(R.at[2, 0, at(e), c], f_r.at[0, e])
        arrived(R.at[2, 1, at(e), c], f_r.at[1, e])
        keep(send(R.at[2, :, at(e), c], R.at[2, :, at(e), c], p_s.at[2, e], p_r.at[2, e], partner))

    def partner_done(dy):
        for e in ORDER:
            arrived(R.at[dy, :, at(e), 1 - c], p_r.at[dy, e])

    for e in (1, 3, 2):
        keep(send(rho.at[wrap(x + e)], R.at[0, :, x, c], x_s.at[e], x_r.at[e], dev(x + e, y, z, c)))
    spread(0)
    my_lanes = lanes(zh * 2 + c)
    for dz in (1, 3, 2):
        keep(send(xin, XF.at[:, :, :, my_lanes], v_s.at[dz], v_r.at[dz, c], dev(x, y, z + dz, zl)))

    @pl.when(jnp.logical_not(aligned))
    def _():
        send(xin, XF.at[:, :, :, my_lanes], v_s.at[0], v_r.at[0, c], partner)

    @pl.when(aligned)
    def _():
        send(FQ.at[0], FQ.at[1], q_s, q_r, dev(x, y, z - 1, c))

    for dy, dx, cc in plane:
        send(D.at[x * 2 + c], D.at[dy * 8 + x * 2 + c], d_s, d_r, dev(x + dx, y + dy, z, c + cc))

    def vectors_done():
        @pl.when(aligned)
        def _():
            arrived(XF.at[:, :, :, lanes(zh * 2 + 1 - c)], v_r.at[0, 1 - c])
            for cc in range(2):
                arrived(XF.at[:, :, :, lanes((1 - zh) * 2 + cc)], v_r.at[2, cc])

        @pl.when(jnp.logical_not(aligned))
        def _():
            for dz in (1, 3):
                for cc in range(2):
                    arrived(XF.at[:, :, :, lanes((wrap(z - dz) // 2) * 2 + cc)], v_r.at[dz, cc])

    def cross(dy):
        v = XF[...].reshape(512, 2048)
        t_re = dot_nt(v, R[dy, 0].reshape(256, 2048)).reshape(4, 2, 64, 256)
        t_im = dot_nt(v, R[dy, 1].reshape(256, 2048)).reshape(4, 2, 64, 256)
        re = t_re[:, 0] + t_im[:, 1]
        im = t_re[:, 1] - t_im[:, 0]
        C32[dy, :, 0] = re
        C32[dy, :, 1] = im
        CB[dy, :, 0] = re.astype(jnp.bfloat16)
        CB[dy, :, 1] = im.astype(jnp.bfloat16)
        for e in (1, 3, 2):
            keep(send(CB.at[dy, wrap(x + e)], CR.at[dy, e], c_s.at[dy, e], c_r.at[dy, e], dev(x + e, y, z, c)))

    def scale(dy):
        total = C32[dy, x]
        for e in (1, 2, 3):
            arrived(CR.at[dy, e], c_r.at[dy, e])
        for e in (1, 2, 3):
            total = total + CR[dy, e].astype(jnp.float32)
        halves = []
        for h in range(2):
            first = dy * 8 + h * 4
            halves.append(D[first] + D[first + 1] + D[first + 2] + D[first + 3])
        delta = jnp.concatenate(halves, axis=1)[0:1]
        own = FQ[1, x][0:1, 0:1]
        ratio = delta / (delta * delta + own * own)
        weight = (-4.0 * prefactor * ratio).astype(jnp.bfloat16).astype(jnp.float32)
        scaled = (weight[None] * total).astype(jnp.bfloat16)
        SF[dy, x] = scaled
        for e in (1, 3, 2):
            keep(send(SF.at[dy, x], SF.at[dy, x], g_s.at[dy, e], g_r.at[dy, e], dev(x + e, y, z, c)))
        flat = total.reshape(128, 256)
        high = flat.astype(jnp.bfloat16)
        low = (flat - high.astype(jnp.float32)).astype(jnp.bfloat16)
        part = dot_nt(jnp.concatenate([high, low], axis=0), scaled.reshape(128, 256))
        if dy == 0:
            SA[...] = part
        else:
            SA[...] += part

    def gathered(dy):
        for e in (1, 3, 2):
            arrived(SF.at[dy, at(e)], g_r.at[dy, e])
        re, im = SF[dy, :, 0], SF[dy, :, 1]
        L[:, 0, :, 0:256] = re
        L[:, 0, :, 256:512] = -im
        L[:, 1, :, 0:256] = im
        L[:, 1, :, 256:512] = re

    def image_tile(dy, block):
        at_lanes = lanes(block)
        return jnp.dot(
            L[...].reshape(512, 512),
            R[dy, :, :, :, :, at_lanes].reshape(512, 512),
            preferred_element_type=jnp.float32,
        )

    def image(dy):
        gathered(dy)

        @pl.loop(0, 4)
        def _(block):
            part = image_tile(dy, block)
            if dy == 0:
                acc[:, lanes(block)] = part
            else:
                acc[:, lanes(block)] += part

    for e in (1, 3):
        arrived(R.at[0, :, at(e), c], x_r.at[e])
        spread(e)
    pass_on(0)
    arrived(R.at[0, :, at(2), c], x_r.at[2])
    spread(2)
    pass_on(1)
    pass_on(3)
    vectors_done()
    partner_done(0)
    cross(0)
    pass_on(2)
    partner_done(1)
    cross(1)
    partner_done(3)
    cross(3)
    most = D.at[pl.ds(0, 31)]
    arrived(most, d_r)
    sent(most, d_s)

    @pl.when(aligned)
    def _():
        sent(FQ.at[0], q_s)

    @pl.when(jnp.logical_not(aligned))
    def _():
        arrived(FQ.at[1], q_r)

    scale(0)
    scale(1)
    scale(3)
    pass_far(0)
    image(0)
    pass_far(1)
    image(1)
    pass_far(3)
    image(3)
    pass_far(2)
    partner_done(2)
    cross(2)
    scale(2)

    both = SA[0:128] + SA[128:256]
    re = both[0:64, 0:64] + both[64:128, 64:128]
    im = both[0:64, 64:128] - both[64:128, 0:64]
    mine_sub = jnp.concatenate([re, im], axis=1) / grid_count

    gathered(2)
    for step in range(4):
        h = 1 - zh if step < 2 else zh
        cc = 1 - c if step % 2 == 0 else c
        block = h * 2 + cc
        total = acc[:, lanes(block)] + image_tile(2, block)
        to_z = h * 2 + c
        dz = wrap(to_z - z)
        half = total.astype(jnp.bfloat16).reshape(4, 2, 64, 512)
        if step < 3:
            SB[step] = half
            keep(send(SB.at[step], RI.at[dz], i_s.at[step], i_r.at[dz], dev(x, y, to_z, cc)))
        else:
            SB[step] = half

            @pl.when(jnp.logical_not(aligned))
            def _():
                send(SB.at[3], RI.at[dz], i_s.at[3], i_r.at[dz], dev(x, y, to_z, cc))

            @pl.when(aligned)
            def _():
                RI[0] = half

    return_sub(
        mine_sub, sub, SZ, SO, x, y, z, zh, c, aligned, send, keep, arrived, sent, u_s, u_r, w_s, w_r, at
    )

    for dz in (1, 3, 2):
        arrived(RI.at[dz], i_r.at[dz])

    @pl.when(jnp.logical_not(aligned))
    def _():
        arrived(RI.at[0], i_r.at[0])

    @pl.loop(0, 4)
    def _(f):
        total = RI[0, f].astype(jnp.float32)
        for dz in (1, 2, 3):
            total = total + RI[dz, f].astype(jnp.float32)
        img[f] = total

    for copy in pending:
        copy.wait_send()

    @pl.when(jnp.logical_not(aligned))
    def _():
        sent(xin, v_s.at[0])
        sent(SB.at[3], i_s.at[3])


def return_sub(mine_sub, sub, SZ, SO, x, y, z, zh, c, aligned, send, keep, arrived, sent, u_s, u_r, w_s, w_r, at):
    SZ[0] = mine_sub

    @pl.when(aligned)
    def _():
        SZ[1 + z] = mine_sub
        send(SZ.at[0], SZ.at[1 + z], u_s.at[0], u_r.at[2], dev(x, y, z + 2, c))
        for dz in (1, 3, 2):
            arrived(SZ.at[1 + wrap(z - dz)], u_r.at[dz])
        SO[x] = SZ[1] + SZ[2] + SZ[3] + SZ[4]
        for e in (1, 3, 2):
            for cc in range(2):
                send(SO.at[x], SO.at[x], w_s.at[e, cc], w_r.at[e], dev(x + e, y, z, cc))
        send(SO.at[x], SO.at[x], w_s.at[0, 0], w_r.at[0], dev(x, y, z, 1 - c))
        sent(SZ.at[0], u_s.at[0])
        for e in (1, 3, 2):
            for cc in range(2):
                sent(SO.at[x], w_s.at[e, cc])
        sent(SO.at[x], w_s.at[0, 0])

    @pl.when(jnp.logical_not(aligned))
    def _():
        for k, dz in enumerate((1, 3)):
            send(SZ.at[0], SZ.at[1 + z], u_s.at[k], u_r.at[dz], dev(x, y, z + dz, c))
        for k in range(2):
            sent(SZ.at[0], u_s.at[k])
        arrived(SO.at[x], w_r.at[0])

    for e in (1, 3, 2):
        arrived(SO.at[at(e)], w_r.at[e])
    for f in range(4):
        both = SO[f]
        sub[f, 0] = both[:, 0:64]
        sub[f, 1] = both[:, 64:128]


def shards(pair_density, trial_vectors, frequency, val_energy, cond_energy, pair_index):
    groups = lax.axis_size("freq")
    members = lax.axis_size("band")
    pair_count = pair_density.shape[0] * groups * members
    grid_count = trial_vectors.shape[3] * members
    prefactor = 1.0 / math.sqrt(2.0 * grid_count * pair_count)
    pieces = jnp.transpose(pair_density.reshape(32, 2, 4, 2048), (2, 1, 0, 3))
    bf, f32 = jnp.bfloat16, jnp.float32
    vmem = pl.BlockSpec(memory_space=pltpu.VMEM)
    smem = pl.BlockSpec(memory_space=pltpu.SMEM)
    dma = pltpu.SemaphoreType.DMA
    return pl.pallas_call(
        functools.partial(kernel, (prefactor, grid_count)),
        name="response",
        out_shape=(
            jax.ShapeDtypeStruct((4, 2, 64, 512), f32),
            jax.ShapeDtypeStruct((4, 2, 64, 64), f32),
        ),
        in_specs=[vmem, vmem, smem, smem, smem, smem],
        out_specs=(vmem, vmem),
        scratch_shapes=[
            pltpu.VMEM((4, 2, 4, 2, 32, 2048), bf),
            pltpu.VMEM((4, 2, 64, 2048), bf),
            pltpu.VMEM((512, 2048), f32),
            pltpu.VMEM((4, 4, 2, 64, 256), f32),
            pltpu.VMEM((4, 4, 2, 64, 256), bf),
            pltpu.VMEM((4, 4, 2, 64, 256), bf),
            pltpu.VMEM((4, 4, 2, 64, 256), bf),
            pltpu.VMEM((4, 2, 64, 512), bf),
            pltpu.VMEM((4, 4, 2, 64, 512), bf),
            pltpu.VMEM((4, 4, 2, 64, 512), bf),
            pltpu.VMEM((32, 8, 128), f32),
            pltpu.VMEM((5, 64, 128), f32),
            pltpu.VMEM((4, 64, 128), f32),
            pltpu.VMEM((256, 128), f32),
            pltpu.VMEM((2, 4, 8, 128), f32),
            dma((4,)), dma((4,)),
            dma((2, 4)), dma((2, 4)),
            dma((2, 4)), dma((2, 4)),
            dma((4, 4)), dma((4, 4)),
            dma((4,)), dma((4, 2)),
            dma((4, 4)), dma((4, 4)),
            dma((4, 4)), dma((4, 4)),
            dma((4,)), dma((4,)),
            dma, dma,
            dma((2,)), dma((4,)),
            dma((4, 2)), dma((4,)),
            dma, dma,
        ],
        compiler_params=pltpu.CompilerParams(
            collective_id=0, has_side_effects=True, vmem_limit_bytes=56 * 2**20
        ),
    )(pieces, trial_vectors, pair_index, cond_energy, val_energy, frequency)


def solution(mesh):
    return jax.shard_map(
        shards,
        mesh=mesh,
        in_specs=(
            P(("freq", "band"), None, None),
            P("freq", None, None, "band"),
            P("freq"),
            P(),
            P(),
            P(("freq", "band")),
        ),
        out_specs=(P("freq", None, None, "band"), P("freq", None, None, None)),
        check_vma=False,
    )
```

```python
import functools
import math

import jax
import jax.numpy as jnp
from jax import lax
from jax.experimental import pallas as pl
from jax.experimental.pallas import tpu as pltpu
from jax.sharding import PartitionSpec as P

MESH = pl.DeviceIdType.MESH
ORDER = (0, 1, 3, 2)


def wrap(v, n=4):
    return lax.rem(v + n, n)


def dev(x, y, z, c):
    x, y, z, c = wrap(x), wrap(y), wrap(z), wrap(c, 2)
    return (lax.rem(z, 2) * 4 + y, x * 4 + (z // 2) * 2 + c)


def dot_nt(a, b):
    return lax.dot_general(a, b, (((1,), (1,)), ((), ())), preferred_element_type=jnp.float32)


def kernel(
    consts,
    rho, xin, idx, cond, val, freq,
    img, sub,
    R, XF, acc, C32, CB, CR, SF, L, SB, RI, RC, D, SZ, SO, SA, FQ,
    x_s, x_r, y_s, y_r, f_s, f_r, p_s, p_r, v_s, v_r, c_s, c_r, g_s, g_r,
    i_s, i_r, k_r, d_s, d_r, u_s, u_r, w_s, w_r, q_s, q_r,
):
    prefactor, grid_count = consts
    fi, bi = lax.axis_index("freq"), lax.axis_index("band")
    zl, y = fi // 4, lax.rem(fi, 4)
    x, zh, c = bi // 4, lax.rem(bi // 2, 2), lax.rem(bi, 2)
    z = zh * 2 + zl
    me = (fi, bi)
    partner = dev(x, y, z, 1 - c)
    aligned = zl == c
    unaligned = jnp.logical_not(aligned)
    pending = []

    def send(src, dst, ss, rs, to):
        copy = pltpu.make_async_remote_copy(
            src_ref=src, dst_ref=dst, send_sem=ss, recv_sem=rs, device_id=to, device_id_type=MESH
        )
        copy.start()
        return copy

    def keep(copy):
        pending.append(copy)

    def arrived(dst, rs):
        pltpu.make_async_remote_copy(
            src_ref=dst, dst_ref=dst, send_sem=rs, recv_sem=rs, device_id=me, device_id_type=MESH
        ).wait_recv()

    def sent(src, ss):
        pltpu.make_async_remote_copy(
            src_ref=src, dst_ref=src, send_sem=ss, recv_sem=ss, device_id=me, device_id_type=MESH
        ).wait_send()

    plane = [
        (dy, dx, cc) for dy in range(4) for dx in range(4) for cc in range(2) if (dy, dx, cc) != (0, 0, 0)
    ]
    barrier = pltpu.get_barrier_semaphore()
    for dy, dx, cc in plane:
        pl.semaphore_signal(barrier, inc=1, device_id=dev(x + dx, y + dy, z, c + cc), device_id_type=MESH)
    for dz in (1, 2, 3):
        for cc in range(2):
            pl.semaphore_signal(barrier, inc=1, device_id=dev(x, y, z + dz, cc), device_id_type=MESH)

    lane = lax.broadcasted_iota(jnp.int32, (8, 128), 1)
    lane32 = jnp.bitwise_and(lane, 31)
    number = jnp.zeros((8, 128), jnp.int32)
    for i in range(32):
        number = jnp.where(lane32 == i, idx[i], number)
    cond_no = jnp.bitwise_and(number, 127)
    val_no = jnp.right_shift(number, 7)
    zero = jnp.zeros((8, 128), jnp.float32)
    cond_pick = lax.fori_loop(0, 128, lambda j, a: jnp.where(cond_no == j, cond[j], a), zero)
    val_pick = lax.fori_loop(0, 32, lambda j, a: jnp.where(val_no == j, val[j], a), zero)
    mine = jnp.right_shift(lane, 5) == lax.rem(x, 2) * 2 + c
    D[x * 2 + c] = jnp.where(mine, cond_pick - val_pick, 0.0)
    R[0, :, x, c] = rho[x]

    def lanes(block):
        return pl.ds(pl.multiple_of(block * 512, 512), 512)

    for f in range(4):
        FQ[0, f] = jnp.full((8, 128), freq[f], jnp.float32)

    @pl.when(aligned)
    def _():
        XF[:, :, :, lanes(zh * 2 + c)] = xin[...]
        FQ[1] = FQ[0]

    with jax.named_scope("entry"):
        pl.semaphore_wait(barrier, len(plane) + 6)

    def at(e):
        return wrap(x - e)

    def spread(e):
        src = rho.at[x] if e == 0 else R.at[0, :, at(e), c]
        keep(send(src, R.at[1, :, at(e), c], y_s.at[0, e], y_r.at[0, e], dev(x, y + 1, z, c)))
        keep(send(src, R.at[3, :, at(e), c], y_s.at[1, e], y_r.at[1, e], dev(x, y - 1, z, c)))
        keep(send(src, R.at[0, :, at(e), c], p_s.at[0, e], p_r.at[0, e], partner))

    def pass_on(e):
        arrived(R.at[1, :, at(e), c], y_r.at[0, e])
        keep(send(R.at[1, 0, at(e), c], R.at[2, 0, at(e), c], f_s.at[0, e], f_r.at[0, e], dev(x, y + 1, z, c)))
        keep(send(R.at[1, :, at(e), c], R.at[1, :, at(e), c], p_s.at[1, e], p_r.at[1, e], partner))
        arrived(R.at[3, :, at(e), c], y_r.at[1, e])
        keep(send(R.at[3, 1, at(e), c], R.at[2, 1, at(e), c], f_s.at[1, e], f_r.at[1, e], dev(x, y - 1, z, c)))
        keep(send(R.at[3, :, at(e), c], R.at[3, :, at(e), c], p_s.at[3, e], p_r.at[3, e], partner))

    def pass_far(e):
        arrived(R.at[2, 0, at(e), c], f_r.at[0, e])
        arrived(R.at[2, 1, at(e), c], f_r.at[1, e])
        keep(send(R.at[2, :, at(e), c], R.at[2, :, at(e), c], p_s.at[2, e], p_r.at[2, e], partner))

    def partner_done(dy):
        for e in ORDER:
            arrived(R.at[dy, :, at(e), 1 - c], p_r.at[dy, e])

    for e in (1, 3, 2):
        keep(send(rho.at[wrap(x + e)], R.at[0, :, x, c], x_s.at[e], x_r.at[e], dev(x + e, y, z, c)))
    spread(0)
    my_lanes = lanes(zh * 2 + c)
    for dz in (1, 3, 2):
        keep(send(xin, XF.at[:, :, :, my_lanes], v_s.at[dz], v_r.at[dz, c], dev(x, y, z + dz, zl)))

    @pl.when(unaligned)
    def _():
        send(xin, XF.at[:, :, :, my_lanes], v_s.at[0], v_r.at[0, c], partner)

    @pl.when(aligned)
    def _():
        send(FQ.at[0], FQ.at[1], q_s, q_r, dev(x, y, z - 1, c))

    for dy, dx, cc in plane:
        send(D.at[x * 2 + c], D.at[dy * 8 + x * 2 + c], d_s, d_r, dev(x + dx, y + dy, z, c + cc))

    def vectors_done():
        @pl.when(aligned)
        def _():
            arrived(XF.at[:, :, :, lanes(zh * 2 + 1 - c)], v_r.at[0, 1 - c])
            for cc in range(2):
                arrived(XF.at[:, :, :, lanes((1 - zh) * 2 + cc)], v_r.at[2, cc])

        @pl.when(unaligned)
        def _():
            for dz in (1, 3):
                for cc in range(2):
                    arrived(XF.at[:, :, :, lanes((wrap(z - dz) // 2) * 2 + cc)], v_r.at[dz, cc])

    def cross(dy):
        v = XF[...].reshape(512, 2048)
        t_re = dot_nt(v, R[dy, 0].reshape(256, 2048)).reshape(4, 2, 64, 256)
        t_im = dot_nt(v, R[dy, 1].reshape(256, 2048)).reshape(4, 2, 64, 256)
        re = t_re[:, 0] + t_im[:, 1]
        im = t_re[:, 1] - t_im[:, 0]
        C32[dy, :, 0] = re
        C32[dy, :, 1] = im
        CB[dy, :, 0] = re.astype(jnp.bfloat16)
        CB[dy, :, 1] = im.astype(jnp.bfloat16)
        for e in (1, 3, 2):
            keep(send(CB.at[dy, wrap(x + e)], CR.at[dy, e], c_s.at[dy, e], c_r.at[dy, e], dev(x + e, y, z, c)))

    def scale(dy):
        total = C32[dy, x]
        for e in (1, 2, 3):
            arrived(CR.at[dy, e], c_r.at[dy, e])
        for e in (1, 2, 3):
            total = total + CR[dy, e].astype(jnp.float32)
        halves = []
        for h in range(2):
            first = dy * 8 + h * 4
            halves.append(D[first] + D[first + 1] + D[first + 2] + D[first + 3])
        delta = jnp.concatenate(halves, axis=1)[0:1]
        own = FQ[1, x][0:1, 0:1]
        ratio = delta / (delta * delta + own * own)
        weight = (-4.0 * prefactor * ratio).astype(jnp.bfloat16).astype(jnp.float32)
        scaled = (weight[None] * total).astype(jnp.bfloat16)
        SF[dy, x] = scaled
        for e in (1, 3, 2):
            keep(send(SF.at[dy, x], SF.at[dy, x], g_s.at[dy, e], g_r.at[dy, e], dev(x + e, y, z, c)))
        flat = total.reshape(128, 256)
        high = flat.astype(jnp.bfloat16)
        low = (flat - high.astype(jnp.float32)).astype(jnp.bfloat16)
        part = dot_nt(jnp.concatenate([high, low], axis=0), scaled.reshape(128, 256))
        if dy == 0:
            SA[...] = part
        else:
            SA[...] += part

    def gathered(dy):
        for e in (1, 3, 2):
            arrived(SF.at[dy, at(e)], g_r.at[dy, e])
        re, im = SF[dy, :, 0], SF[dy, :, 1]
        L[:, 0, :, 0:256] = re
        L[:, 0, :, 256:512] = -im
        L[:, 1, :, 0:256] = im
        L[:, 1, :, 256:512] = re

    def image_tile(dy, block):
        at_lanes = lanes(block)
        return jnp.dot(
            L[...].reshape(512, 512),
            R[dy, :, :, :, :, at_lanes].reshape(512, 512),
            preferred_element_type=jnp.float32,
        )

    def image(dy):
        gathered(dy)

        @pl.loop(0, 4)
        def _(block):
            part = image_tile(dy, block)
            if dy == 0:
                acc[:, lanes(block)] = part
            else:
                acc[:, lanes(block)] += part

    def stage(name, fn, *args):
        with jax.named_scope(name):
            fn(*args)

    def from_x(e):
        arrived(R.at[0, :, at(e), c], x_r.at[e])
        spread(e)

    def energies_done():
        most = D.at[pl.ds(0, 31)]
        arrived(most, d_r)
        sent(most, d_s)

        @pl.when(aligned)
        def _():
            sent(FQ.at[0], q_s)

        @pl.when(unaligned)
        def _():
            arrived(FQ.at[1], q_r)

    stage("x1", from_x, 1)
    stage("x3", from_x, 3)
    stage("pass0", pass_on, 0)
    stage("x2", from_x, 2)
    stage("pass1", pass_on, 1)
    stage("pass3", pass_on, 3)
    stage("vectors", vectors_done)
    stage("partner0", partner_done, 0)
    stage("cross0", cross, 0)
    stage("pass2", pass_on, 2)
    stage("partner1", partner_done, 1)
    stage("cross1", cross, 1)
    stage("partner3", partner_done, 3)
    stage("cross3", cross, 3)
    stage("far0", pass_far, 0)
    stage("energies", energies_done)
    stage("scale0", scale, 0)
    stage("far1", pass_far, 1)
    stage("far3", pass_far, 3)
    stage("scale1", scale, 1)
    stage("far2", pass_far, 2)
    stage("partner2", partner_done, 2)
    stage("cross2", cross, 2)
    stage("scale3", scale, 3)
    stage("image0", image, 0)
    stage("image1", image, 1)
    stage("scale2", scale, 2)

    def project_z():
        both = SA[0:128] + SA[128:256]
        re = both[0:64, 0:64] + both[64:128, 64:128]
        im = both[0:64, 64:128] - both[64:128, 0:64]
        SZ[z] = jnp.concatenate([re, im], axis=1) / grid_count

        @pl.when(aligned)
        def _():
            send(SZ.at[z], SZ.at[z], u_s.at[0], u_r.at[2], dev(x, y, z + 2, c))

        @pl.when(unaligned)
        def _():
            for k, dz in enumerate((1, 3)):
                send(SZ.at[z], SZ.at[z], u_s.at[k], u_r.at[dz], dev(x, y, z + dz, c))

    def project_x():
        @pl.when(aligned)
        def _():
            for dz in (1, 3, 2):
                arrived(SZ.at[wrap(z - dz)], u_r.at[dz])
            SO[x] = SZ[0] + SZ[1] + SZ[2] + SZ[3]
            for e in (1, 3, 2):
                for cc in range(2):
                    send(SO.at[x], SO.at[x], w_s.at[e, cc], w_r.at[e], dev(x + e, y, z, cc))
            send(SO.at[x], SO.at[x], w_s.at[0, 0], w_r.at[0], dev(x, y, z, 1 - c))

    def project_done():
        @pl.when(unaligned)
        def _():
            arrived(SO.at[x], w_r.at[0])

        for e in (1, 3, 2):
            arrived(SO.at[at(e)], w_r.at[e])
        for f in range(4):
            both = SO[f]
            sub[f, 0] = both[:, 0:64]
            sub[f, 1] = both[:, 64:128]

    stage("project_z", project_z)
    stage("image3", image, 3)
    stage("gathered2", gathered, 2)

    def target(step):
        h = 1 - zh if step < 2 else zh
        cc = 1 - c if step % 2 == 0 else c
        to_z = h * 2 + c
        dz = wrap(to_z - z)
        return h * 2 + cc, cc, to_z, dz, (3 - dz) // 2

    def image_out(step):
        block, cc, to_z, dz, direct = target(step)
        total = acc[:, lanes(block)] + image_tile(2, block)
        half = total.astype(jnp.bfloat16).reshape(2, 2, 2, 64, 512)
        SB[step] = half

        @pl.when(unaligned)
        def _():
            acc[:, lanes(block)] = total
            send(SB.at[step, direct], RI.at[dz, direct], i_s.at[step, direct], i_r.at[dz, direct], dev(x, y, to_z, cc))

        @pl.when(aligned)
        def _():
            if step < 2:
                send(SB.at[step, 0], RC.at[0, cc], i_s.at[step, 0], k_r.at[0, cc], dev(x, y, z + 1, c))
                send(SB.at[step, 1], RC.at[1, cc], i_s.at[step, 1], k_r.at[1, cc], dev(x, y, z - 1, c))
            elif step == 2:
                send(SB.at[step], RI.at[0], i_s.at[step, 0], i_r.at[0, 0], partner)
            else:
                RI[0] = half

    def image_join(step):
        block, cc, to_z, dz, direct = target(step)
        joined = 1 - direct
        arrived(RC.at[joined, cc], k_r.at[joined, cc])
        rows = pl.ds(pl.multiple_of(joined * 256, 256), 256)
        total = acc[rows, lanes(block)].reshape(2, 2, 64, 512) + RC[joined, cc].astype(jnp.float32)
        SB[step, joined] = total.astype(jnp.bfloat16)
        send(SB.at[step, joined], RI.at[dz, joined], i_s.at[step, joined], i_r.at[dz, joined], dev(x, y, to_z, cc))

    for step in range(4):
        stage(f"out{step}", image_out, step)
    stage("project_x", project_x)

    @pl.when(unaligned)
    def _():
        for step in (0, 2, 1, 3):
            stage(f"join{step}", image_join, step)

    stage("project", project_done)

    def images_done():
        for dz in (1, 3):
            for q in range(2):
                arrived(RI.at[dz, q], i_r.at[dz, q])

        @pl.when(unaligned)
        def _():
            arrived(RI.at[0], i_r.at[0, 0])

    stage("images", images_done)

    @pl.loop(0, 2)
    def _(q):
        for r in range(2):
            total = RI[0, q, r].astype(jnp.float32)
            for dz in (1, 3):
                total = total + RI[dz, q, r].astype(jnp.float32)
            img[q * 2 + r] = total

    def drain():
        for copy in pending:
            copy.wait_send()

        @pl.when(unaligned)
        def _():
            sent(xin, v_s.at[0])
            for step in range(4):
                for q in range(2):
                    sent(SB.at[step, q], i_s.at[step, q])
            for k in range(2):
                sent(SZ.at[z], u_s.at[k])

        @pl.when(aligned)
        def _():
            for step in range(2):
                for q in range(2):
                    sent(SB.at[step, q], i_s.at[step, q])
            sent(SB.at[2], i_s.at[2, 0])
            sent(SZ.at[z], u_s.at[0])
            for e in (1, 3, 2):
                for cc in range(2):
                    sent(SO.at[x], w_s.at[e, cc])
            sent(SO.at[x], w_s.at[0, 0])

    stage("drain", drain)


def shards(pair_density, trial_vectors, frequency, val_energy, cond_energy, pair_index):
    groups = lax.axis_size("freq")
    members = lax.axis_size("band")
    pair_count = pair_density.shape[0] * groups * members
    grid_count = trial_vectors.shape[3] * members
    prefactor = 1.0 / math.sqrt(2.0 * grid_count * pair_count)
    pieces = jnp.transpose(pair_density.reshape(32, 2, 4, 2048), (2, 1, 0, 3))
    bf, f32 = jnp.bfloat16, jnp.float32
    vmem = pl.BlockSpec(memory_space=pltpu.VMEM)
    smem = pl.BlockSpec(memory_space=pltpu.SMEM)
    dma = pltpu.SemaphoreType.DMA
    return pl.pallas_call(
        functools.partial(kernel, (prefactor, grid_count)),
        name="response",
        out_shape=(
            jax.ShapeDtypeStruct((4, 2, 64, 512), f32),
            jax.ShapeDtypeStruct((4, 2, 64, 64), f32),
        ),
        in_specs=[vmem, vmem, smem, smem, smem, smem],
        out_specs=(vmem, vmem),
        scratch_shapes=[
            pltpu.VMEM((4, 2, 4, 2, 32, 2048), bf),
            pltpu.VMEM((4, 2, 64, 2048), bf),
            pltpu.VMEM((512, 2048), f32),
            pltpu.VMEM((4, 4, 2, 64, 256), f32),
            pltpu.VMEM((4, 4, 2, 64, 256), bf),
            pltpu.VMEM((4, 4, 2, 64, 256), bf),
            pltpu.VMEM((4, 4, 2, 64, 256), bf),
            pltpu.VMEM((4, 2, 64, 512), bf),
            pltpu.VMEM((4, 2, 2, 2, 64, 512), bf),
            pltpu.VMEM((4, 2, 2, 2, 64, 512), bf),
            pltpu.VMEM((2, 2, 2, 2, 64, 512), bf),
            pltpu.VMEM((32, 8, 128), f32),
            pltpu.VMEM((4, 64, 128), f32),
            pltpu.VMEM((4, 64, 128), f32),
            pltpu.VMEM((256, 128), f32),
            pltpu.VMEM((2, 4, 8, 128), f32),
            dma((4,)), dma((4,)),
            dma((2, 4)), dma((2, 4)),
            dma((2, 4)), dma((2, 4)),
            dma((4, 4)), dma((4, 4)),
            dma((4,)), dma((4, 2)),
            dma((4, 4)), dma((4, 4)),
            dma((4, 4)), dma((4, 4)),
            dma((4, 2)), dma((4, 2)), dma((2, 2)),
            dma, dma,
            dma((2,)), dma((4,)),
            dma((4, 2)), dma((4,)),
            dma, dma,
        ],
        compiler_params=pltpu.CompilerParams(
            collective_id=0, has_side_effects=True, vmem_limit_bytes=56 * 2**20
        ),
    )(pieces, trial_vectors, pair_index, cond_energy, val_energy, frequency)


def solution(mesh):
    return jax.shard_map(
        shards,
        mesh=mesh,
        in_specs=(
            P(("freq", "band"), None, None),
            P("freq", None, None, "band"),
            P("freq"),
            P(),
            P(),
            P(("freq", "band")),
        ),
        out_specs=(P("freq", None, None, "band"), P("freq", None, None, None)),
        check_vma=False,
    )
```

```python
import functools
import math

import jax
import jax.numpy as jnp
from jax import lax
from jax.experimental import pallas as pl
from jax.experimental.pallas import tpu as pltpu
from jax.sharding import PartitionSpec as P

MESH = pl.DeviceIdType.MESH
ORDER = (0, 1, 3, 2)


def wrap(v, n=4):
    return lax.rem(v + n, n)


def dev(x, y, z, c):
    x, y, z, c = wrap(x), wrap(y), wrap(z), wrap(c, 2)
    return (lax.rem(z, 2) * 4 + y, x * 4 + (z // 2) * 2 + c)


def dot_nt(a, b):
    return lax.dot_general(a, b, (((1,), (1,)), ((), ())), preferred_element_type=jnp.float32)


def kernel(
    consts,
    rho, xin, idx, cond, val, freq,
    img, sub,
    R, XF, acc, C32, CB, CR, SF, L, SB, RI, RC, D, SZ, SO, SA, FQ,
    x_s, x_r, y_s, y_r, f_s, f_r, p_s, p_r, v_s, v_r, t_s, c_s, c_r, g_s, g_r,
    i_s, i_r, k_r, d_s, d_r, u_s, u_r, w_s, w_r, q_s, q_r,
):
    prefactor, grid_count = consts
    fi, bi = lax.axis_index("freq"), lax.axis_index("band")
    zl, y = fi // 4, lax.rem(fi, 4)
    x, zh, c = bi // 4, lax.rem(bi // 2, 2), lax.rem(bi, 2)
    z = zh * 2 + zl
    me = (fi, bi)
    partner = dev(x, y, z, 1 - c)
    aligned = zl == c
    unaligned = jnp.logical_not(aligned)
    pending = []

    def send(src, dst, ss, rs, to):
        copy = pltpu.make_async_remote_copy(
            src_ref=src, dst_ref=dst, send_sem=ss, recv_sem=rs, device_id=to, device_id_type=MESH
        )
        copy.start()
        return copy

    def keep(copy):
        pending.append(copy)

    def arrived(dst, rs):
        pltpu.make_async_remote_copy(
            src_ref=dst, dst_ref=dst, send_sem=rs, recv_sem=rs, device_id=me, device_id_type=MESH
        ).wait_recv()

    def sent(src, ss):
        pltpu.make_async_remote_copy(
            src_ref=src, dst_ref=src, send_sem=ss, recv_sem=ss, device_id=me, device_id_type=MESH
        ).wait_send()

    plane = [
        (dy, dx, cc) for dy in range(4) for dx in range(4) for cc in range(2) if (dy, dx, cc) != (0, 0, 0)
    ]
    barrier = pltpu.get_barrier_semaphore()
    for dy, dx, cc in plane:
        pl.semaphore_signal(barrier, inc=1, device_id=dev(x + dx, y + dy, z, c + cc), device_id_type=MESH)
    for dz in (1, 2, 3):
        for cc in range(2):
            pl.semaphore_signal(barrier, inc=1, device_id=dev(x, y, z + dz, cc), device_id_type=MESH)
    with jax.named_scope("entry"):
        pl.semaphore_wait(barrier, len(plane) + 6)

    def lanes(block):
        return pl.ds(pl.multiple_of(block * 512, 512), 512)

    def stage(name, fn, *args):
        with jax.named_scope(name):
            fn(*args)

    def at(e):
        return wrap(x - e)

    def spread(h, e):
        src = rho.at[x, h] if e == 0 else R.at[h, 0, :, at(e), c]
        keep(send(src, R.at[h, 1, :, at(e), c], y_s.at[h, 0, e], y_r.at[h, 0, e], dev(x, y + 1, z, c)))
        keep(send(src, R.at[h, 2, :, at(e), c], y_s.at[h, 1, e], y_r.at[h, 1, e], dev(x, y - 1, z, c)))
        keep(send(src, R.at[h, 0, :, at(e), c], p_s.at[h, 0, e], p_r.at[h, 0, e], partner))

    def pass_on(h, e):
        for side in range(2):
            to = dev(x, y + 1 - 2 * side, z, c)
            piece = R.at[h, 1 + side, :, at(e), c]
            arrived(piece, y_r.at[h, side, e])
            part = R.at[h, 1 + side, side, at(e), c]
            keep(send(part, R.at[h, 3, side, at(e), c], f_s.at[h, side, e], f_r.at[h, side, e], to))
            keep(send(piece, piece, p_s.at[h, 1 + side, e], p_r.at[h, 1 + side, e], partner))

    def pass_far(h, e):
        for side in range(2):
            arrived(R.at[h, 3, side, at(e), c], f_r.at[h, side, e])
        piece = R.at[h, 3, :, at(e), c]
        keep(send(piece, piece, p_s.at[h, 3, e], p_r.at[h, 3, e], partner))

    def partner_done(h, pos):
        for e in ORDER:
            arrived(R.at[h, pos, :, at(e), 1 - c], p_r.at[h, pos, e])

    def from_x(h, e):
        arrived(R.at[h, 0, :, at(e), c], x_r.at[h, e])
        spread(h, e)

    my_lanes = lanes(zh * 2 + c)

    def vector_piece(q, zz, cc):
        return XF.at[pl.ds(2 * q, 2), :, :, lanes((wrap(zz) // 2) * 2 + cc)]

    def begin():
        spread(0, 0)
        for h in range(2):
            for e in (1, 3, 2):
                keep(send(rho.at[wrap(x + e), h], R.at[h, 0, :, x, c], x_s.at[h, e], x_r.at[h, e], dev(x + e, y, z, c)))
        for k in range(2):
            for side in range(2):
                q = (k + side) % 2
                dz = 1 + 2 * side
                keep(send(xin.at[pl.ds(2 * q, 2)], vector_piece(q, z, c), v_s.at[dz, q], v_r.at[dz, c, q], dev(x, y, z + dz, zl)))
        spread(1, 0)

        @pl.when(unaligned)
        def _():
            send(xin, XF.at[:, :, :, my_lanes], v_s.at[0, 0], v_r.at[0, c, 0], partner)

        for f in range(4):
            FQ[0, f] = jnp.full((8, 128), freq[f], jnp.float32)

        lane = lax.broadcasted_iota(jnp.int32, (8, 128), 1)
        row = lax.broadcasted_iota(jnp.int32, (8, 128), 0)
        place = jnp.bitwise_and(row, 1) * 16 + jnp.bitwise_and(lane, 15)
        number = jnp.zeros((8, 128), jnp.int32)
        for i in range(32):
            number = jnp.where(place == i, idx[i], number)
        cond_no = jnp.bitwise_and(number, 127)
        val_no = jnp.right_shift(number, 7)
        zero = jnp.zeros((8, 128), jnp.float32)
        cond_pick = lax.fori_loop(0, 128, lambda j, a: jnp.where(cond_no == j, cond[j], a), zero)
        val_pick = lax.fori_loop(0, 32, lambda j, a: jnp.where(val_no == j, val[j], a), zero)
        D[x * 2 + c] = jnp.where(jnp.right_shift(lane, 4) == x * 2 + c, cond_pick - val_pick, 0.0)
        for h in range(2):
            R[h, 0, :, x, c] = rho[x, h]

        @pl.when(aligned)
        def _():
            XF[:, :, :, my_lanes] = xin[...]
            FQ[1] = FQ[0]

        @pl.when(aligned)
        def _():
            send(FQ.at[0], FQ.at[1], q_s, q_r, dev(x, y, z - 1, c))

        for dy, dx, cc in plane:
            pos = (0, 1, 3, 2)[dy]
            send(D.at[x * 2 + c], D.at[pos * 8 + x * 2 + c], d_s, d_r, dev(x + dx, y + dy, z, c + cc))

    def vectors_pass():
        @pl.when(unaligned)
        def _():
            for q in range(2):
                dz = 1 + 2 * q
                for cc in range(2):
                    piece = vector_piece(q, z - dz, cc)
                    arrived(piece, v_r.at[dz, cc, q])
                    send(piece, piece, t_s.at[q, cc], v_r.at[2, cc, q], dev(x, y, z + dz, c))

    def vectors_done():
        @pl.when(aligned)
        def _():
            arrived(XF.at[:, :, :, lanes(zh * 2 + 1 - c)], v_r.at[0, 1 - c, 0])
            for q in range(2):
                for cc in range(2):
                    arrived(vector_piece(q, z + 2, cc), v_r.at[2, cc, q])

        @pl.when(unaligned)
        def _():
            for q in range(2):
                dz = 3 - 2 * q
                for cc in range(2):
                    arrived(vector_piece(q, z - dz, cc), v_r.at[dz, cc, q])

    A, FAR, B, LAST = (0, 0, 3), (0, 3, 4), (1, 0, 3), (1, 3, 4)

    def cross(h, pos):
        t = dot_nt(XF[...].reshape(512, 2048), R[h, pos].reshape(256, 2048)).reshape(4, 2, 64, 256)
        re = t[:, 0, :, 0:128] + t[:, 1, :, 128:256]
        im = t[:, 1, :, 0:128] - t[:, 0, :, 128:256]
        C32[h, :, pos, 0] = re
        C32[h, :, pos, 1] = im
        CB[h, :, pos, 0] = re.astype(jnp.bfloat16)
        CB[h, :, pos, 1] = im.astype(jnp.bfloat16)

    def cross_out(h, pos):
        for e in (1, 3, 2):
            keep(send(CB.at[h, wrap(x + e), pos], CR.at[h, e, pos], c_s.at[h, pos, e], c_r.at[h, pos, e], dev(x + e, y, z, c)))

    def scale(h, pos):
        for e in (1, 3, 2):
            arrived(CR.at[h, e, pos], c_r.at[h, pos, e])
        own = FQ[1, x][0:1, 0:1]
        total = C32[h, x, pos]
        for e in (1, 2, 3):
            total = total + CR[h, e, pos].astype(jnp.float32)
        delta = D[pos * 8]
        for k in range(1, 8):
            delta = delta + D[pos * 8 + k]
        delta = delta[h : h + 1]
        ratio = delta / (delta * delta + own * own)
        weight = (-4.0 * prefactor * ratio).astype(jnp.bfloat16).astype(jnp.float32)
        SF[h, x, pos] = (weight[None] * total).astype(jnp.bfloat16)
        C32[h, x, pos] = total
        for e in (1, 3, 2):
            keep(send(SF.at[h, x, pos], SF.at[h, x, pos], g_s.at[h, pos, e], g_r.at[h, pos, e], dev(x + e, y, z, c)))

    def project_add(group):
        h = group[0]
        for pos in range(group[1], group[2]):
            flat = C32[h, x, pos].reshape(128, 128)
            high = flat.astype(jnp.bfloat16)
            low = (flat - high.astype(jnp.float32)).astype(jnp.bfloat16)
            part = dot_nt(jnp.concatenate([high, low], axis=0), SF[h, x, pos].reshape(128, 128))
            if h == 0 and pos == 0:
                SA[...] = part
            else:
                SA[...] += part

    def gathered(group):
        h = group[0]
        for pos in range(group[1], group[2]):
            for e in (1, 3, 2):
                arrived(SF.at[h, at(e), pos], g_r.at[h, pos, e])
        for pos in range(group[1], group[2]):
            base = (pos - group[1]) * 256
            re, im = SF[h, :, pos, 0], SF[h, :, pos, 1]
            L[:, 0, :, base : base + 128] = re
            L[:, 0, :, base + 128 : base + 256] = -im
            L[:, 1, :, base : base + 128] = im
            L[:, 1, :, base + 128 : base + 256] = re

    def image_tile(group, block):
        h, some = group[0], pl.ds(group[1], group[2] - group[1])
        depth = (group[2] - group[1]) * 256
        return jnp.dot(
            L[:, :, :, 0:depth].reshape(512, depth),
            R[h, some, :, :, :, :, lanes(block)].reshape(depth, 512),
            preferred_element_type=jnp.float32,
        )

    def image(group):
        gathered(group)
        for block in range(4):
            part = image_tile(group, block)
            if group == A:
                acc[:, block * 512 : block * 512 + 512] = part
            else:
                acc[:, block * 512 : block * 512 + 512] += part

    def energies_done():
        most = D.at[pl.ds(0, 31)]
        arrived(most, d_r)
        sent(most, d_s)

        @pl.when(aligned)
        def _():
            sent(FQ.at[0], q_s)

        @pl.when(unaligned)
        def _():
            arrived(FQ.at[1], q_r)

    stage("begin", begin)
    stage("xA1", from_x, 0, 1)
    stage("xA3", from_x, 0, 3)
    stage("passA0", pass_on, 0, 0)
    stage("xA2", from_x, 0, 2)
    stage("relay", vectors_pass)
    stage("passA1", pass_on, 0, 1)
    stage("passA3", pass_on, 0, 3)
    stage("xB1", from_x, 1, 1)
    stage("xB3", from_x, 1, 3)
    stage("farA0", pass_far, 0, 0)
    stage("passA2", pass_on, 0, 2)
    stage("passB0", pass_on, 1, 0)
    stage("xB2", from_x, 1, 2)
    stage("vectors", vectors_done)
    stage("partA0", partner_done, 0, 0)
    stage("crossA0", cross, 0, 0)
    stage("outA0", cross_out, 0, 0)
    stage("farA1", pass_far, 0, 1)
    stage("partA1", partner_done, 0, 1)
    stage("crossA1", cross, 0, 1)
    stage("outA1", cross_out, 0, 1)
    stage("farA3", pass_far, 0, 3)
    stage("partA2", partner_done, 0, 2)
    stage("crossA2", cross, 0, 2)
    stage("outA2", cross_out, 0, 2)
    stage("partB0", partner_done, 1, 0)
    stage("crossB0", cross, 1, 0)
    stage("outB0", cross_out, 1, 0)
    stage("passB1", pass_on, 1, 1)
    stage("energies", energies_done)
    stage("scaleA0", scale, 0, 0)
    stage("scaleA1", scale, 0, 1)
    stage("passB3", pass_on, 1, 3)
    stage("farA2", pass_far, 0, 2)
    stage("partA3", partner_done, 0, 3)
    stage("crossA3", cross, 0, 3)
    stage("outA3", cross_out, 0, 3)
    stage("scaleA2", scale, 0, 2)
    stage("passB2", pass_on, 1, 2)
    stage("farB0", pass_far, 1, 0)
    stage("partB1", partner_done, 1, 1)
    stage("crossB1", cross, 1, 1)
    stage("outB1", cross_out, 1, 1)
    stage("scaleB0", scale, 1, 0)
    stage("farB1", pass_far, 1, 1)
    stage("partB2", partner_done, 1, 2)
    stage("crossB2", cross, 1, 2)
    stage("outB2", cross_out, 1, 2)
    stage("farB3", pass_far, 1, 3)
    stage("scaleA3", scale, 0, 3)
    stage("farB2", pass_far, 1, 2)
    stage("partB3", partner_done, 1, 3)
    stage("crossB3", cross, 1, 3)
    stage("outB3", cross_out, 1, 3)
    stage("scaleB1", scale, 1, 1)
    stage("imageA", image, A)
    stage("scaleB2", scale, 1, 2)
    stage("scaleB3", scale, 1, 3)
    stage("imageF", image, FAR)
    stage("addA", project_add, A)
    stage("addF", project_add, FAR)
    stage("addB", project_add, B)
    stage("addL", project_add, LAST)

    def project_z():
        both = SA[0:128] + SA[128:256]
        re = both[0:64, 0:64] + both[64:128, 64:128]
        im = both[0:64, 64:128] - both[64:128, 0:64]
        SZ[z] = jnp.concatenate([re, im], axis=1) / grid_count

        @pl.when(aligned)
        def _():
            send(SZ.at[z], SZ.at[z], u_s.at[0], u_r.at[2], dev(x, y, z + 2, c))

        @pl.when(unaligned)
        def _():
            for k, dz in enumerate((1, 3)):
                send(SZ.at[z], SZ.at[z], u_s.at[k], u_r.at[dz], dev(x, y, z + dz, c))

    def project_x():
        @pl.when(aligned)
        def _():
            for dz in (1, 3, 2):
                arrived(SZ.at[wrap(z - dz)], u_r.at[dz])
            SO[x] = SZ[0] + SZ[1] + SZ[2] + SZ[3]
            for e in (1, 3, 2):
                for cc in range(2):
                    send(SO.at[x], SO.at[x], w_s.at[e, cc], w_r.at[e], dev(x + e, y, z, cc))
            send(SO.at[x], SO.at[x], w_s.at[0, 0], w_r.at[0], dev(x, y, z, 1 - c))

    def project_done():
        @pl.when(unaligned)
        def _():
            arrived(SO.at[x], w_r.at[0])

        for e in (1, 3, 2):
            arrived(SO.at[at(e)], w_r.at[e])
        for f in range(4):
            both = SO[f]
            sub[f, 0] = both[:, 0:64]
            sub[f, 1] = both[:, 64:128]

    stage("project_z", project_z)
    stage("imageB", image, B)
    stage("gatheredL", gathered, LAST)

    def target(step):
        h = 1 - zh if step < 2 else zh
        cc = 1 - c if step % 2 == 0 else c
        to_z = h * 2 + c
        dz = wrap(to_z - z)
        return h * 2 + cc, cc, to_z, dz, (3 - dz) // 2

    def image_out(step):
        block, cc, to_z, dz, direct = target(step)
        total = acc[:, lanes(block)] + image_tile(LAST, block)
        half = total.astype(jnp.bfloat16).reshape(2, 2, 2, 64, 512)
        SB[step] = half

        @pl.when(unaligned)
        def _():
            acc[:, lanes(block)] = total
            send(SB.at[step, direct], RI.at[dz, direct], i_s.at[step, direct], i_r.at[dz, direct], dev(x, y, to_z, cc))

        @pl.when(aligned)
        def _():
            if step < 2:
                send(SB.at[step, 0], RC.at[0, cc], i_s.at[step, 0], k_r.at[0, cc], dev(x, y, z + 1, c))
                send(SB.at[step, 1], RC.at[1, cc], i_s.at[step, 1], k_r.at[1, cc], dev(x, y, z - 1, c))
            elif step == 2:
                send(SB.at[step], RI.at[0], i_s.at[step, 0], i_r.at[0, 0], partner)
            else:
                RI[0] = half

    def image_join(step):
        block, cc, to_z, dz, direct = target(step)
        joined = 1 - direct
        arrived(RC.at[joined, cc], k_r.at[joined, cc])
        rows = pl.ds(pl.multiple_of(joined * 256, 256), 256)
        total = acc[rows, lanes(block)].reshape(2, 2, 64, 512) + RC[joined, cc].astype(jnp.float32)
        SB[step, joined] = total.astype(jnp.bfloat16)
        send(SB.at[step, joined], RI.at[dz, joined], i_s.at[step, joined], i_r.at[dz, joined], dev(x, y, to_z, cc))

    for step in range(4):
        stage(f"out{step}", image_out, step)
    stage("project_x", project_x)

    @pl.when(unaligned)
    def _():
        for step in (0, 2, 1, 3):
            stage(f"join{step}", image_join, step)

    stage("project", project_done)

    def images_done():
        for dz in (1, 3):
            for q in range(2):
                arrived(RI.at[dz, q], i_r.at[dz, q])

        @pl.when(unaligned)
        def _():
            arrived(RI.at[0], i_r.at[0, 0])

    stage("images", images_done)

    @pl.loop(0, 2)
    def _(q):
        for r in range(2):
            total = RI[0, q, r].astype(jnp.float32)
            for dz in (1, 3):
                total = total + RI[dz, q, r].astype(jnp.float32)
            img[q * 2 + r] = total

    def drain():
        for copy in pending:
            copy.wait_send()

        @pl.when(unaligned)
        def _():
            sent(xin, v_s.at[0, 0])
            for q in range(2):
                for cc in range(2):
                    sent(vector_piece(q, z - 1 - 2 * q, cc), t_s.at[q, cc])
            for step in range(4):
                for q in range(2):
                    sent(SB.at[step, q], i_s.at[step, q])
            for k in range(2):
                sent(SZ.at[z], u_s.at[k])

        @pl.when(aligned)
        def _():
            for step in range(2):
                for q in range(2):
                    sent(SB.at[step, q], i_s.at[step, q])
            sent(SB.at[2], i_s.at[2, 0])
            sent(SZ.at[z], u_s.at[0])
            for e in (1, 3, 2):
                for cc in range(2):
                    sent(SO.at[x], w_s.at[e, cc])
            sent(SO.at[x], w_s.at[0, 0])

    stage("drain", drain)


def shards(pair_density, trial_vectors, frequency, val_energy, cond_energy, pair_index):
    groups = lax.axis_size("freq")
    members = lax.axis_size("band")
    pair_count = pair_density.shape[0] * groups * members
    grid_count = trial_vectors.shape[3] * members
    prefactor = 1.0 / math.sqrt(2.0 * grid_count * pair_count)
    pieces = jnp.transpose(pair_density.reshape(2, 16, 2, 4, 2048), (3, 0, 2, 1, 4))
    bf, f32 = jnp.bfloat16, jnp.float32
    vmem = pl.BlockSpec(memory_space=pltpu.VMEM)
    smem = pl.BlockSpec(memory_space=pltpu.SMEM)
    dma = pltpu.SemaphoreType.DMA
    return pl.pallas_call(
        functools.partial(kernel, (prefactor, grid_count)),
        name="response",
        out_shape=(
            jax.ShapeDtypeStruct((4, 2, 64, 512), f32),
            jax.ShapeDtypeStruct((4, 2, 64, 64), f32),
        ),
        in_specs=[vmem, vmem, smem, smem, smem, smem],
        out_specs=(vmem, vmem),
        scratch_shapes=[
            pltpu.VMEM((2, 4, 2, 4, 2, 16, 2048), bf),
            pltpu.VMEM((4, 2, 64, 2048), bf),
            pltpu.VMEM((512, 2048), f32),
            pltpu.VMEM((2, 4, 4, 2, 64, 128), f32),
            pltpu.VMEM((2, 4, 4, 2, 64, 128), bf),
            pltpu.VMEM((2, 4, 4, 2, 64, 128), bf),
            pltpu.VMEM((2, 4, 4, 2, 64, 128), bf),
            pltpu.VMEM((4, 2, 64, 768), bf),
            pltpu.VMEM((4, 2, 2, 2, 64, 512), bf),
            pltpu.VMEM((4, 2, 2, 2, 64, 512), bf),
            pltpu.VMEM((2, 2, 2, 2, 64, 512), bf),
            pltpu.VMEM((32, 8, 128), f32),
            pltpu.VMEM((4, 64, 128), f32),
            pltpu.VMEM((4, 64, 128), f32),
            pltpu.VMEM((256, 128), f32),
            pltpu.VMEM((2, 4, 8, 128), f32),
            dma((2, 4)), dma((2, 4)),
            dma((2, 2, 4)), dma((2, 2, 4)),
            dma((2, 2, 4)), dma((2, 2, 4)),
            dma((2, 4, 4)), dma((2, 4, 4)),
            dma((4, 2)), dma((4, 2, 2)), dma((2, 2)),
            dma((2, 4, 4)), dma((2, 4, 4)),
            dma((2, 4, 4)), dma((2, 4, 4)),
            dma((4, 2)), dma((4, 2)), dma((2, 2)),
            dma, dma,
            dma((2,)), dma((4,)),
            dma((4, 2)), dma((4,)),
            dma, dma,
        ],
        compiler_params=pltpu.CompilerParams(
            collective_id=0, has_side_effects=True, vmem_limit_bytes=56 * 2**20
        ),
    )(pieces, trial_vectors, pair_index, cond_energy, val_energy, frequency)


def solution(mesh):
    return jax.shard_map(
        shards,
        mesh=mesh,
        in_specs=(
            P(("freq", "band"), None, None),
            P("freq", None, None, "band"),
            P("freq"),
            P(),
            P(),
            P(("freq", "band")),
        ),
        out_specs=(P("freq", None, None, "band"), P("freq", None, None, None)),
        check_vma=False,
    )
```

```python
import functools
import math

import jax
import jax.numpy as jnp
from jax import lax
from jax.experimental import pallas as pl
from jax.experimental.pallas import tpu as pltpu
from jax.sharding import PartitionSpec as P

MESH = pl.DeviceIdType.MESH
ORDER = (0, 1, 3, 2)


def wrap(v, n=4):
    return lax.rem(v + n, n)


def dev(x, y, z, c):
    x, y, z, c = wrap(x), wrap(y), wrap(z), wrap(c, 2)
    return (lax.rem(z, 2) * 4 + y, x * 4 + (z // 2) * 2 + c)


def dot_nt(a, b):
    return lax.dot_general(a, b, (((1,), (1,)), ((), ())), preferred_element_type=jnp.float32)


def kernel(
    consts,
    rho, xin, idx, cond, val, freq,
    RI, sub,
    R, XF, acc, C32, CB, CR, SF, L, SB, RC, D, SZ, SO, SA, FQ,
    x_s, x_r, y_s, y_r, f_s, f_r, p_s, p_r, v_s, v_r, t_s, c_s, c_r, g_s, g_r,
    i_s, i_r, k_r, d_s, d_r, u_s, u_r, w_s, w_r, q_s, q_r,
):
    prefactor, grid_count = consts
    fi, bi = lax.axis_index("freq"), lax.axis_index("band")
    zl, y = fi // 4, lax.rem(fi, 4)
    x, zh, c = bi // 4, lax.rem(bi // 2, 2), lax.rem(bi, 2)
    z = zh * 2 + zl
    me = (fi, bi)
    partner = dev(x, y, z, 1 - c)
    aligned = zl == c
    unaligned = jnp.logical_not(aligned)
    pending = []

    def send(src, dst, ss, rs, to):
        copy = pltpu.make_async_remote_copy(
            src_ref=src, dst_ref=dst, send_sem=ss, recv_sem=rs, device_id=to, device_id_type=MESH
        )
        copy.start()
        return copy

    def keep(copy):
        pending.append(copy)

    def arrived(dst, rs):
        pltpu.make_async_remote_copy(
            src_ref=dst, dst_ref=dst, send_sem=rs, recv_sem=rs, device_id=me, device_id_type=MESH
        ).wait_recv()

    def sent(src, ss):
        pltpu.make_async_remote_copy(
            src_ref=src, dst_ref=src, send_sem=ss, recv_sem=ss, device_id=me, device_id_type=MESH
        ).wait_send()

    plane = [
        (dy, dx, cc) for dy in range(4) for dx in range(4) for cc in range(2) if (dy, dx, cc) != (0, 0, 0)
    ]
    barrier = pltpu.get_barrier_semaphore()
    for dy, dx, cc in plane:
        pl.semaphore_signal(barrier, inc=1, device_id=dev(x + dx, y + dy, z, c + cc), device_id_type=MESH)
    for dz in (1, 2, 3):
        for cc in range(2):
            pl.semaphore_signal(barrier, inc=1, device_id=dev(x, y, z + dz, cc), device_id_type=MESH)
    with jax.named_scope("entry"):
        pl.semaphore_wait(barrier, len(plane) + 6)

    def lanes(block):
        return pl.ds(pl.multiple_of(block * 512, 512), 512)

    def stage(name, fn, *args):
        with jax.named_scope(name):
            fn(*args)

    def at(e):
        return wrap(x - e)

    def columns(block):
        return pl.ds(pl.multiple_of(block * 2048, 2048), 2048)

    def own_piece(h, block):
        return rho.at[:, pl.ds(16 * h, 16), columns(block)]

    def spread(h, e):
        src = own_piece(h, x) if e == 0 else R.at[h, 0, :, at(e), c]
        keep(send(src, R.at[h, 1, :, at(e), c], y_s.at[h, 0, e], y_r.at[h, 0, e], dev(x, y + 1, z, c)))
        keep(send(src, R.at[h, 2, :, at(e), c], y_s.at[h, 1, e], y_r.at[h, 1, e], dev(x, y - 1, z, c)))
        keep(send(src, R.at[h, 0, :, at(e), c], p_s.at[h, 0, e], p_r.at[h, 0, e], partner))

    def pass_on(h, e):
        for side in range(2):
            to = dev(x, y + 1 - 2 * side, z, c)
            piece = R.at[h, 1 + side, :, at(e), c]
            arrived(piece, y_r.at[h, side, e])
            part = R.at[h, 1 + side, side, at(e), c]
            keep(send(part, R.at[h, 3, side, at(e), c], f_s.at[h, side, e], f_r.at[h, side, e], to))
            keep(send(piece, piece, p_s.at[h, 1 + side, e], p_r.at[h, 1 + side, e], partner))

    def pass_far(h, e):
        for side in range(2):
            arrived(R.at[h, 3, side, at(e), c], f_r.at[h, side, e])
        piece = R.at[h, 3, :, at(e), c]
        keep(send(piece, piece, p_s.at[h, 3, e], p_r.at[h, 3, e], partner))

    def partner_done(h, pos):
        for e in ORDER:
            arrived(R.at[h, pos, :, at(e), 1 - c], p_r.at[h, pos, e])

    def from_x(h, e):
        arrived(R.at[h, 0, :, at(e), c], x_r.at[h, e])
        spread(h, e)

    my_lanes = lanes(zh * 2 + c)

    def vector_piece(q, zz, cc):
        return XF.at[pl.ds(2 * q, 2), :, :, lanes((wrap(zz) // 2) * 2 + cc)]

    def begin():
        spread(0, 0)
        for h in range(2):
            for e in (1, 3, 2):
                keep(send(own_piece(h, wrap(x + e)), R.at[h, 0, :, x, c], x_s.at[h, e], x_r.at[h, e], dev(x + e, y, z, c)))
        for k in range(2):
            for side in range(2):
                q = (k + side) % 2
                dz = 1 + 2 * side
                keep(send(xin.at[pl.ds(2 * q, 2)], vector_piece(q, z, c), v_s.at[dz, q], v_r.at[dz, c, q], dev(x, y, z + dz, zl)))
        spread(1, 0)

        @pl.when(unaligned)
        def _():
            send(xin, XF.at[:, :, :, my_lanes], v_s.at[0, 0], v_r.at[0, c, 0], partner)

        for f in range(4):
            FQ[0, f] = jnp.full((8, 128), freq[f], jnp.float32)

        lane = lax.broadcasted_iota(jnp.int32, (8, 128), 1)
        row = lax.broadcasted_iota(jnp.int32, (8, 128), 0)
        place = jnp.bitwise_and(row, 1) * 16 + jnp.bitwise_and(lane, 15)
        number = jnp.zeros((8, 128), jnp.int32)
        for i in range(32):
            number = jnp.where(place == i, idx[i], number)
        cond_no = jnp.bitwise_and(number, 127)
        val_no = jnp.right_shift(number, 7)
        zero = jnp.zeros((8, 128), jnp.float32)
        cond_pick = lax.fori_loop(0, 128, lambda j, a: jnp.where(cond_no == j, cond[j], a), zero)
        val_pick = lax.fori_loop(0, 32, lambda j, a: jnp.where(val_no == j, val[j], a), zero)
        D[x * 2 + c] = jnp.where(jnp.right_shift(lane, 4) == x * 2 + c, cond_pick - val_pick, 0.0)
        for h in range(2):
            R[h, 0, :, x, c] = rho[:, 16 * h : 16 * h + 16, columns(x)]

        @pl.when(aligned)
        def _():
            XF[:, :, :, my_lanes] = xin[...]
            FQ[1] = FQ[0]

        @pl.when(aligned)
        def _():
            send(FQ.at[0], FQ.at[1], q_s, q_r, dev(x, y, z - 1, c))

        for dy, dx, cc in plane:
            pos = (0, 1, 3, 2)[dy]
            send(D.at[x * 2 + c], D.at[pos * 8 + x * 2 + c], d_s, d_r, dev(x + dx, y + dy, z, c + cc))

    def vectors_pass():
        @pl.when(unaligned)
        def _():
            for q in range(2):
                dz = 1 + 2 * q
                for cc in range(2):
                    piece = vector_piece(q, z - dz, cc)
                    arrived(piece, v_r.at[dz, cc, q])
                    send(piece, piece, t_s.at[q, cc], v_r.at[2, cc, q], dev(x, y, z + dz, c))

    def vectors_done():
        @pl.when(aligned)
        def _():
            arrived(XF.at[:, :, :, lanes(zh * 2 + 1 - c)], v_r.at[0, 1 - c, 0])
            for q in range(2):
                for cc in range(2):
                    arrived(vector_piece(q, z + 2, cc), v_r.at[2, cc, q])

        @pl.when(unaligned)
        def _():
            for q in range(2):
                dz = 3 - 2 * q
                for cc in range(2):
                    arrived(vector_piece(q, z - dz, cc), v_r.at[dz, cc, q])

    A, FAR, B, LAST = (0, 0, 3), (0, 3, 4), (1, 0, 3), (1, 3, 4)

    def cross(h, pos):
        t = dot_nt(XF[...].reshape(512, 2048), R[h, pos].reshape(256, 2048)).reshape(4, 2, 64, 256)
        re = t[:, 0, :, 0:128] + t[:, 1, :, 128:256]
        im = t[:, 1, :, 0:128] - t[:, 0, :, 128:256]
        C32[h, :, pos, 0] = re
        C32[h, :, pos, 1] = im
        CB[h, :, pos, 0] = re.astype(jnp.bfloat16)
        CB[h, :, pos, 1] = im.astype(jnp.bfloat16)

    def cross_out(h, pos):
        for e in (1, 3, 2):
            keep(send(CB.at[h, wrap(x + e), pos], CR.at[h, e, pos], c_s.at[h, pos, e], c_r.at[h, pos, e], dev(x + e, y, z, c)))

    def scale(h, pos):
        for e in (1, 3, 2):
            arrived(CR.at[h, e, pos], c_r.at[h, pos, e])
        own = FQ[1, x][0:1, 0:1]
        total = C32[h, x, pos]
        for e in (1, 2, 3):
            total = total + CR[h, e, pos].astype(jnp.float32)
        delta = D[pos * 8]
        for k in range(1, 8):
            delta = delta + D[pos * 8 + k]
        delta = delta[h : h + 1]
        ratio = delta / (delta * delta + own * own)
        weight = (-4.0 * prefactor * ratio).astype(jnp.bfloat16).astype(jnp.float32)
        SF[h, x, pos] = (weight[None] * total).astype(jnp.bfloat16)
        C32[h, x, pos] = total
        for e in (1, 3, 2):
            keep(send(SF.at[h, x, pos], SF.at[h, x, pos], g_s.at[h, pos, e], g_r.at[h, pos, e], dev(x + e, y, z, c)))

    def project_add(group):
        h = group[0]
        for pos in range(group[1], group[2]):
            flat = C32[h, x, pos].reshape(128, 128)
            high = flat.astype(jnp.bfloat16)
            low = (flat - high.astype(jnp.float32)).astype(jnp.bfloat16)
            part = dot_nt(jnp.concatenate([high, low], axis=0), SF[h, x, pos].reshape(128, 128))
            if h == 0 and pos == 0:
                SA[...] = part
            else:
                SA[...] += part

    def gathered(group):
        h = group[0]
        for pos in range(group[1], group[2]):
            for e in (1, 3, 2):
                arrived(SF.at[h, at(e), pos], g_r.at[h, pos, e])
        for pos in range(group[1], group[2]):
            base = (pos - group[1]) * 256
            re, im = SF[h, :, pos, 0], SF[h, :, pos, 1]
            L[:, 0, :, base : base + 128] = re
            L[:, 0, :, base + 128 : base + 256] = -im
            L[:, 1, :, base : base + 128] = im
            L[:, 1, :, base + 128 : base + 256] = re

    def image_tile(group, block):
        h, some = group[0], pl.ds(group[1], group[2] - group[1])
        depth = (group[2] - group[1]) * 256
        return jnp.dot(
            L[:, :, :, 0:depth].reshape(512, depth),
            R[h, some, :, :, :, :, lanes(block)].reshape(depth, 512),
            preferred_element_type=jnp.float32,
        )

    def image(group):
        gathered(group)
        for block in range(4):
            part = image_tile(group, block)
            if group == A:
                acc[:, block * 512 : block * 512 + 512] = part
            else:
                acc[:, block * 512 : block * 512 + 512] += part

    def energies_done():
        most = D.at[pl.ds(0, 31)]
        arrived(most, d_r)
        sent(most, d_s)

        @pl.when(aligned)
        def _():
            sent(FQ.at[0], q_s)

        @pl.when(unaligned)
        def _():
            arrived(FQ.at[1], q_r)

    stage("begin", begin)
    stage("xA1", from_x, 0, 1)
    stage("xA3", from_x, 0, 3)
    stage("passA0", pass_on, 0, 0)
    stage("xA2", from_x, 0, 2)
    stage("relay", vectors_pass)
    stage("passA1", pass_on, 0, 1)
    stage("passA3", pass_on, 0, 3)
    stage("xB1", from_x, 1, 1)
    stage("xB3", from_x, 1, 3)
    stage("farA0", pass_far, 0, 0)
    stage("passA2", pass_on, 0, 2)
    stage("passB0", pass_on, 1, 0)
    stage("xB2", from_x, 1, 2)
    stage("vectors", vectors_done)
    stage("partA0", partner_done, 0, 0)
    stage("crossA0", cross, 0, 0)
    stage("outA0", cross_out, 0, 0)
    stage("farA1", pass_far, 0, 1)
    stage("partA1", partner_done, 0, 1)
    stage("crossA1", cross, 0, 1)
    stage("outA1", cross_out, 0, 1)
    stage("farA3", pass_far, 0, 3)
    stage("partA2", partner_done, 0, 2)
    stage("crossA2", cross, 0, 2)
    stage("outA2", cross_out, 0, 2)
    stage("partB0", partner_done, 1, 0)
    stage("crossB0", cross, 1, 0)
    stage("outB0", cross_out, 1, 0)
    stage("passB1", pass_on, 1, 1)
    stage("energies", energies_done)
    stage("scaleA0", scale, 0, 0)
    stage("scaleA1", scale, 0, 1)
    stage("passB3", pass_on, 1, 3)
    stage("farA2", pass_far, 0, 2)
    stage("partA3", partner_done, 0, 3)
    stage("crossA3", cross, 0, 3)
    stage("outA3", cross_out, 0, 3)
    stage("scaleA2", scale, 0, 2)
    stage("passB2", pass_on, 1, 2)
    stage("farB0", pass_far, 1, 0)
    stage("partB1", partner_done, 1, 1)
    stage("crossB1", cross, 1, 1)
    stage("outB1", cross_out, 1, 1)
    stage("scaleB0", scale, 1, 0)
    stage("farB1", pass_far, 1, 1)
    stage("partB2", partner_done, 1, 2)
    stage("crossB2", cross, 1, 2)
    stage("outB2", cross_out, 1, 2)
    stage("farB3", pass_far, 1, 3)
    stage("scaleA3", scale, 0, 3)
    stage("farB2", pass_far, 1, 2)
    stage("partB3", partner_done, 1, 3)
    stage("crossB3", cross, 1, 3)
    stage("outB3", cross_out, 1, 3)
    stage("scaleB1", scale, 1, 1)
    stage("imageA", image, A)
    stage("scaleB2", scale, 1, 2)
    stage("scaleB3", scale, 1, 3)
    stage("imageF", image, FAR)
    stage("addA", project_add, A)
    stage("addF", project_add, FAR)
    stage("addB", project_add, B)
    stage("addL", project_add, LAST)

    def project_z():
        both = SA[0:128] + SA[128:256]
        re = both[0:64, 0:64] + both[64:128, 64:128]
        im = both[0:64, 64:128] - both[64:128, 0:64]
        SZ[z] = jnp.concatenate([re, im], axis=1) / grid_count

        @pl.when(aligned)
        def _():
            send(SZ.at[z], SZ.at[z], u_s.at[0], u_r.at[2], dev(x, y, z + 2, c))

        @pl.when(unaligned)
        def _():
            for k, dz in enumerate((1, 3)):
                send(SZ.at[z], SZ.at[z], u_s.at[k], u_r.at[dz], dev(x, y, z + dz, c))

    def project_x():
        @pl.when(aligned)
        def _():
            for dz in (1, 3, 2):
                arrived(SZ.at[wrap(z - dz)], u_r.at[dz])
            SO[x] = SZ[0] + SZ[1] + SZ[2] + SZ[3]
            for e in (1, 3, 2):
                for cc in range(2):
                    send(SO.at[x], SO.at[x], w_s.at[e, cc], w_r.at[e], dev(x + e, y, z, cc))
            send(SO.at[x], SO.at[x], w_s.at[0, 0], w_r.at[0], dev(x, y, z, 1 - c))

    def project_done():
        @pl.when(unaligned)
        def _():
            arrived(SO.at[x], w_r.at[0])

        for e in (1, 3, 2):
            arrived(SO.at[at(e)], w_r.at[e])
        for f in range(4):
            both = SO[f]
            sub[f, 0] = both[:, 0:64]
            sub[f, 1] = both[:, 64:128]

    stage("project_z", project_z)
    stage("imageB", image, B)
    stage("gatheredL", gathered, LAST)

    def target(step):
        h = 1 - zh if step < 2 else zh
        cc = 1 - c if step % 2 == 0 else c
        to_z = h * 2 + c
        dz = wrap(to_z - z)
        return h * 2 + cc, cc, to_z, (dz + 1) // 2, (3 - dz) // 2

    def image_out(step):
        block, cc, to_z, slot, direct = target(step)
        total = acc[:, lanes(block)] + image_tile(LAST, block)
        half = total.astype(jnp.bfloat16).reshape(2, 2, 2, 64, 512)
        SB[step] = half

        @pl.when(unaligned)
        def _():
            acc[:, lanes(block)] = total
            send(SB.at[step, direct], RI.at[slot, direct], i_s.at[step, direct], i_r.at[slot, direct], dev(x, y, to_z, cc))

        @pl.when(aligned)
        def _():
            if step < 2:
                send(SB.at[step, 0], RC.at[0, cc], i_s.at[step, 0], k_r.at[0, cc], dev(x, y, z + 1, c))
                send(SB.at[step, 1], RC.at[1, cc], i_s.at[step, 1], k_r.at[1, cc], dev(x, y, z - 1, c))
            elif step == 2:
                send(SB.at[step], RI.at[0], i_s.at[step, 0], i_r.at[0, 0], partner)
            else:
                RI[0] = half

    def image_join(step):
        block, cc, to_z, slot, direct = target(step)
        joined = 1 - direct
        arrived(RC.at[joined, cc], k_r.at[joined, cc])
        rows = pl.ds(pl.multiple_of(joined * 256, 256), 256)
        total = acc[rows, lanes(block)].reshape(2, 2, 64, 512) + RC[joined, cc].astype(jnp.float32)
        SB[step, joined] = total.astype(jnp.bfloat16)
        send(SB.at[step, joined], RI.at[slot, joined], i_s.at[step, joined], i_r.at[slot, joined], dev(x, y, to_z, cc))

    for step in range(4):
        stage(f"out{step}", image_out, step)
    stage("project_x", project_x)

    @pl.when(unaligned)
    def _():
        for step in (0, 2, 1, 3):
            stage(f"join{step}", image_join, step)

    stage("project", project_done)

    def images_done():
        for slot in (1, 2):
            for q in range(2):
                arrived(RI.at[slot, q], i_r.at[slot, q])

        @pl.when(unaligned)
        def _():
            arrived(RI.at[0], i_r.at[0, 0])

    stage("images", images_done)

    def drain():
        for copy in pending:
            copy.wait_send()

        @pl.when(unaligned)
        def _():
            sent(xin, v_s.at[0, 0])
            for q in range(2):
                for cc in range(2):
                    sent(vector_piece(q, z - 1 - 2 * q, cc), t_s.at[q, cc])
            for step in range(4):
                for q in range(2):
                    sent(SB.at[step, q], i_s.at[step, q])
            for k in range(2):
                sent(SZ.at[z], u_s.at[k])

        @pl.when(aligned)
        def _():
            for step in range(2):
                for q in range(2):
                    sent(SB.at[step, q], i_s.at[step, q])
            sent(SB.at[2], i_s.at[2, 0])
            sent(SZ.at[z], u_s.at[0])
            for e in (1, 3, 2):
                for cc in range(2):
                    sent(SO.at[x], w_s.at[e, cc])
            sent(SO.at[x], w_s.at[0, 0])

    stage("drain", drain)


def shards(pair_density, trial_vectors, frequency, val_energy, cond_energy, pair_index):
    groups = lax.axis_size("freq")
    members = lax.axis_size("band")
    pair_count = pair_density.shape[0] * groups * members
    grid_count = trial_vectors.shape[3] * members
    prefactor = 1.0 / math.sqrt(2.0 * grid_count * pair_count)
    pieces = jnp.transpose(pair_density, (1, 0, 2))
    bf, f32 = jnp.bfloat16, jnp.float32
    vmem = pl.BlockSpec(memory_space=pltpu.VMEM)
    smem = pl.BlockSpec(memory_space=pltpu.SMEM)
    dma = pltpu.SemaphoreType.DMA
    parts, subspace = pl.pallas_call(
        functools.partial(kernel, (prefactor, grid_count)),
        name="response",
        out_shape=(
            jax.ShapeDtypeStruct((3, 2, 2, 2, 64, 512), bf),
            jax.ShapeDtypeStruct((4, 2, 64, 64), f32),
        ),
        in_specs=[vmem, vmem, smem, smem, smem, smem],
        out_specs=(vmem, vmem),
        scratch_shapes=[
            pltpu.VMEM((2, 4, 2, 4, 2, 16, 2048), bf),
            pltpu.VMEM((4, 2, 64, 2048), bf),
            pltpu.VMEM((512, 2048), f32),
            pltpu.VMEM((2, 4, 4, 2, 64, 128), f32),
            pltpu.VMEM((2, 4, 4, 2, 64, 128), bf),
            pltpu.VMEM((2, 4, 4, 2, 64, 128), bf),
            pltpu.VMEM((2, 4, 4, 2, 64, 128), bf),
            pltpu.VMEM((4, 2, 64, 768), bf),
            pltpu.VMEM((4, 2, 2, 2, 64, 512), bf),
            pltpu.VMEM((2, 2, 2, 2, 64, 512), bf),
            pltpu.VMEM((32, 8, 128), f32),
            pltpu.VMEM((4, 64, 128), f32),
            pltpu.VMEM((4, 64, 128), f32),
            pltpu.VMEM((256, 128), f32),
            pltpu.VMEM((2, 4, 8, 128), f32),
            dma((2, 4)), dma((2, 4)),
            dma((2, 2, 4)), dma((2, 2, 4)),
            dma((2, 2, 4)), dma((2, 2, 4)),
            dma((2, 4, 4)), dma((2, 4, 4)),
            dma((4, 2)), dma((4, 2, 2)), dma((2, 2)),
            dma((2, 4, 4)), dma((2, 4, 4)),
            dma((2, 4, 4)), dma((2, 4, 4)),
            dma((4, 2)), dma((4, 2)), dma((2, 2)),
            dma, dma,
            dma((2,)), dma((4,)),
            dma((4, 2)), dma((4,)),
            dma, dma,
        ],
        compiler_params=pltpu.CompilerParams(
            collective_id=0, has_side_effects=True, vmem_limit_bytes=36 * 2**20
        ),
    )(pieces, trial_vectors, pair_index, cond_energy, val_energy, frequency)
    images = parts[0].astype(f32) + parts[1].astype(f32) + parts[2].astype(f32)
    return images.reshape(4, 2, 64, 512), subspace


def solution(mesh):
    return jax.shard_map(
        shards,
        mesh=mesh,
        in_specs=(
            P(("freq", "band"), None, None),
            P("freq", None, None, "band"),
            P("freq"),
            P(),
            P(),
            P(("freq", "band")),
        ),
        out_specs=(P("freq", None, None, "band"), P("freq", None, None, None)),
        check_vma=False,
    )
```

```python
import functools
import math

import jax
import jax.numpy as jnp
from jax import lax
from jax.experimental import pallas as pl
from jax.experimental.pallas import tpu as pltpu
from jax.sharding import PartitionSpec as P

MESH = pl.DeviceIdType.MESH
ORDER = (0, 1, 3, 2)


def wrap(v, n=4):
    return lax.rem(v + n, n)


def dev(x, y, z, c):
    x, y, z, c = wrap(x), wrap(y), wrap(z), wrap(c, 2)
    return (lax.rem(z, 2) * 4 + y, x * 4 + (z // 2) * 2 + c)


def dot_nt(a, b):
    return lax.dot_general(a, b, (((1,), (1,)), ((), ())), preferred_element_type=jnp.float32)


def kernel(
    consts,
    rho, xin, idx, cond, val, freq,
    RI, sub,
    R, XF, acc, C32, CB, CR, SF, L, SB, RC, D, SZ, SO, SA, FQ,
    x_s, x_r, y_s, y_r, f_s, f_r, p_s, p_r, v_s, v_r, t_s, c_s, c_r, g_s, g_r,
    i_s, i_r, k_r, d_s, d_r, u_s, u_r, w_s, w_r, q_s, q_r,
):
    prefactor, grid_count = consts
    fi, bi = lax.axis_index("freq"), lax.axis_index("band")
    zl, y = fi // 4, lax.rem(fi, 4)
    x, zh, c = bi // 4, lax.rem(bi // 2, 2), lax.rem(bi, 2)
    z = zh * 2 + zl
    me = (fi, bi)
    partner = dev(x, y, z, 1 - c)
    aligned = zl == c
    unaligned = jnp.logical_not(aligned)
    pending = []

    def send(src, dst, ss, rs, to):
        copy = pltpu.make_async_remote_copy(
            src_ref=src, dst_ref=dst, send_sem=ss, recv_sem=rs, device_id=to, device_id_type=MESH
        )
        copy.start()
        return copy

    def keep(copy):
        pending.append(copy)

    def arrived(dst, rs):
        pltpu.make_async_remote_copy(
            src_ref=dst, dst_ref=dst, send_sem=rs, recv_sem=rs, device_id=me, device_id_type=MESH
        ).wait_recv()

    def sent(src, ss):
        pltpu.make_async_remote_copy(
            src_ref=src, dst_ref=src, send_sem=ss, recv_sem=ss, device_id=me, device_id_type=MESH
        ).wait_send()

    plane = [
        (dy, dx, cc) for dy in range(4) for dx in range(4) for cc in range(2) if (dy, dx, cc) != (0, 0, 0)
    ]
    barrier = pltpu.get_barrier_semaphore()
    for dy, dx, cc in plane:
        pl.semaphore_signal(barrier, inc=1, device_id=dev(x + dx, y + dy, z, c + cc), device_id_type=MESH)
    for dz in (1, 2, 3):
        for cc in range(2):
            pl.semaphore_signal(barrier, inc=1, device_id=dev(x, y, z + dz, cc), device_id_type=MESH)
    with jax.named_scope("entry"):
        pl.semaphore_wait(barrier, len(plane) + 6)

    def lanes(block):
        return pl.ds(pl.multiple_of(block * 512, 512), 512)

    def stage(name, fn, *args):
        with jax.named_scope(name):
            fn(*args)

    def at(e):
        return wrap(x - e)

    def columns(block):
        return pl.ds(pl.multiple_of(block * 2048, 2048), 2048)

    def own_piece(h, block):
        return rho.at[:, pl.ds(16 * h, 16), columns(block)]

    def spread(h, e):
        src = own_piece(h, x) if e == 0 else R.at[h, 0, :, at(e), c]
        keep(send(src, R.at[h, 1, :, at(e), c], y_s.at[h, 0, e], y_r.at[h, 0, e], dev(x, y + 1, z, c)))
        keep(send(src, R.at[h, 2, :, at(e), c], y_s.at[h, 1, e], y_r.at[h, 1, e], dev(x, y - 1, z, c)))
        keep(send(src, R.at[h, 0, :, at(e), c], p_s.at[h, 0, e], p_r.at[h, 0, e], partner))

    def pass_on(h, e):
        for side in range(2):
            to = dev(x, y + 1 - 2 * side, z, c)
            piece = R.at[h, 1 + side, :, at(e), c]
            arrived(piece, y_r.at[h, side, e])
            part = R.at[h, 1 + side, side, at(e), c]
            keep(send(part, R.at[h, 3, side, at(e), c], f_s.at[h, side, e], f_r.at[h, side, e], to))
            keep(send(piece, piece, p_s.at[h, 1 + side, e], p_r.at[h, 1 + side, e], partner))

    def pass_far(h, e):
        for side in range(2):
            arrived(R.at[h, 3, side, at(e), c], f_r.at[h, side, e])
        piece = R.at[h, 3, :, at(e), c]
        keep(send(piece, piece, p_s.at[h, 3, e], p_r.at[h, 3, e], partner))

    def partner_done(h, pos):
        for e in ORDER:
            arrived(R.at[h, pos, :, at(e), 1 - c], p_r.at[h, pos, e])

    def from_x(h, e):
        arrived(R.at[h, 0, :, at(e), c], x_r.at[h, e])
        spread(h, e)

    my_lanes = lanes(zh * 2 + c)

    def vector_piece(q, zz, cc):
        return XF.at[pl.ds(2 * q, 2), :, :, lanes((wrap(zz) // 2) * 2 + cc)]

    def begin():
        spread(0, 0)
        for h in range(2):
            for e in (1, 3, 2):
                keep(send(own_piece(h, wrap(x + e)), R.at[h, 0, :, x, c], x_s.at[h, e], x_r.at[h, e], dev(x + e, y, z, c)))
        for k in range(2):
            for side in range(2):
                q = (k + side) % 2
                dz = 1 + 2 * side
                keep(send(xin.at[pl.ds(2 * q, 2)], vector_piece(q, z, c), v_s.at[dz, q], v_r.at[dz, c, q], dev(x, y, z + dz, zl)))
        spread(1, 0)

        @pl.when(unaligned)
        def _():
            send(xin, XF.at[:, :, :, my_lanes], v_s.at[0, 0], v_r.at[0, c, 0], partner)

        for f in range(4):
            FQ[0, f] = jnp.full((8, 128), freq[f], jnp.float32)

        lane = lax.broadcasted_iota(jnp.int32, (8, 128), 1)
        row = lax.broadcasted_iota(jnp.int32, (8, 128), 0)
        place = jnp.bitwise_and(row, 1) * 16 + jnp.bitwise_and(lane, 15)
        number = jnp.zeros((8, 128), jnp.int32)
        for i in range(32):
            number = jnp.where(place == i, idx[i], number)
        cond_no = jnp.bitwise_and(number, 127)
        val_no = jnp.right_shift(number, 7)
        zero = jnp.zeros((8, 128), jnp.float32)
        cond_pick = lax.fori_loop(0, 128, lambda j, a: jnp.where(cond_no == j, cond[j], a), zero)
        val_pick = lax.fori_loop(0, 32, lambda j, a: jnp.where(val_no == j, val[j], a), zero)
        D[x * 2 + c] = jnp.where(jnp.right_shift(lane, 4) == x * 2 + c, cond_pick - val_pick, 0.0)
        for h in range(2):
            R[h, 0, :, x, c] = rho[:, 16 * h : 16 * h + 16, columns(x)]

        @pl.when(aligned)
        def _():
            XF[:, :, :, my_lanes] = xin[...]
            FQ[1] = FQ[0]

        @pl.when(aligned)
        def _():
            send(FQ.at[0], FQ.at[1], q_s, q_r, dev(x, y, z - 1, c))

        for dy, dx, cc in plane:
            pos = (0, 1, 3, 2)[dy]
            send(D.at[x * 2 + c], D.at[pos * 8 + x * 2 + c], d_s, d_r, dev(x + dx, y + dy, z, c + cc))

    def vectors_pass():
        @pl.when(unaligned)
        def _():
            for q in range(2):
                dz = 1 + 2 * q
                for cc in range(2):
                    piece = vector_piece(q, z - dz, cc)
                    arrived(piece, v_r.at[dz, cc, q])
                    send(piece, piece, t_s.at[q, cc], v_r.at[2, cc, q], dev(x, y, z + dz, c))

    def vectors_done():
        @pl.when(aligned)
        def _():
            arrived(XF.at[:, :, :, lanes(zh * 2 + 1 - c)], v_r.at[0, 1 - c, 0])
            for q in range(2):
                for cc in range(2):
                    arrived(vector_piece(q, z + 2, cc), v_r.at[2, cc, q])

        @pl.when(unaligned)
        def _():
            for q in range(2):
                dz = 3 - 2 * q
                for cc in range(2):
                    arrived(vector_piece(q, z - dz, cc), v_r.at[dz, cc, q])

    A, FAR, B, LAST = (0, 0, 3), (0, 3, 4), (1, 0, 2), (1, 2, 4)

    def cross(h, pos):
        t = dot_nt(XF[...].reshape(512, 2048), R[h, pos].reshape(256, 2048)).reshape(4, 2, 64, 256)
        re = t[:, 0, :, 0:128] + t[:, 1, :, 128:256]
        im = t[:, 1, :, 0:128] - t[:, 0, :, 128:256]
        C32[h, :, pos, 0] = re
        C32[h, :, pos, 1] = im
        CB[h, :, pos, 0] = re.astype(jnp.bfloat16)
        CB[h, :, pos, 1] = im.astype(jnp.bfloat16)

    def cross_out(h, pos):
        for e in (2, 1, 3):
            keep(send(CB.at[h, wrap(x + e), pos], CR.at[h, e, pos], c_s.at[h, pos, e], c_r.at[h, pos, e], dev(x + e, y, z, c)))

    def scale(h, pos):
        for e in (1, 3, 2):
            arrived(CR.at[h, e, pos], c_r.at[h, pos, e])
        own = FQ[1, x][0:1, 0:1]
        total = C32[h, x, pos]
        for e in (1, 2, 3):
            total = total + CR[h, e, pos].astype(jnp.float32)
        delta = D[pos * 8]
        for k in range(1, 8):
            delta = delta + D[pos * 8 + k]
        delta = delta[h : h + 1]
        ratio = delta / (delta * delta + own * own)
        weight = (-4.0 * prefactor * ratio).astype(jnp.bfloat16).astype(jnp.float32)
        SF[h, x, pos] = (weight[None] * total).astype(jnp.bfloat16)
        C32[h, x, pos] = total
        for e in (2, 1, 3):
            keep(send(SF.at[h, x, pos], SF.at[h, x, pos], g_s.at[h, pos, e], g_r.at[h, pos, e], dev(x + e, y, z, c)))

    def project_add(group):
        h = group[0]
        for pos in range(group[1], group[2]):
            flat = C32[h, x, pos].reshape(128, 128)
            high = flat.astype(jnp.bfloat16)
            low = (flat - high.astype(jnp.float32)).astype(jnp.bfloat16)
            part = dot_nt(jnp.concatenate([high, low], axis=0), SF[h, x, pos].reshape(128, 128))
            if h == 0 and pos == 0:
                SA[...] = part
            else:
                SA[...] += part

    def gathered(group):
        h = group[0]
        for pos in range(group[1], group[2]):
            for e in (1, 3, 2):
                arrived(SF.at[h, at(e), pos], g_r.at[h, pos, e])
        for pos in range(group[1], group[2]):
            base = (pos - group[1]) * 256
            re, im = SF[h, :, pos, 0], SF[h, :, pos, 1]
            L[:, 0, :, base : base + 128] = re
            L[:, 0, :, base + 128 : base + 256] = -im
            L[:, 1, :, base : base + 128] = im
            L[:, 1, :, base + 128 : base + 256] = re

    def image_tile(group, block):
        h, some = group[0], pl.ds(group[1], group[2] - group[1])
        depth = (group[2] - group[1]) * 256
        return jnp.dot(
            L[:, :, :, 0:depth].reshape(512, depth),
            R[h, some, :, :, :, :, lanes(block)].reshape(depth, 512),
            preferred_element_type=jnp.float32,
        )

    def image(group):
        gathered(group)
        for block in range(4):
            part = image_tile(group, block)
            if group == A:
                acc[:, block * 512 : block * 512 + 512] = part
            else:
                acc[:, block * 512 : block * 512 + 512] += part

    def energies_done():
        most = D.at[pl.ds(0, 31)]
        arrived(most, d_r)
        sent(most, d_s)

        @pl.when(aligned)
        def _():
            sent(FQ.at[0], q_s)

        @pl.when(unaligned)
        def _():
            arrived(FQ.at[1], q_r)

    stage("begin", begin)
    stage("xA1", from_x, 0, 1)
    stage("xA3", from_x, 0, 3)
    stage("passA0", pass_on, 0, 0)
    stage("xA2", from_x, 0, 2)
    stage("relay", vectors_pass)
    stage("passA1", pass_on, 0, 1)
    stage("passA3", pass_on, 0, 3)
    stage("xB1", from_x, 1, 1)
    stage("xB3", from_x, 1, 3)
    stage("farA0", pass_far, 0, 0)
    stage("passA2", pass_on, 0, 2)
    stage("passB0", pass_on, 1, 0)
    stage("xB2", from_x, 1, 2)
    stage("vectors", vectors_done)
    stage("partA0", partner_done, 0, 0)
    stage("crossA0", cross, 0, 0)
    stage("outA0", cross_out, 0, 0)
    stage("farA1", pass_far, 0, 1)
    stage("partA1", partner_done, 0, 1)
    stage("crossA1", cross, 0, 1)
    stage("outA1", cross_out, 0, 1)
    stage("farA3", pass_far, 0, 3)
    stage("partA2", partner_done, 0, 2)
    stage("crossA2", cross, 0, 2)
    stage("outA2", cross_out, 0, 2)
    stage("partB0", partner_done, 1, 0)
    stage("crossB0", cross, 1, 0)
    stage("outB0", cross_out, 1, 0)
    stage("passB1", pass_on, 1, 1)
    stage("energies", energies_done)
    stage("scaleA0", scale, 0, 0)
    stage("scaleA1", scale, 0, 1)
    stage("passB3", pass_on, 1, 3)
    stage("farA2", pass_far, 0, 2)
    stage("partA3", partner_done, 0, 3)
    stage("crossA3", cross, 0, 3)
    stage("outA3", cross_out, 0, 3)
    stage("scaleA2", scale, 0, 2)
    stage("scaleB0", scale, 1, 0)
    stage("passB2", pass_on, 1, 2)
    stage("farB0", pass_far, 1, 0)
    stage("partB1", partner_done, 1, 1)
    stage("crossB1", cross, 1, 1)
    stage("outB1", cross_out, 1, 1)
    stage("farB1", pass_far, 1, 1)
    stage("farB3", pass_far, 1, 3)
    stage("farB2", pass_far, 1, 2)
    stage("scaleA3", scale, 0, 3)
    stage("partB2", partner_done, 1, 2)
    stage("crossB2", cross, 1, 2)
    stage("outB2", cross_out, 1, 2)
    stage("partB3", partner_done, 1, 3)
    stage("crossB3", cross, 1, 3)
    stage("outB3", cross_out, 1, 3)
    stage("scaleB1", scale, 1, 1)
    stage("imageA", image, A)
    stage("scaleB2", scale, 1, 2)
    stage("scaleB3", scale, 1, 3)
    stage("imageF", image, FAR)
    stage("addA", project_add, A)
    stage("addF", project_add, FAR)
    stage("addB", project_add, B)
    stage("addL", project_add, LAST)

    def project_z():
        both = SA[0:128] + SA[128:256]
        re = both[0:64, 0:64] + both[64:128, 64:128]
        im = both[0:64, 64:128] - both[64:128, 0:64]
        SZ[z] = jnp.concatenate([re, im], axis=1) / grid_count

        @pl.when(aligned)
        def _():
            send(SZ.at[z], SZ.at[z], u_s.at[0], u_r.at[2], dev(x, y, z + 2, c))

        @pl.when(unaligned)
        def _():
            for k, dz in enumerate((1, 3)):
                send(SZ.at[z], SZ.at[z], u_s.at[k], u_r.at[dz], dev(x, y, z + dz, c))

    def project_x():
        @pl.when(aligned)
        def _():
            for dz in (1, 3, 2):
                arrived(SZ.at[wrap(z - dz)], u_r.at[dz])
            SO[x] = SZ[0] + SZ[1] + SZ[2] + SZ[3]
            for e in (1, 3, 2):
                for cc in range(2):
                    send(SO.at[x], SO.at[x], w_s.at[e, cc], w_r.at[e], dev(x + e, y, z, cc))
            send(SO.at[x], SO.at[x], w_s.at[0, 0], w_r.at[0], dev(x, y, z, 1 - c))

    def project_done():
        @pl.when(unaligned)
        def _():
            arrived(SO.at[x], w_r.at[0])

        for e in (1, 3, 2):
            arrived(SO.at[at(e)], w_r.at[e])
        for f in range(4):
            both = SO[f]
            sub[f, 0] = both[:, 0:64]
            sub[f, 1] = both[:, 64:128]

    stage("project_z", project_z)
    stage("imageB", image, B)
    stage("gatheredL", gathered, LAST)

    def target(step):
        h = 1 - zh if step < 2 else zh
        cc = 1 - c if step % 2 == 0 else c
        to_z = h * 2 + c
        dz = wrap(to_z - z)
        return h * 2 + cc, cc, to_z, (dz + 1) // 2, (3 - dz) // 2

    def image_out(step):
        block, cc, to_z, slot, direct = target(step)
        total = acc[:, lanes(block)] + image_tile(LAST, block)
        half = total.astype(jnp.bfloat16).reshape(2, 2, 2, 64, 512)
        SB[step] = half

        @pl.when(unaligned)
        def _():
            acc[:, lanes(block)] = total
            send(SB.at[step, direct], RI.at[slot, direct], i_s.at[step, direct], i_r.at[slot, direct], dev(x, y, to_z, cc))

        @pl.when(aligned)
        def _():
            if step < 2:
                send(SB.at[step, 0], RC.at[0, cc], i_s.at[step, 0], k_r.at[0, cc], dev(x, y, z + 1, c))
                send(SB.at[step, 1], RC.at[1, cc], i_s.at[step, 1], k_r.at[1, cc], dev(x, y, z - 1, c))
            elif step == 2:
                send(SB.at[step], RI.at[0], i_s.at[step, 0], i_r.at[0, 0], partner)
            else:
                RI[0] = half

    def image_join(step):
        block, cc, to_z, slot, direct = target(step)
        joined = 1 - direct
        arrived(RC.at[joined, cc], k_r.at[joined, cc])
        rows = pl.ds(pl.multiple_of(joined * 256, 256), 256)
        total = acc[rows, lanes(block)].reshape(2, 2, 64, 512) + RC[joined, cc].astype(jnp.float32)
        SB[step, joined] = total.astype(jnp.bfloat16)
        send(SB.at[step, joined], RI.at[slot, joined], i_s.at[step, joined], i_r.at[slot, joined], dev(x, y, to_z, cc))

    for step in range(4):
        stage(f"out{step}", image_out, step)
    stage("project_x", project_x)

    @pl.when(unaligned)
    def _():
        for step in (0, 2, 1, 3):
            stage(f"join{step}", image_join, step)

    stage("project", project_done)

    def images_done():
        for slot in (1, 2):
            for q in range(2):
                arrived(RI.at[slot, q], i_r.at[slot, q])

        @pl.when(unaligned)
        def _():
            arrived(RI.at[0], i_r.at[0, 0])

    stage("images", images_done)

    def drain():
        for copy in pending:
            copy.wait_send()

        @pl.when(unaligned)
        def _():
            sent(xin, v_s.at[0, 0])
            for q in range(2):
                for cc in range(2):
                    sent(vector_piece(q, z - 1 - 2 * q, cc), t_s.at[q, cc])
            for step in range(4):
                for q in range(2):
                    sent(SB.at[step, q], i_s.at[step, q])
            for k in range(2):
                sent(SZ.at[z], u_s.at[k])

        @pl.when(aligned)
        def _():
            for step in range(2):
                for q in range(2):
                    sent(SB.at[step, q], i_s.at[step, q])
            sent(SB.at[2], i_s.at[2, 0])
            sent(SZ.at[z], u_s.at[0])
            for e in (1, 3, 2):
                for cc in range(2):
                    sent(SO.at[x], w_s.at[e, cc])
            sent(SO.at[x], w_s.at[0, 0])

    stage("drain", drain)


def shards(pair_density, trial_vectors, frequency, val_energy, cond_energy, pair_index):
    groups = lax.axis_size("freq")
    members = lax.axis_size("band")
    pair_count = pair_density.shape[0] * groups * members
    grid_count = trial_vectors.shape[3] * members
    prefactor = 1.0 / math.sqrt(2.0 * grid_count * pair_count)
    pieces = jnp.transpose(pair_density, (1, 0, 2))
    bf, f32 = jnp.bfloat16, jnp.float32
    vmem = pl.BlockSpec(memory_space=pltpu.VMEM)
    smem = pl.BlockSpec(memory_space=pltpu.SMEM)
    dma = pltpu.SemaphoreType.DMA
    parts, subspace = pl.pallas_call(
        functools.partial(kernel, (prefactor, grid_count)),
        name="response",
        out_shape=(
            jax.ShapeDtypeStruct((3, 2, 2, 2, 64, 512), bf),
            jax.ShapeDtypeStruct((4, 2, 64, 64), f32),
        ),
        in_specs=[vmem, vmem, smem, smem, smem, smem],
        out_specs=(vmem, vmem),
        scratch_shapes=[
            pltpu.VMEM((2, 4, 2, 4, 2, 16, 2048), bf),
            pltpu.VMEM((4, 2, 64, 2048), bf),
            pltpu.VMEM((512, 2048), f32),
            pltpu.VMEM((2, 4, 4, 2, 64, 128), f32),
            pltpu.VMEM((2, 4, 4, 2, 64, 128), bf),
            pltpu.VMEM((2, 4, 4, 2, 64, 128), bf),
            pltpu.VMEM((2, 4, 4, 2, 64, 128), bf),
            pltpu.VMEM((4, 2, 64, 768), bf),
            pltpu.VMEM((4, 2, 2, 2, 64, 512), bf),
            pltpu.VMEM((2, 2, 2, 2, 64, 512), bf),
            pltpu.VMEM((32, 8, 128), f32),
            pltpu.VMEM((4, 64, 128), f32),
            pltpu.VMEM((4, 64, 128), f32),
            pltpu.VMEM((256, 128), f32),
            pltpu.VMEM((2, 4, 8, 128), f32),
            dma((2, 4)), dma((2, 4)),
            dma((2, 2, 4)), dma((2, 2, 4)),
            dma((2, 2, 4)), dma((2, 2, 4)),
            dma((2, 4, 4)), dma((2, 4, 4)),
            dma((4, 2)), dma((4, 2, 2)), dma((2, 2)),
            dma((2, 4, 4)), dma((2, 4, 4)),
            dma((2, 4, 4)), dma((2, 4, 4)),
            dma((4, 2)), dma((4, 2)), dma((2, 2)),
            dma, dma,
            dma((2,)), dma((4,)),
            dma((4, 2)), dma((4,)),
            dma, dma,
        ],
        compiler_params=pltpu.CompilerParams(
            collective_id=0, has_side_effects=True, vmem_limit_bytes=36 * 2**20
        ),
    )(pieces, trial_vectors, pair_index, cond_energy, val_energy, frequency)
    images = parts[0].astype(f32) + parts[1].astype(f32) + parts[2].astype(f32)
    return images.reshape(4, 2, 64, 512), subspace


def solution(mesh):
    return jax.shard_map(
        shards,
        mesh=mesh,
        in_specs=(
            P(("freq", "band"), None, None),
            P("freq", None, None, "band"),
            P("freq"),
            P(),
            P(),
            P(("freq", "band")),
        ),
        out_specs=(P("freq", None, None, "band"), P("freq", None, None, None)),
        check_vma=False,
    )
```

```python
import functools
import math

import jax
import jax.numpy as jnp
from jax import lax
from jax.experimental import pallas as pl
from jax.experimental.pallas import tpu as pltpu
from jax.sharding import PartitionSpec as P

MESH = pl.DeviceIdType.MESH
ORDER = (0, 1, 3, 2)


def wrap(v, n=4):
    return lax.rem(v + n, n)


def dev(x, y, z, c):
    x, y, z, c = wrap(x), wrap(y), wrap(z), wrap(c, 2)
    return (lax.rem(z, 2) * 4 + y, x * 4 + (z // 2) * 2 + c)


def dot_nt(a, b):
    return lax.dot_general(a, b, (((1,), (1,)), ((), ())), preferred_element_type=jnp.float32)


def kernel(
    consts,
    rho, xin, idx, cond, val, freq,
    RI, sub,
    R, XF, acc, C32, CB, CR, SF, L, SB, RC, D, SZ, SO, SA, FQ,
    x_s, x_r, y_s, y_r, f_s, f_r, p_s, p_r, v_s, v_r, t_s, c_s, c_r, g_s, g_r,
    i_s, i_r, k_r, d_s, d_r, u_s, u_r, w_s, w_r, q_s, q_r,
):
    prefactor, grid_count = consts
    fi, bi = lax.axis_index("freq"), lax.axis_index("band")
    zl, y = fi // 4, lax.rem(fi, 4)
    x, zh, c = bi // 4, lax.rem(bi // 2, 2), lax.rem(bi, 2)
    z = zh * 2 + zl
    me = (fi, bi)
    partner = dev(x, y, z, 1 - c)
    aligned = zl == c
    unaligned = jnp.logical_not(aligned)
    pending = []

    def send(src, dst, ss, rs, to):
        copy = pltpu.make_async_remote_copy(
            src_ref=src, dst_ref=dst, send_sem=ss, recv_sem=rs, device_id=to, device_id_type=MESH
        )
        copy.start()
        return copy

    def keep(copy):
        pending.append(copy)

    def arrived(dst, rs):
        pltpu.make_async_remote_copy(
            src_ref=dst, dst_ref=dst, send_sem=rs, recv_sem=rs, device_id=me, device_id_type=MESH
        ).wait_recv()

    def sent(src, ss):
        pltpu.make_async_remote_copy(
            src_ref=src, dst_ref=src, send_sem=ss, recv_sem=ss, device_id=me, device_id_type=MESH
        ).wait_send()

    lines = [dev(x + e, y, z, cc) for e in (1, 2, 3) for cc in range(2)]
    lines += [dev(x, y + dy, z, c) for dy in (1, 2, 3)]
    lines += [dev(x, y, z + dz, cc) for dz in (1, 2, 3) for cc in range(2)]
    lines.append(partner)
    barrier = pltpu.get_barrier_semaphore()
    for other in lines:
        pl.semaphore_signal(barrier, inc=1, device_id=other, device_id_type=MESH)
    with jax.named_scope("entry"):
        pl.semaphore_wait(barrier, len(lines))

    def lanes(block):
        return pl.ds(pl.multiple_of(block * 512, 512), 512)

    def stage(name, fn, *args):
        with jax.named_scope(name):
            fn(*args)

    def at(e):
        return wrap(x - e)

    def columns(block):
        return pl.ds(pl.multiple_of(block * 2048, 2048), 2048)

    def own_piece(h, block):
        return rho.at[:, pl.ds(16 * h, 16), columns(block)]

    def spread(h, e):
        src = own_piece(h, x) if e == 0 else R.at[h, 0, :, at(e), c]
        keep(send(src, R.at[h, 1, :, at(e), c], y_s.at[h, 0, e], y_r.at[h, 0, e], dev(x, y + 1, z, c)))
        keep(send(src, R.at[h, 2, :, at(e), c], y_s.at[h, 1, e], y_r.at[h, 1, e], dev(x, y - 1, z, c)))
        keep(send(src, R.at[h, 0, :, at(e), c], p_s.at[h, 0, e], p_r.at[h, 0, e], partner))

    def pass_on(h, e):
        for side in range(2):
            to = dev(x, y + 1 - 2 * side, z, c)
            piece = R.at[h, 1 + side, :, at(e), c]
            arrived(piece, y_r.at[h, side, e])
            part = R.at[h, 1 + side, side, at(e), c]
            keep(send(part, R.at[h, 3, side, at(e), c], f_s.at[h, side, e], f_r.at[h, side, e], to))
            keep(send(piece, piece, p_s.at[h, 1 + side, e], p_r.at[h, 1 + side, e], partner))

    def pass_far(h, e):
        for side in range(2):
            arrived(R.at[h, 3, side, at(e), c], f_r.at[h, side, e])
        piece = R.at[h, 3, :, at(e), c]
        keep(send(piece, piece, p_s.at[h, 3, e], p_r.at[h, 3, e], partner))

    def partner_done(h, pos):
        for e in ORDER:
            arrived(R.at[h, pos, :, at(e), 1 - c], p_r.at[h, pos, e])

    def from_x(h, e):
        arrived(R.at[h, 0, :, at(e), c], x_r.at[h, e])
        spread(h, e)

    my_lanes = lanes(zh * 2 + c)

    def vector_piece(q, zz, cc):
        return XF.at[pl.ds(2 * q, 2), :, :, lanes((wrap(zz) // 2) * 2 + cc)]

    def begin():
        spread(0, 0)
        def to_x(h):
            for e in (1, 3, 2):
                keep(send(own_piece(h, wrap(x + e)), R.at[h, 0, :, x, c], x_s.at[h, e], x_r.at[h, e], dev(x + e, y, z, c)))

        to_x(0)
        for k in range(2):
            for side in range(2):
                q = (k + side) % 2
                dz = 1 + 2 * side
                keep(send(xin.at[pl.ds(2 * q, 2)], vector_piece(q, z, c), v_s.at[dz, q], v_r.at[dz, c, q], dev(x, y, z + dz, zl)))
        spread(1, 0)

        @pl.when(unaligned)
        def _():
            send(xin, XF.at[:, :, :, my_lanes], v_s.at[0, 0], v_r.at[0, c, 0], partner)

        for f in range(4):
            FQ[0, f] = jnp.full((8, 128), freq[f], jnp.float32)

        lane = lax.broadcasted_iota(jnp.int32, (8, 128), 1)
        row = lax.broadcasted_iota(jnp.int32, (8, 128), 0)
        place = jnp.bitwise_and(row, 1) * 16 + jnp.bitwise_and(lane, 15)
        number = jnp.zeros((8, 128), jnp.int32)
        for i in range(32):
            number = jnp.where(place == i, idx[i], number)
        cond_no = jnp.bitwise_and(number, 127)
        val_no = jnp.right_shift(number, 7)
        zero = jnp.zeros((8, 128), jnp.float32)
        cond_pick = lax.fori_loop(0, 128, lambda j, a: jnp.where(cond_no == j, cond[j], a), zero)
        val_pick = lax.fori_loop(0, 32, lambda j, a: jnp.where(val_no == j, val[j], a), zero)
        D[c * 16 + x] = jnp.where(jnp.right_shift(lane, 4) == x * 2 + c, cond_pick - val_pick, 0.0)
        for h in range(2):
            R[h, 0, :, x, c] = rho[:, 16 * h : 16 * h + 16, columns(x)]

        @pl.when(aligned)
        def _():
            XF[:, :, :, my_lanes] = xin[...]
            FQ[1] = FQ[0]

        @pl.when(aligned)
        def _():
            send(FQ.at[0], FQ.at[1], q_s, q_r, dev(x, y, z - 1, c))

        for e in (1, 3, 2):
            keep(send(D.at[c * 16 + x], D.at[c * 16 + x], d_s.at[0, e], d_r.at[0, e], dev(x + e, y, z, c)))
        to_x(1)

    def energies_y():
        for e in (1, 3, 2):
            arrived(D.at[c * 16 + at(e)], d_r.at[0, e])
        row = D.at[pl.ds(c * 16, 4)]
        for dy, pos in ((1, 1), (3, 2), (2, 3)):
            keep(send(row, D.at[pl.ds(c * 16 + pos * 4, 4)], d_s.at[1, dy], d_r.at[1, dy], dev(x, y + dy, z, c)))

    def energies_core():
        for dy, pos in ((1, 1), (3, 2), (2, 3)):
            arrived(D.at[pl.ds(c * 16 + pos * 4, 4)], d_r.at[1, dy])
        keep(send(D.at[pl.ds(c * 16, 16)], D.at[pl.ds(c * 16, 16)], d_s.at[0, 0], d_r.at[0, 0], partner))

    def vectors_pass():
        @pl.when(unaligned)
        def _():
            for q in range(2):
                dz = 1 + 2 * q
                for cc in range(2):
                    piece = vector_piece(q, z - dz, cc)
                    arrived(piece, v_r.at[dz, cc, q])
                    send(piece, piece, t_s.at[q, cc], v_r.at[2, cc, q], dev(x, y, z + dz, c))

    def vectors_done():
        @pl.when(aligned)
        def _():
            arrived(XF.at[:, :, :, lanes(zh * 2 + 1 - c)], v_r.at[0, 1 - c, 0])
            for q in range(2):
                for cc in range(2):
                    arrived(vector_piece(q, z + 2, cc), v_r.at[2, cc, q])

        @pl.when(unaligned)
        def _():
            for q in range(2):
                dz = 3 - 2 * q
                for cc in range(2):
                    arrived(vector_piece(q, z - dz, cc), v_r.at[dz, cc, q])

    A, FAR, B, LAST = (0, 0, 3), (0, 3, 4), (1, 0, 2), (1, 2, 4)

    def cross(h, pos):
        t = dot_nt(XF[...].reshape(512, 2048), R[h, pos].reshape(256, 2048)).reshape(4, 2, 64, 256)
        re = t[:, 0, :, 0:128] + t[:, 1, :, 128:256]
        im = t[:, 1, :, 0:128] - t[:, 0, :, 128:256]
        C32[h, :, pos, 0] = re
        C32[h, :, pos, 1] = im
        CB[h, :, pos, 0] = re.astype(jnp.bfloat16)
        CB[h, :, pos, 1] = im.astype(jnp.bfloat16)

    def cross_out(h, pos):
        for e in (2, 1, 3):
            keep(send(CB.at[h, wrap(x + e), pos], CR.at[h, e, pos], c_s.at[h, pos, e], c_r.at[h, pos, e], dev(x + e, y, z, c)))

    def scale(h, pos):
        for e in (1, 3, 2):
            arrived(CR.at[h, e, pos], c_r.at[h, pos, e])
        own = FQ[1, x][0:1, 0:1]
        total = C32[h, x, pos]
        for e in (1, 2, 3):
            total = total + CR[h, e, pos].astype(jnp.float32)
        delta = D[pos * 4]
        for k in range(1, 8):
            delta = delta + D[(k // 4) * 16 + pos * 4 + k % 4]
        delta = delta[h : h + 1]
        ratio = delta / (delta * delta + own * own)
        weight = (-4.0 * prefactor * ratio).astype(jnp.bfloat16).astype(jnp.float32)
        SF[h, x, pos] = (weight[None] * total).astype(jnp.bfloat16)
        C32[h, x, pos] = total
        for e in (2, 1, 3):
            keep(send(SF.at[h, x, pos], SF.at[h, x, pos], g_s.at[h, pos, e], g_r.at[h, pos, e], dev(x + e, y, z, c)))

    def project_add(group):
        h = group[0]
        for pos in range(group[1], group[2]):
            flat = C32[h, x, pos].reshape(128, 128)
            high = flat.astype(jnp.bfloat16)
            low = (flat - high.astype(jnp.float32)).astype(jnp.bfloat16)
            part = dot_nt(jnp.concatenate([high, low], axis=0), SF[h, x, pos].reshape(128, 128))
            if h == 0 and pos == 0:
                SA[...] = part
            else:
                SA[...] += part

    def gathered(group):
        h = group[0]
        for pos in range(group[1], group[2]):
            for e in (1, 3, 2):
                arrived(SF.at[h, at(e), pos], g_r.at[h, pos, e])
        for pos in range(group[1], group[2]):
            base = (pos - group[1]) * 256
            re, im = SF[h, :, pos, 0], SF[h, :, pos, 1]
            L[:, 0, :, base : base + 128] = re
            L[:, 0, :, base + 128 : base + 256] = -im
            L[:, 1, :, base : base + 128] = im
            L[:, 1, :, base + 128 : base + 256] = re

    def image_tile(group, block):
        h, some = group[0], pl.ds(group[1], group[2] - group[1])
        depth = (group[2] - group[1]) * 256
        return jnp.dot(
            L[:, :, :, 0:depth].reshape(512, depth),
            R[h, some, :, :, :, :, lanes(block)].reshape(depth, 512),
            preferred_element_type=jnp.float32,
        )

    def image(group):
        gathered(group)
        for block in range(4):
            part = image_tile(group, block)
            if group == A:
                acc[:, block * 512 : block * 512 + 512] = part
            else:
                acc[:, block * 512 : block * 512 + 512] += part

    def energies_done():
        arrived(D.at[pl.ds((1 - c) * 16, 16)], d_r.at[0, 0])

        @pl.when(aligned)
        def _():
            sent(FQ.at[0], q_s)

        @pl.when(unaligned)
        def _():
            arrived(FQ.at[1], q_r)

    stage("begin", begin)
    stage("xA1", from_x, 0, 1)
    stage("xA3", from_x, 0, 3)
    stage("passA0", pass_on, 0, 0)
    stage("xA2", from_x, 0, 2)
    stage("relay", vectors_pass)
    stage("energies_y", energies_y)
    stage("passA1", pass_on, 0, 1)
    stage("passA3", pass_on, 0, 3)
    stage("xB1", from_x, 1, 1)
    stage("xB3", from_x, 1, 3)
    stage("farA0", pass_far, 0, 0)
    stage("passA2", pass_on, 0, 2)
    stage("passB0", pass_on, 1, 0)
    stage("xB2", from_x, 1, 2)
    stage("energies_core", energies_core)
    stage("vectors", vectors_done)
    stage("partA0", partner_done, 0, 0)
    stage("crossA0", cross, 0, 0)
    stage("outA0", cross_out, 0, 0)
    stage("farA1", pass_far, 0, 1)
    stage("partA1", partner_done, 0, 1)
    stage("crossA1", cross, 0, 1)
    stage("outA1", cross_out, 0, 1)
    stage("farA3", pass_far, 0, 3)
    stage("partA2", partner_done, 0, 2)
    stage("crossA2", cross, 0, 2)
    stage("outA2", cross_out, 0, 2)
    stage("partB0", partner_done, 1, 0)
    stage("crossB0", cross, 1, 0)
    stage("outB0", cross_out, 1, 0)
    stage("passB1", pass_on, 1, 1)
    stage("energies", energies_done)
    stage("scaleA0", scale, 0, 0)
    stage("scaleA1", scale, 0, 1)
    stage("passB3", pass_on, 1, 3)
    stage("farA2", pass_far, 0, 2)
    stage("partA3", partner_done, 0, 3)
    stage("crossA3", cross, 0, 3)
    stage("outA3", cross_out, 0, 3)
    stage("scaleA2", scale, 0, 2)
    stage("scaleB0", scale, 1, 0)
    stage("passB2", pass_on, 1, 2)
    stage("farB0", pass_far, 1, 0)
    stage("partB1", partner_done, 1, 1)
    stage("crossB1", cross, 1, 1)
    stage("outB1", cross_out, 1, 1)
    stage("farB1", pass_far, 1, 1)
    stage("farB3", pass_far, 1, 3)
    stage("farB2", pass_far, 1, 2)
    stage("scaleA3", scale, 0, 3)
    stage("partB2", partner_done, 1, 2)
    stage("crossB2", cross, 1, 2)
    stage("outB2", cross_out, 1, 2)
    stage("partB3", partner_done, 1, 3)
    stage("crossB3", cross, 1, 3)
    stage("outB3", cross_out, 1, 3)
    stage("scaleB1", scale, 1, 1)
    stage("imageA", image, A)
    stage("scaleB2", scale, 1, 2)
    stage("scaleB3", scale, 1, 3)
    stage("imageF", image, FAR)
    stage("addA", project_add, A)
    stage("addF", project_add, FAR)
    stage("addB", project_add, B)
    stage("addL", project_add, LAST)

    def project_z():
        both = SA[0:128] + SA[128:256]
        re = both[0:64, 0:64] + both[64:128, 64:128]
        im = both[0:64, 64:128] - both[64:128, 0:64]
        SZ[z] = jnp.concatenate([re, im], axis=1) / grid_count

        @pl.when(aligned)
        def _():
            send(SZ.at[z], SZ.at[z], u_s.at[0], u_r.at[2], dev(x, y, z + 2, c))

        @pl.when(unaligned)
        def _():
            for k, dz in enumerate((1, 3)):
                send(SZ.at[z], SZ.at[z], u_s.at[k], u_r.at[dz], dev(x, y, z + dz, c))

    def project_x():
        @pl.when(aligned)
        def _():
            for dz in (1, 3, 2):
                arrived(SZ.at[wrap(z - dz)], u_r.at[dz])
            SO[x] = SZ[0] + SZ[1] + SZ[2] + SZ[3]
            for e in (1, 3, 2):
                for cc in range(2):
                    send(SO.at[x], SO.at[x], w_s.at[e, cc], w_r.at[e], dev(x + e, y, z, cc))
            send(SO.at[x], SO.at[x], w_s.at[0, 0], w_r.at[0], dev(x, y, z, 1 - c))

    def project_done():
        @pl.when(unaligned)
        def _():
            arrived(SO.at[x], w_r.at[0])

        for e in (1, 3, 2):
            arrived(SO.at[at(e)], w_r.at[e])
        for f in range(4):
            both = SO[f]
            sub[f, 0] = both[:, 0:64]
            sub[f, 1] = both[:, 64:128]

    stage("project_z", project_z)
    stage("imageB", image, B)
    stage("gatheredL", gathered, LAST)

    def target(step):
        h = 1 - zh if step < 2 else zh
        cc = 1 - c if step % 2 == 0 else c
        to_z = h * 2 + c
        dz = wrap(to_z - z)
        return h * 2 + cc, cc, to_z, (dz + 1) // 2, (3 - dz) // 2

    def image_out(step):
        block, cc, to_z, slot, direct = target(step)
        total = acc[:, lanes(block)] + image_tile(LAST, block)
        half = total.astype(jnp.bfloat16).reshape(2, 2, 2, 64, 512)
        SB[step] = half

        @pl.when(unaligned)
        def _():
            acc[:, lanes(block)] = total
            send(SB.at[step, direct], RI.at[slot, direct], i_s.at[step, direct], i_r.at[slot, direct], dev(x, y, to_z, cc))

        @pl.when(aligned)
        def _():
            if step < 2:
                send(SB.at[step, 0], RC.at[0, cc], i_s.at[step, 0], k_r.at[0, cc], dev(x, y, z + 1, c))
                send(SB.at[step, 1], RC.at[1, cc], i_s.at[step, 1], k_r.at[1, cc], dev(x, y, z - 1, c))
            elif step == 2:
                send(SB.at[step], RI.at[0], i_s.at[step, 0], i_r.at[0, 0], partner)
            else:
                RI[0] = half

    def image_join(step):
        block, cc, to_z, slot, direct = target(step)
        joined = 1 - direct
        arrived(RC.at[joined, cc], k_r.at[joined, cc])
        rows = pl.ds(pl.multiple_of(joined * 256, 256), 256)
        total = acc[rows, lanes(block)].reshape(2, 2, 64, 512) + RC[joined, cc].astype(jnp.float32)
        SB[step, joined] = total.astype(jnp.bfloat16)
        send(SB.at[step, joined], RI.at[slot, joined], i_s.at[step, joined], i_r.at[slot, joined], dev(x, y, to_z, cc))

    for step in range(4):
        stage(f"out{step}", image_out, step)
    stage("project_x", project_x)

    @pl.when(unaligned)
    def _():
        for step in (0, 2, 1, 3):
            stage(f"join{step}", image_join, step)

    stage("project", project_done)

    def images_done():
        for slot in (1, 2):
            for q in range(2):
                arrived(RI.at[slot, q], i_r.at[slot, q])

        @pl.when(unaligned)
        def _():
            arrived(RI.at[0], i_r.at[0, 0])

    stage("images", images_done)

    def drain():
        for copy in pending:
            copy.wait_send()

        @pl.when(unaligned)
        def _():
            sent(xin, v_s.at[0, 0])
            for q in range(2):
                for cc in range(2):
                    sent(vector_piece(q, z - 1 - 2 * q, cc), t_s.at[q, cc])
            for step in range(4):
                for q in range(2):
                    sent(SB.at[step, q], i_s.at[step, q])
            for k in range(2):
                sent(SZ.at[z], u_s.at[k])

        @pl.when(aligned)
        def _():
            for step in range(2):
                for q in range(2):
                    sent(SB.at[step, q], i_s.at[step, q])
            sent(SB.at[2], i_s.at[2, 0])
            sent(SZ.at[z], u_s.at[0])
            for e in (1, 3, 2):
                for cc in range(2):
                    sent(SO.at[x], w_s.at[e, cc])
            sent(SO.at[x], w_s.at[0, 0])

    stage("drain", drain)


def shards(pair_density, trial_vectors, frequency, val_energy, cond_energy, pair_index):
    groups = lax.axis_size("freq")
    members = lax.axis_size("band")
    pair_count = pair_density.shape[0] * groups * members
    grid_count = trial_vectors.shape[3] * members
    prefactor = 1.0 / math.sqrt(2.0 * grid_count * pair_count)
    pieces = jnp.transpose(pair_density, (1, 0, 2))
    bf, f32 = jnp.bfloat16, jnp.float32
    vmem = pl.BlockSpec(memory_space=pltpu.VMEM)
    smem = pl.BlockSpec(memory_space=pltpu.SMEM)
    dma = pltpu.SemaphoreType.DMA
    parts, subspace = pl.pallas_call(
        functools.partial(kernel, (prefactor, grid_count)),
        name="response",
        out_shape=(
            jax.ShapeDtypeStruct((3, 2, 2, 2, 64, 512), bf),
            jax.ShapeDtypeStruct((4, 2, 64, 64), f32),
        ),
        in_specs=[vmem, vmem, smem, smem, smem, smem],
        out_specs=(vmem, vmem),
        scratch_shapes=[
            pltpu.VMEM((2, 4, 2, 4, 2, 16, 2048), bf),
            pltpu.VMEM((4, 2, 64, 2048), bf),
            pltpu.VMEM((512, 2048), f32),
            pltpu.VMEM((2, 4, 4, 2, 64, 128), f32),
            pltpu.VMEM((2, 4, 4, 2, 64, 128), bf),
            pltpu.VMEM((2, 4, 4, 2, 64, 128), bf),
            pltpu.VMEM((2, 4, 4, 2, 64, 128), bf),
            pltpu.VMEM((4, 2, 64, 768), bf),
            pltpu.VMEM((4, 2, 2, 2, 64, 512), bf),
            pltpu.VMEM((2, 2, 2, 2, 64, 512), bf),
            pltpu.VMEM((32, 8, 128), f32),
            pltpu.VMEM((4, 64, 128), f32),
            pltpu.VMEM((4, 64, 128), f32),
            pltpu.VMEM((256, 128), f32),
            pltpu.VMEM((2, 4, 8, 128), f32),
            dma((2, 4)), dma((2, 4)),
            dma((2, 2, 4)), dma((2, 2, 4)),
            dma((2, 2, 4)), dma((2, 2, 4)),
            dma((2, 4, 4)), dma((2, 4, 4)),
            dma((4, 2)), dma((4, 2, 2)), dma((2, 2)),
            dma((2, 4, 4)), dma((2, 4, 4)),
            dma((2, 4, 4)), dma((2, 4, 4)),
            dma((4, 2)), dma((4, 2)), dma((2, 2)),
            dma((2, 4)), dma((2, 4)),
            dma((2,)), dma((4,)),
            dma((4, 2)), dma((4,)),
            dma, dma,
        ],
        compiler_params=pltpu.CompilerParams(
            collective_id=0, has_side_effects=True, vmem_limit_bytes=36 * 2**20
        ),
    )(pieces, trial_vectors, pair_index, cond_energy, val_energy, frequency)
    images = parts[0].astype(f32) + parts[1].astype(f32) + parts[2].astype(f32)
    return images.reshape(4, 2, 64, 512), subspace


def solution(mesh):
    return jax.shard_map(
        shards,
        mesh=mesh,
        in_specs=(
            P(("freq", "band"), None, None),
            P("freq", None, None, "band"),
            P("freq"),
            P(),
            P(),
            P(("freq", "band")),
        ),
        out_specs=(P("freq", None, None, "band"), P("freq", None, None, None)),
        check_vma=False,
    )
```

```python
import functools
import math

import jax
import jax.numpy as jnp
from jax import lax
from jax.experimental import pallas as pl
from jax.experimental.pallas import tpu as pltpu
from jax.sharding import PartitionSpec as P

MESH = pl.DeviceIdType.MESH
ORDER = (0, 1, 3, 2)


def wrap(v, n=4):
    return lax.rem(v + n, n)


def dev(x, y, z, c):
    x, y, z, c = wrap(x), wrap(y), wrap(z), wrap(c, 2)
    return (lax.rem(z, 2) * 4 + y, x * 4 + (z // 2) * 2 + c)


def dot_nt(a, b):
    return lax.dot_general(a, b, (((1,), (1,)), ((), ())), preferred_element_type=jnp.float32)


def kernel(
    consts,
    rho, xin, idx, cond, val, freq,
    RI, sub,
    R, XF, acc, C32, CB, CR, SF, L, SB, RC, D, SZ, SO, SA, FQ,
    x_s, x_r, y_s, y_r, f_s, f_r, p_s, p_r, v_s, v_r, t_s, c_s, c_r, g_s, g_r,
    i_s, i_r, k_r, d_s, d_r, u_s, u_r, w_s, w_r, q_s, q_r,
):
    prefactor, grid_count = consts
    fi, bi = lax.axis_index("freq"), lax.axis_index("band")
    zl, y = fi // 4, lax.rem(fi, 4)
    x, zh, c = bi // 4, lax.rem(bi // 2, 2), lax.rem(bi, 2)
    z = zh * 2 + zl
    me = (fi, bi)
    partner = dev(x, y, z, 1 - c)
    aligned = zl == c
    unaligned = jnp.logical_not(aligned)
    pending = []

    def send(src, dst, ss, rs, to):
        copy = pltpu.make_async_remote_copy(
            src_ref=src, dst_ref=dst, send_sem=ss, recv_sem=rs, device_id=to, device_id_type=MESH
        )
        copy.start()
        return copy

    def keep(copy):
        pending.append(copy)

    def arrived(dst, rs):
        pltpu.make_async_remote_copy(
            src_ref=dst, dst_ref=dst, send_sem=rs, recv_sem=rs, device_id=me, device_id_type=MESH
        ).wait_recv()

    def sent(src, ss):
        pltpu.make_async_remote_copy(
            src_ref=src, dst_ref=src, send_sem=ss, recv_sem=ss, device_id=me, device_id_type=MESH
        ).wait_send()

    lines = [dev(x + e, y, z, cc) for e in (1, 2, 3) for cc in range(2)]
    lines += [dev(x, y + dy, z, c) for dy in (1, 2, 3)]
    lines += [dev(x, y, z + dz, cc) for dz in (1, 2, 3) for cc in range(2)]
    lines.append(partner)
    barrier = pltpu.get_barrier_semaphore()
    for other in lines:
        pl.semaphore_signal(barrier, inc=1, device_id=other, device_id_type=MESH)
    with jax.named_scope("entry"):
        pl.semaphore_wait(barrier, len(lines))

    def lanes(block):
        return pl.ds(pl.multiple_of(block * 512, 512), 512)

    def stage(name, fn, *args):
        with jax.named_scope(name):
            fn(*args)

    def at(e):
        return wrap(x - e)

    def columns(block):
        return pl.ds(pl.multiple_of(block * 2048, 2048), 2048)

    def own_piece(h, block):
        return rho.at[:, pl.ds(16 * h, 16), columns(block)]

    def spread(h, e):
        src = own_piece(h, x) if e == 0 else R.at[h, 0, :, at(e), c]
        keep(send(src, R.at[h, 1, :, at(e), c], y_s.at[h, 0, e], y_r.at[h, 0, e], dev(x, y + 1, z, c)))
        keep(send(src, R.at[h, 2, :, at(e), c], y_s.at[h, 1, e], y_r.at[h, 1, e], dev(x, y - 1, z, c)))
        keep(send(src, R.at[h, 0, :, at(e), c], p_s.at[h, 0, e], p_r.at[h, 0, e], partner))

    def pass_on(h, e):
        for side in range(2):
            to = dev(x, y + 1 - 2 * side, z, c)
            piece = R.at[h, 1 + side, :, at(e), c]
            arrived(piece, y_r.at[h, side, e])
            part = R.at[h, 1 + side, side, at(e), c]
            keep(send(part, R.at[h, 3, side, at(e), c], f_s.at[h, side, e], f_r.at[h, side, e], to))
            keep(send(piece, piece, p_s.at[h, 1 + side, e], p_r.at[h, 1 + side, e], partner))

    def pass_far(h, e):
        for side in range(2):
            arrived(R.at[h, 3, side, at(e), c], f_r.at[h, side, e])
        piece = R.at[h, 3, :, at(e), c]
        keep(send(piece, piece, p_s.at[h, 3, e], p_r.at[h, 3, e], partner))

    def partner_done(h, pos):
        for e in ORDER:
            arrived(R.at[h, pos, :, at(e), 1 - c], p_r.at[h, pos, e])

    def from_x(h, e):
        arrived(R.at[h, 0, :, at(e), c], x_r.at[h, e])
        spread(h, e)

    my_lanes = lanes(zh * 2 + c)

    def vector_piece(q, zz, cc):
        return XF.at[pl.ds(2 * q, 2), :, :, lanes((wrap(zz) // 2) * 2 + cc)]

    def begin():
        spread(0, 0)
        def to_x(h):
            for e in (1, 3, 2):
                keep(send(own_piece(h, wrap(x + e)), R.at[h, 0, :, x, c], x_s.at[h, e], x_r.at[h, e], dev(x + e, y, z, c)))

        to_x(0)
        for k in range(2):
            for side in range(2):
                q = (k + side) % 2
                dz = 1 + 2 * side
                keep(send(xin.at[pl.ds(2 * q, 2)], vector_piece(q, z, c), v_s.at[dz, q], v_r.at[dz, c, q], dev(x, y, z + dz, zl)))
        spread(1, 0)

        @pl.when(unaligned)
        def _():
            send(xin, XF.at[:, :, :, my_lanes], v_s.at[0, 0], v_r.at[0, c, 0], partner)

        for f in range(4):
            FQ[0, f] = jnp.full((8, 128), freq[f], jnp.float32)

        lane = lax.broadcasted_iota(jnp.int32, (8, 128), 1)
        row = lax.broadcasted_iota(jnp.int32, (8, 128), 0)
        place = jnp.bitwise_and(row, 1) * 16 + jnp.bitwise_and(lane, 15)
        number = jnp.zeros((8, 128), jnp.int32)
        for i in range(32):
            number = jnp.where(place == i, idx[i], number)
        cond_no = jnp.bitwise_and(number, 127)
        val_no = jnp.right_shift(number, 7)
        zero = jnp.zeros((8, 128), jnp.float32)
        cond_pick = lax.fori_loop(0, 128, lambda j, a: jnp.where(cond_no == j, cond[j], a), zero)
        val_pick = lax.fori_loop(0, 32, lambda j, a: jnp.where(val_no == j, val[j], a), zero)
        D[c * 16 + x] = jnp.where(jnp.right_shift(lane, 4) == x * 2 + c, cond_pick - val_pick, 0.0)
        for h in range(2):
            R[h, 0, :, x, c] = rho[:, 16 * h : 16 * h + 16, columns(x)]

        @pl.when(aligned)
        def _():
            XF[:, :, :, my_lanes] = xin[...]
            FQ[1] = FQ[0]

        @pl.when(aligned)
        def _():
            send(FQ.at[0], FQ.at[1], q_s, q_r, dev(x, y, z - 1, c))

        for e in (1, 3, 2):
            keep(send(D.at[c * 16 + x], D.at[c * 16 + x], d_s.at[0, e], d_r.at[0, e], dev(x + e, y, z, c)))
        to_x(1)

    def energies_y():
        for e in (1, 3, 2):
            arrived(D.at[c * 16 + at(e)], d_r.at[0, e])
        row = D.at[pl.ds(c * 16, 4)]
        for dy, pos in ((1, 1), (3, 2), (2, 3)):
            keep(send(row, D.at[pl.ds(c * 16 + pos * 4, 4)], d_s.at[1, dy], d_r.at[1, dy], dev(x, y + dy, z, c)))

    def energies_core():
        for dy, pos in ((1, 1), (3, 2), (2, 3)):
            arrived(D.at[pl.ds(c * 16 + pos * 4, 4)], d_r.at[1, dy])
        keep(send(D.at[pl.ds(c * 16, 16)], D.at[pl.ds(c * 16, 16)], d_s.at[0, 0], d_r.at[0, 0], partner))

    def vectors_pass():
        @pl.when(unaligned)
        def _():
            for q in range(2):
                dz = 1 + 2 * q
                for cc in range(2):
                    piece = vector_piece(q, z - dz, cc)
                    arrived(piece, v_r.at[dz, cc, q])
                    send(piece, piece, t_s.at[q, cc], v_r.at[2, cc, q], dev(x, y, z + dz, c))

    def vectors_done():
        @pl.when(aligned)
        def _():
            arrived(XF.at[:, :, :, lanes(zh * 2 + 1 - c)], v_r.at[0, 1 - c, 0])
            for q in range(2):
                for cc in range(2):
                    arrived(vector_piece(q, z + 2, cc), v_r.at[2, cc, q])

        @pl.when(unaligned)
        def _():
            for q in range(2):
                dz = 3 - 2 * q
                for cc in range(2):
                    arrived(vector_piece(q, z - dz, cc), v_r.at[dz, cc, q])

    A, FAR, B, LAST = (0, 0, 3), (0, 3, 4), (1, 0, 2), (1, 2, 4)

    def cross(h, pos):
        t = dot_nt(XF[...].reshape(512, 2048), R[h, pos].reshape(256, 2048)).reshape(4, 2, 64, 256)
        re = t[:, 0, :, 0:128] + t[:, 1, :, 128:256]
        im = t[:, 1, :, 0:128] - t[:, 0, :, 128:256]
        C32[h, :, pos, 0] = re
        C32[h, :, pos, 1] = im
        CB[h, :, pos, 0] = re.astype(jnp.bfloat16)
        CB[h, :, pos, 1] = im.astype(jnp.bfloat16)

    def cross_out(h, pos):
        for e in (2, 1, 3):
            keep(send(CB.at[h, wrap(x + e), pos], CR.at[h, e, pos], c_s.at[h, pos, e], c_r.at[h, pos, e], dev(x + e, y, z, c)))

    def scale(h, pos):
        for e in (1, 3, 2):
            arrived(CR.at[h, e, pos], c_r.at[h, pos, e])
        own = FQ[1, x][0:1, 0:1]
        total = C32[h, x, pos]
        for e in (1, 2, 3):
            total = total + CR[h, e, pos].astype(jnp.float32)
        delta = D[pos * 4]
        for k in range(1, 8):
            delta = delta + D[(k // 4) * 16 + pos * 4 + k % 4]
        delta = delta[h : h + 1]
        ratio = delta / (delta * delta + own * own)
        weight = (-4.0 * prefactor * ratio).astype(jnp.bfloat16).astype(jnp.float32)
        SF[h, x, pos] = (weight[None] * total).astype(jnp.bfloat16)
        C32[h, x, pos] = total
        for e in (2, 1, 3):
            keep(send(SF.at[h, x, pos], SF.at[h, x, pos], g_s.at[h, pos, e], g_r.at[h, pos, e], dev(x + e, y, z, c)))

    def project_add(group):
        h = group[0]
        for pos in range(group[1], group[2]):
            flat = C32[h, x, pos].reshape(128, 128)
            high = flat.astype(jnp.bfloat16)
            low = (flat - high.astype(jnp.float32)).astype(jnp.bfloat16)
            part = dot_nt(jnp.concatenate([high, low], axis=0), SF[h, x, pos].reshape(128, 128))
            if h == 0 and pos == 0:
                SA[...] = part
            else:
                SA[...] += part

    def gathered(group):
        h = group[0]
        for pos in range(group[1], group[2]):
            for e in (1, 3, 2):
                arrived(SF.at[h, at(e), pos], g_r.at[h, pos, e])
        for pos in range(group[1], group[2]):
            base = (pos - group[1]) * 256
            re, im = SF[h, :, pos, 0], SF[h, :, pos, 1]
            L[:, 0, :, base : base + 128] = re
            L[:, 0, :, base + 128 : base + 256] = -im
            L[:, 1, :, base : base + 128] = im
            L[:, 1, :, base + 128 : base + 256] = re

    def image_tile(group, block):
        h, some = group[0], pl.ds(group[1], group[2] - group[1])
        depth = (group[2] - group[1]) * 256
        return jnp.dot(
            L[:, :, :, 0:depth].reshape(512, depth),
            R[h, some, :, :, :, :, lanes(block)].reshape(depth, 512),
            preferred_element_type=jnp.float32,
        )

    def image(group):
        gathered(group)
        for block in range(4):
            part = image_tile(group, block)
            if group == A:
                acc[:, block * 512 : block * 512 + 512] = part
            else:
                acc[:, block * 512 : block * 512 + 512] += part

    def energies_done():
        arrived(D.at[pl.ds((1 - c) * 16, 16)], d_r.at[0, 0])

        @pl.when(aligned)
        def _():
            sent(FQ.at[0], q_s)

        @pl.when(unaligned)
        def _():
            arrived(FQ.at[1], q_r)

    stage("begin", begin)
    stage("xA1", from_x, 0, 1)
    stage("xA3", from_x, 0, 3)
    stage("passA0", pass_on, 0, 0)
    stage("xA2", from_x, 0, 2)
    stage("relay", vectors_pass)
    stage("energies_y", energies_y)
    stage("passA1", pass_on, 0, 1)
    stage("passA3", pass_on, 0, 3)
    stage("xB1", from_x, 1, 1)
    stage("xB3", from_x, 1, 3)
    stage("farA0", pass_far, 0, 0)
    stage("passA2", pass_on, 0, 2)
    stage("passB0", pass_on, 1, 0)
    stage("xB2", from_x, 1, 2)
    stage("energies_core", energies_core)
    stage("vectors", vectors_done)
    stage("partA0", partner_done, 0, 0)
    stage("crossA0", cross, 0, 0)
    stage("outA0", cross_out, 0, 0)
    stage("farA1", pass_far, 0, 1)
    stage("partA1", partner_done, 0, 1)
    stage("crossA1", cross, 0, 1)
    stage("outA1", cross_out, 0, 1)
    stage("farA3", pass_far, 0, 3)
    stage("partA2", partner_done, 0, 2)
    stage("crossA2", cross, 0, 2)
    stage("outA2", cross_out, 0, 2)
    stage("partB0", partner_done, 1, 0)
    stage("crossB0", cross, 1, 0)
    stage("outB0", cross_out, 1, 0)
    stage("passB1", pass_on, 1, 1)
    stage("energies", energies_done)
    stage("scaleA0", scale, 0, 0)
    stage("scaleA1", scale, 0, 1)
    stage("passB3", pass_on, 1, 3)
    stage("farA2", pass_far, 0, 2)
    stage("partA3", partner_done, 0, 3)
    stage("crossA3", cross, 0, 3)
    stage("outA3", cross_out, 0, 3)
    stage("scaleA2", scale, 0, 2)
    stage("scaleB0", scale, 1, 0)
    stage("passB2", pass_on, 1, 2)
    stage("farB0", pass_far, 1, 0)
    stage("partB1", partner_done, 1, 1)
    stage("crossB1", cross, 1, 1)
    stage("outB1", cross_out, 1, 1)
    stage("farB1", pass_far, 1, 1)
    stage("partB2", partner_done, 1, 2)
    stage("crossB2", cross, 1, 2)
    stage("outB2", cross_out, 1, 2)
    stage("farB3", pass_far, 1, 3)
    stage("farB2", pass_far, 1, 2)
    stage("scaleA3", scale, 0, 3)
    stage("partB3", partner_done, 1, 3)
    stage("crossB3", cross, 1, 3)
    stage("outB3", cross_out, 1, 3)
    stage("scaleB1", scale, 1, 1)
    stage("imageA", image, A)
    stage("scaleB2", scale, 1, 2)
    stage("scaleB3", scale, 1, 3)
    stage("imageF", image, FAR)
    stage("addA", project_add, A)
    stage("addF", project_add, FAR)
    stage("addB", project_add, B)
    stage("addL", project_add, LAST)

    def project_z():
        both = SA[0:128] + SA[128:256]
        re = both[0:64, 0:64] + both[64:128, 64:128]
        im = both[0:64, 64:128] - both[64:128, 0:64]
        SZ[z] = jnp.concatenate([re, im], axis=1) / grid_count

        @pl.when(aligned)
        def _():
            send(SZ.at[z], SZ.at[z], u_s.at[0], u_r.at[2], dev(x, y, z + 2, c))

        @pl.when(unaligned)
        def _():
            for k, dz in enumerate((1, 3)):
                send(SZ.at[z], SZ.at[z], u_s.at[k], u_r.at[dz], dev(x, y, z + dz, c))

    def project_x():
        @pl.when(aligned)
        def _():
            for dz in (1, 3, 2):
                arrived(SZ.at[wrap(z - dz)], u_r.at[dz])
            SO[x] = SZ[0] + SZ[1] + SZ[2] + SZ[3]
            for e in (1, 3, 2):
                for cc in range(2):
                    send(SO.at[x], SO.at[x], w_s.at[e, cc], w_r.at[e], dev(x + e, y, z, cc))
            send(SO.at[x], SO.at[x], w_s.at[0, 0], w_r.at[0], dev(x, y, z, 1 - c))

    def project_done():
        @pl.when(unaligned)
        def _():
            arrived(SO.at[x], w_r.at[0])

        for e in (1, 3, 2):
            arrived(SO.at[at(e)], w_r.at[e])
        for f in range(4):
            both = SO[f]
            sub[f, 0] = both[:, 0:64]
            sub[f, 1] = both[:, 64:128]

    stage("project_z", project_z)
    stage("imageB", image, B)
    stage("gatheredL", gathered, LAST)

    def target(step):
        h = 1 - zh if step < 2 else zh
        cc = 1 - c if step % 2 == 0 else c
        to_z = h * 2 + c
        dz = wrap(to_z - z)
        return h * 2 + cc, cc, to_z, (dz + 1) // 2, (3 - dz) // 2

    def image_out(step):
        block, cc, to_z, slot, direct = target(step)
        total = acc[:, lanes(block)] + image_tile(LAST, block)
        half = total.astype(jnp.bfloat16).reshape(2, 2, 2, 64, 512)
        SB[step] = half

        @pl.when(unaligned)
        def _():
            acc[:, lanes(block)] = total
            send(SB.at[step, direct], RI.at[slot, direct], i_s.at[step, direct], i_r.at[slot, direct], dev(x, y, to_z, cc))

        @pl.when(aligned)
        def _():
            if step < 2:
                send(SB.at[step, 0], RC.at[0, cc], i_s.at[step, 0], k_r.at[0, cc], dev(x, y, z + 1, c))
                send(SB.at[step, 1], RC.at[1, cc], i_s.at[step, 1], k_r.at[1, cc], dev(x, y, z - 1, c))
            elif step == 2:
                send(SB.at[step], RI.at[0], i_s.at[step, 0], i_r.at[0, 0], partner)
            else:
                RI[0] = half

    def image_join(step):
        block, cc, to_z, slot, direct = target(step)
        joined = 1 - direct
        arrived(RC.at[joined, cc], k_r.at[joined, cc])
        rows = pl.ds(pl.multiple_of(joined * 256, 256), 256)
        total = acc[rows, lanes(block)].reshape(2, 2, 64, 512) + RC[joined, cc].astype(jnp.float32)
        SB[step, joined] = total.astype(jnp.bfloat16)
        send(SB.at[step, joined], RI.at[slot, joined], i_s.at[step, joined], i_r.at[slot, joined], dev(x, y, to_z, cc))

    for step in range(4):
        stage(f"out{step}", image_out, step)
    stage("project_x", project_x)

    @pl.when(unaligned)
    def _():
        for step in (0, 2, 1, 3):
            stage(f"join{step}", image_join, step)

    stage("project", project_done)

    def images_done():
        for slot in (1, 2):
            for q in range(2):
                arrived(RI.at[slot, q], i_r.at[slot, q])

        @pl.when(unaligned)
        def _():
            arrived(RI.at[0], i_r.at[0, 0])

    stage("images", images_done)

    def drain():
        for copy in pending:
            copy.wait_send()

        @pl.when(unaligned)
        def _():
            sent(xin, v_s.at[0, 0])
            for q in range(2):
                for cc in range(2):
                    sent(vector_piece(q, z - 1 - 2 * q, cc), t_s.at[q, cc])
            for step in range(4):
                for q in range(2):
                    sent(SB.at[step, q], i_s.at[step, q])
            for k in range(2):
                sent(SZ.at[z], u_s.at[k])

        @pl.when(aligned)
        def _():
            for step in range(2):
                for q in range(2):
                    sent(SB.at[step, q], i_s.at[step, q])
            sent(SB.at[2], i_s.at[2, 0])
            sent(SZ.at[z], u_s.at[0])
            for e in (1, 3, 2):
                for cc in range(2):
                    sent(SO.at[x], w_s.at[e, cc])
            sent(SO.at[x], w_s.at[0, 0])

    stage("drain", drain)


def shards(pair_density, trial_vectors, frequency, val_energy, cond_energy, pair_index):
    groups = lax.axis_size("freq")
    members = lax.axis_size("band")
    pair_count = pair_density.shape[0] * groups * members
    grid_count = trial_vectors.shape[3] * members
    prefactor = 1.0 / math.sqrt(2.0 * grid_count * pair_count)
    pieces = jnp.transpose(pair_density, (1, 0, 2))
    bf, f32 = jnp.bfloat16, jnp.float32
    vmem = pl.BlockSpec(memory_space=pltpu.VMEM)
    smem = pl.BlockSpec(memory_space=pltpu.SMEM)
    dma = pltpu.SemaphoreType.DMA
    parts, subspace = pl.pallas_call(
        functools.partial(kernel, (prefactor, grid_count)),
        name="response",
        out_shape=(
            jax.ShapeDtypeStruct((3, 2, 2, 2, 64, 512), bf),
            jax.ShapeDtypeStruct((4, 2, 64, 64), f32),
        ),
        in_specs=[vmem, vmem, smem, smem, smem, smem],
        out_specs=(vmem, vmem),
        scratch_shapes=[
            pltpu.VMEM((2, 4, 2, 4, 2, 16, 2048), bf),
            pltpu.VMEM((4, 2, 64, 2048), bf),
            pltpu.VMEM((512, 2048), f32),
            pltpu.VMEM((2, 4, 4, 2, 64, 128), f32),
            pltpu.VMEM((2, 4, 4, 2, 64, 128), bf),
            pltpu.VMEM((2, 4, 4, 2, 64, 128), bf),
            pltpu.VMEM((2, 4, 4, 2, 64, 128), bf),
            pltpu.VMEM((4, 2, 64, 768), bf),
            pltpu.VMEM((4, 2, 2, 2, 64, 512), bf),
            pltpu.VMEM((2, 2, 2, 2, 64, 512), bf),
            pltpu.VMEM((32, 8, 128), f32),
            pltpu.VMEM((4, 64, 128), f32),
            pltpu.VMEM((4, 64, 128), f32),
            pltpu.VMEM((256, 128), f32),
            pltpu.VMEM((2, 4, 8, 128), f32),
            dma((2, 4)), dma((2, 4)),
            dma((2, 2, 4)), dma((2, 2, 4)),
            dma((2, 2, 4)), dma((2, 2, 4)),
            dma((2, 4, 4)), dma((2, 4, 4)),
            dma((4, 2)), dma((4, 2, 2)), dma((2, 2)),
            dma((2, 4, 4)), dma((2, 4, 4)),
            dma((2, 4, 4)), dma((2, 4, 4)),
            dma((4, 2)), dma((4, 2)), dma((2, 2)),
            dma((2, 4)), dma((2, 4)),
            dma((2,)), dma((4,)),
            dma((4, 2)), dma((4,)),
            dma, dma,
        ],
        compiler_params=pltpu.CompilerParams(
            collective_id=0, has_side_effects=True, vmem_limit_bytes=36 * 2**20
        ),
    )(pieces, trial_vectors, pair_index, cond_energy, val_energy, frequency)
    images = parts[0].astype(f32) + parts[1].astype(f32) + parts[2].astype(f32)
    return images.reshape(4, 2, 64, 512), subspace


def solution(mesh):
    return jax.shard_map(
        shards,
        mesh=mesh,
        in_specs=(
            P(("freq", "band"), None, None),
            P("freq", None, None, "band"),
            P("freq"),
            P(),
            P(),
            P(("freq", "band")),
        ),
        out_specs=(P("freq", None, None, "band"), P("freq", None, None, None)),
        check_vma=False,
    )
```

```python
import functools
import math

import jax
import jax.numpy as jnp
from jax import lax
from jax.experimental import pallas as pl
from jax.experimental.pallas import tpu as pltpu
from jax.sharding import PartitionSpec as P

MESH = pl.DeviceIdType.MESH
ORDER = (0, 1, 3, 2)


def wrap(v, n=4):
    return lax.rem(v + n, n)


def dev(x, y, z, c):
    x, y, z, c = wrap(x), wrap(y), wrap(z), wrap(c, 2)
    return (lax.rem(z, 2) * 4 + y, x * 4 + (z // 2) * 2 + c)


def dot_nt(a, b):
    return lax.dot_general(a, b, (((1,), (1,)), ((), ())), preferred_element_type=jnp.float32)


def kernel(
    consts,
    rho, xin, idx, cond, val, freq,
    RI, SO,
    R, XF, acc, C32, CB, CR, SF, L, SB, RC, D, SZ, SA, FQ,
    x_s, x_r, y_s, y_r, f_s, f_r, p_s, p_r, v_s, v_r, t_s, c_s, c_r, g_s, g_r,
    i_s, i_r, k_r, d_s, d_r, u_s, u_r, w_s, w_r, q_s, q_r,
):
    prefactor, grid_count = consts
    fi, bi = lax.axis_index("freq"), lax.axis_index("band")
    zl, y = fi // 4, lax.rem(fi, 4)
    x, zh, c = bi // 4, lax.rem(bi // 2, 2), lax.rem(bi, 2)
    z = zh * 2 + zl
    me = (fi, bi)
    partner = dev(x, y, z, 1 - c)
    aligned = zl == c
    unaligned = jnp.logical_not(aligned)
    pending = []

    def send(src, dst, ss, rs, to):
        copy = pltpu.make_async_remote_copy(
            src_ref=src, dst_ref=dst, send_sem=ss, recv_sem=rs, device_id=to, device_id_type=MESH
        )
        copy.start()
        return copy

    def keep(copy):
        pending.append(copy)

    def arrived(dst, rs):
        pltpu.make_async_remote_copy(
            src_ref=dst, dst_ref=dst, send_sem=rs, recv_sem=rs, device_id=me, device_id_type=MESH
        ).wait_recv()

    def sent(src, ss):
        pltpu.make_async_remote_copy(
            src_ref=src, dst_ref=src, send_sem=ss, recv_sem=ss, device_id=me, device_id_type=MESH
        ).wait_send()

    lines = [dev(x + e, y, z, cc) for e in (1, 2, 3) for cc in range(2)]
    lines += [dev(x, y + dy, z, c) for dy in (1, 2, 3)]
    lines += [dev(x, y, z + dz, cc) for dz in (1, 2, 3) for cc in range(2)]
    lines.append(partner)
    barrier = pltpu.get_barrier_semaphore()
    for other in lines:
        pl.semaphore_signal(barrier, inc=1, device_id=other, device_id_type=MESH)
    with jax.named_scope("entry"):
        pl.semaphore_wait(barrier, len(lines))

    def lanes(block):
        return pl.ds(pl.multiple_of(block * 512, 512), 512)

    def stage(name, fn, *args):
        with jax.named_scope(name):
            fn(*args)

    def at(e):
        return wrap(x - e)

    def columns(block):
        return pl.ds(pl.multiple_of(block * 2048, 2048), 2048)

    def own_piece(h, block):
        return rho.at[:, pl.ds(16 * h, 16), columns(block)]

    def spread(h, e):
        src = own_piece(h, x) if e == 0 else R.at[h, 0, :, at(e), c]
        keep(send(src, R.at[h, 1, :, at(e), c], y_s.at[h, 0, e], y_r.at[h, 0, e], dev(x, y + 1, z, c)))
        keep(send(src, R.at[h, 2, :, at(e), c], y_s.at[h, 1, e], y_r.at[h, 1, e], dev(x, y - 1, z, c)))
        keep(send(src, R.at[h, 0, :, at(e), c], p_s.at[h, 0, e], p_r.at[h, 0, e], partner))

    def pass_on(h, e):
        for side in range(2):
            to = dev(x, y + 1 - 2 * side, z, c)
            piece = R.at[h, 1 + side, :, at(e), c]
            arrived(piece, y_r.at[h, side, e])
            part = R.at[h, 1 + side, side, at(e), c]
            keep(send(part, R.at[h, 3, side, at(e), c], f_s.at[h, side, e], f_r.at[h, side, e], to))
            keep(send(piece, piece, p_s.at[h, 1 + side, e], p_r.at[h, 1 + side, e], partner))

    def pass_far(h, e):
        for side in range(2):
            arrived(R.at[h, 3, side, at(e), c], f_r.at[h, side, e])
        piece = R.at[h, 3, :, at(e), c]
        keep(send(piece, piece, p_s.at[h, 3, e], p_r.at[h, 3, e], partner))

    def partner_done(h, pos):
        for e in ORDER:
            arrived(R.at[h, pos, :, at(e), 1 - c], p_r.at[h, pos, e])

    def from_x(h, e):
        arrived(R.at[h, 0, :, at(e), c], x_r.at[h, e])
        spread(h, e)

    my_lanes = lanes(zh * 2 + c)

    def vector_piece(q, zz, cc):
        return XF.at[pl.ds(2 * q, 2), :, :, lanes((wrap(zz) // 2) * 2 + cc)]

    def begin():
        spread(0, 0)
        def to_x(h):
            for e in (1, 3, 2):
                keep(send(own_piece(h, wrap(x + e)), R.at[h, 0, :, x, c], x_s.at[h, e], x_r.at[h, e], dev(x + e, y, z, c)))

        to_x(0)
        for k in range(2):
            for side in range(2):
                q = (k + side) % 2
                dz = 1 + 2 * side
                keep(send(xin.at[pl.ds(2 * q, 2)], vector_piece(q, z, c), v_s.at[dz, q], v_r.at[dz, c, q], dev(x, y, z + dz, zl)))
        spread(1, 0)

        @pl.when(unaligned)
        def _():
            send(xin, XF.at[:, :, :, my_lanes], v_s.at[0, 0], v_r.at[0, c, 0], partner)

        for f in range(4):
            FQ[0, f] = jnp.full((8, 128), freq[f], jnp.float32)

        lane = lax.broadcasted_iota(jnp.int32, (8, 128), 1)
        row = lax.broadcasted_iota(jnp.int32, (8, 128), 0)
        place = jnp.bitwise_and(row, 1) * 16 + jnp.bitwise_and(lane, 15)
        number = jnp.zeros((8, 128), jnp.int32)
        for i in range(32):
            number = jnp.where(place == i, idx[i], number)
        cond_no = jnp.bitwise_and(number, 127)
        val_no = jnp.right_shift(number, 7)
        zero = jnp.zeros((8, 128), jnp.float32)
        cond_pick = lax.fori_loop(0, 128, lambda j, a: jnp.where(cond_no == j, cond[j], a), zero)
        val_pick = lax.fori_loop(0, 32, lambda j, a: jnp.where(val_no == j, val[j], a), zero)
        D[c * 16 + x] = jnp.where(jnp.right_shift(lane, 4) == x * 2 + c, cond_pick - val_pick, 0.0)
        for h in range(2):
            R[h, 0, :, x, c] = rho[:, 16 * h : 16 * h + 16, columns(x)]

        @pl.when(aligned)
        def _():
            XF[:, :, :, my_lanes] = xin[...]
            FQ[1] = FQ[0]

        @pl.when(aligned)
        def _():
            send(FQ.at[0], FQ.at[1], q_s, q_r, dev(x, y, z - 1, c))

        for e in (1, 3, 2):
            keep(send(D.at[c * 16 + x], D.at[c * 16 + x], d_s.at[0, e], d_r.at[0, e], dev(x + e, y, z, c)))
        to_x(1)

    def energies_y():
        for e in (1, 3, 2):
            arrived(D.at[c * 16 + at(e)], d_r.at[0, e])
        row = D.at[pl.ds(c * 16, 4)]
        for dy, pos in ((1, 1), (3, 2), (2, 3)):
            keep(send(row, D.at[pl.ds(c * 16 + pos * 4, 4)], d_s.at[1, dy], d_r.at[1, dy], dev(x, y + dy, z, c)))

    def energies_core():
        for dy, pos in ((1, 1), (3, 2), (2, 3)):
            arrived(D.at[pl.ds(c * 16 + pos * 4, 4)], d_r.at[1, dy])
        keep(send(D.at[pl.ds(c * 16, 16)], D.at[pl.ds(c * 16, 16)], d_s.at[0, 0], d_r.at[0, 0], partner))

    def vectors_pass():
        @pl.when(unaligned)
        def _():
            for q in range(2):
                dz = 1 + 2 * q
                for cc in range(2):
                    piece = vector_piece(q, z - dz, cc)
                    arrived(piece, v_r.at[dz, cc, q])
                    send(piece, piece, t_s.at[q, cc], v_r.at[2, cc, q], dev(x, y, z + dz, c))

    def vectors_done():
        @pl.when(aligned)
        def _():
            arrived(XF.at[:, :, :, lanes(zh * 2 + 1 - c)], v_r.at[0, 1 - c, 0])
            for q in range(2):
                for cc in range(2):
                    arrived(vector_piece(q, z + 2, cc), v_r.at[2, cc, q])

        @pl.when(unaligned)
        def _():
            for q in range(2):
                dz = 3 - 2 * q
                for cc in range(2):
                    arrived(vector_piece(q, z - dz, cc), v_r.at[dz, cc, q])

    A, FAR, B, LAST = (0, 0, 3), (0, 3, 4), (1, 0, 2), (1, 2, 4)

    def cross(h, pos):
        t = dot_nt(XF[...].reshape(512, 2048), R[h, pos].reshape(256, 2048)).reshape(4, 2, 64, 256)
        re = t[:, 0, :, 0:128] + t[:, 1, :, 128:256]
        im = t[:, 1, :, 0:128] - t[:, 0, :, 128:256]
        C32[h, :, pos, 0] = re
        C32[h, :, pos, 1] = im
        CB[h, :, pos, 0] = re.astype(jnp.bfloat16)
        CB[h, :, pos, 1] = im.astype(jnp.bfloat16)

    def cross_out(h, pos):
        for e in (2, 1, 3):
            keep(send(CB.at[h, wrap(x + e), pos], CR.at[h, e, pos], c_s.at[h, pos, e], c_r.at[h, pos, e], dev(x + e, y, z, c)))

    def scale(h, pos):
        for e in (1, 3, 2):
            arrived(CR.at[h, e, pos], c_r.at[h, pos, e])
        own = FQ[1, x][0:1, 0:1]
        total = C32[h, x, pos]
        for e in (1, 2, 3):
            total = total + CR[h, e, pos].astype(jnp.float32)
        delta = D[pos * 4]
        for k in range(1, 8):
            delta = delta + D[(k // 4) * 16 + pos * 4 + k % 4]
        delta = delta[h : h + 1]
        ratio = delta / (delta * delta + own * own)
        weight = (-4.0 * prefactor * ratio).astype(jnp.bfloat16).astype(jnp.float32)
        SF[h, x, pos] = (weight[None] * total).astype(jnp.bfloat16)
        C32[h, x, pos] = total
        for e in (2, 1, 3):
            keep(send(SF.at[h, x, pos], SF.at[h, x, pos], g_s.at[h, pos, e], g_r.at[h, pos, e], dev(x + e, y, z, c)))

    def project_add(group):
        h = group[0]
        for pos in range(group[1], group[2]):
            flat = C32[h, x, pos].reshape(128, 128)
            high = flat.astype(jnp.bfloat16)
            low = (flat - high.astype(jnp.float32)).astype(jnp.bfloat16)
            part = dot_nt(jnp.concatenate([high, low], axis=0), SF[h, x, pos].reshape(128, 128))
            if h == 0 and pos == 0:
                SA[...] = part
            else:
                SA[...] += part

    def gathered(group):
        h = group[0]
        for pos in range(group[1], group[2]):
            for e in (1, 3, 2):
                arrived(SF.at[h, at(e), pos], g_r.at[h, pos, e])
        for pos in range(group[1], group[2]):
            base = (pos - group[1]) * 256
            re, im = SF[h, :, pos, 0], SF[h, :, pos, 1]
            L[:, 0, :, base : base + 128] = re
            L[:, 0, :, base + 128 : base + 256] = -im
            L[:, 1, :, base : base + 128] = im
            L[:, 1, :, base + 128 : base + 256] = re

    def image_tile(group, block):
        h, some = group[0], pl.ds(group[1], group[2] - group[1])
        depth = (group[2] - group[1]) * 256
        return jnp.dot(
            L[:, :, :, 0:depth].reshape(512, depth),
            R[h, some, :, :, :, :, lanes(block)].reshape(depth, 512),
            preferred_element_type=jnp.float32,
        )

    def image(group):
        gathered(group)
        for block in range(4):
            part = image_tile(group, block)
            if group == A:
                acc[:, block * 512 : block * 512 + 512] = part
            else:
                acc[:, block * 512 : block * 512 + 512] += part

    def energies_done():
        arrived(D.at[pl.ds((1 - c) * 16, 16)], d_r.at[0, 0])

        @pl.when(aligned)
        def _():
            sent(FQ.at[0], q_s)

        @pl.when(unaligned)
        def _():
            arrived(FQ.at[1], q_r)

    stage("begin", begin)
    stage("xA1", from_x, 0, 1)
    stage("xA3", from_x, 0, 3)
    stage("passA0", pass_on, 0, 0)
    stage("xA2", from_x, 0, 2)
    stage("relay", vectors_pass)
    stage("energies_y", energies_y)
    stage("passA1", pass_on, 0, 1)
    stage("passA3", pass_on, 0, 3)
    stage("xB1", from_x, 1, 1)
    stage("xB3", from_x, 1, 3)
    stage("farA0", pass_far, 0, 0)
    stage("passA2", pass_on, 0, 2)
    stage("passB0", pass_on, 1, 0)
    stage("xB2", from_x, 1, 2)
    stage("energies_core", energies_core)
    stage("vectors", vectors_done)
    stage("partA0", partner_done, 0, 0)
    stage("crossA0", cross, 0, 0)
    stage("outA0", cross_out, 0, 0)
    stage("farA1", pass_far, 0, 1)
    stage("partA1", partner_done, 0, 1)
    stage("crossA1", cross, 0, 1)
    stage("outA1", cross_out, 0, 1)
    stage("farA3", pass_far, 0, 3)
    stage("partA2", partner_done, 0, 2)
    stage("crossA2", cross, 0, 2)
    stage("outA2", cross_out, 0, 2)
    stage("partB0", partner_done, 1, 0)
    stage("crossB0", cross, 1, 0)
    stage("outB0", cross_out, 1, 0)
    stage("passB1", pass_on, 1, 1)
    stage("energies", energies_done)
    stage("scaleA0", scale, 0, 0)
    stage("scaleA1", scale, 0, 1)
    stage("passB3", pass_on, 1, 3)
    stage("farA2", pass_far, 0, 2)
    stage("partA3", partner_done, 0, 3)
    stage("crossA3", cross, 0, 3)
    stage("outA3", cross_out, 0, 3)
    stage("scaleA2", scale, 0, 2)
    stage("scaleB0", scale, 1, 0)
    stage("passB2", pass_on, 1, 2)
    stage("farB0", pass_far, 1, 0)
    stage("partB1", partner_done, 1, 1)
    stage("crossB1", cross, 1, 1)
    stage("outB1", cross_out, 1, 1)
    stage("farB1", pass_far, 1, 1)
    stage("partB2", partner_done, 1, 2)
    stage("crossB2", cross, 1, 2)
    stage("outB2", cross_out, 1, 2)
    stage("farB3", pass_far, 1, 3)
    stage("farB2", pass_far, 1, 2)
    stage("scaleA3", scale, 0, 3)
    stage("partB3", partner_done, 1, 3)
    stage("crossB3", cross, 1, 3)
    stage("outB3", cross_out, 1, 3)
    stage("scaleB1", scale, 1, 1)
    stage("imageA", image, A)
    stage("scaleB2", scale, 1, 2)
    stage("scaleB3", scale, 1, 3)
    stage("imageF", image, FAR)
    stage("addA", project_add, A)
    stage("addF", project_add, FAR)
    stage("addB", project_add, B)
    stage("addL", project_add, LAST)

    def project_z():
        both = SA[0:128] + SA[128:256]
        re = both[0:64, 0:64] + both[64:128, 64:128]
        im = both[0:64, 64:128] - both[64:128, 0:64]
        SZ[z] = jnp.concatenate([re, im], axis=1) / grid_count

        @pl.when(aligned)
        def _():
            send(SZ.at[z], SZ.at[z], u_s.at[0], u_r.at[2], dev(x, y, z + 2, c))

        @pl.when(unaligned)
        def _():
            for k, dz in enumerate((1, 3)):
                send(SZ.at[z], SZ.at[z], u_s.at[k], u_r.at[dz], dev(x, y, z + dz, c))

    def project_x():
        @pl.when(aligned)
        def _():
            for dz in (1, 3, 2):
                arrived(SZ.at[wrap(z - dz)], u_r.at[dz])
            SO[x] = SZ[0] + SZ[1] + SZ[2] + SZ[3]
            for e in (1, 3, 2):
                for cc in range(2):
                    send(SO.at[x], SO.at[x], w_s.at[e, cc], w_r.at[e], dev(x + e, y, z, cc))
            send(SO.at[x], SO.at[x], w_s.at[0, 0], w_r.at[0], dev(x, y, z, 1 - c))

    def project_done():
        @pl.when(unaligned)
        def _():
            arrived(SO.at[x], w_r.at[0])

        for e in (1, 3, 2):
            arrived(SO.at[at(e)], w_r.at[e])

    stage("project_z", project_z)
    stage("imageB", image, B)
    stage("gatheredL", gathered, LAST)

    def target(step):
        h = 1 - zh if step < 2 else zh
        cc = 1 - c if step % 2 == 0 else c
        to_z = h * 2 + c
        dz = wrap(to_z - z)
        return h * 2 + cc, cc, to_z, (dz + 1) // 2, (3 - dz) // 2

    def image_out(step):
        block, cc, to_z, slot, direct = target(step)
        total = acc[:, lanes(block)] + image_tile(LAST, block)
        half = total.astype(jnp.bfloat16).reshape(2, 2, 2, 64, 512)
        SB[step] = half

        @pl.when(unaligned)
        def _():
            acc[:, lanes(block)] = total
            send(SB.at[step, direct], RI.at[slot, direct], i_s.at[step, direct], i_r.at[slot, direct], dev(x, y, to_z, cc))

        @pl.when(aligned)
        def _():
            if step < 2:
                send(SB.at[step, 0], RC.at[0, cc], i_s.at[step, 0], k_r.at[0, cc], dev(x, y, z + 1, c))
                send(SB.at[step, 1], RC.at[1, cc], i_s.at[step, 1], k_r.at[1, cc], dev(x, y, z - 1, c))
            elif step == 2:
                send(SB.at[step], RI.at[0], i_s.at[step, 0], i_r.at[0, 0], partner)
            else:
                RI[0] = half

    def image_join(step):
        block, cc, to_z, slot, direct = target(step)
        joined = 1 - direct
        arrived(RC.at[joined, cc], k_r.at[joined, cc])
        rows = pl.ds(pl.multiple_of(joined * 256, 256), 256)
        total = acc[rows, lanes(block)].reshape(2, 2, 64, 512) + RC[joined, cc].astype(jnp.float32)
        SB[step, joined] = total.astype(jnp.bfloat16)
        send(SB.at[step, joined], RI.at[slot, joined], i_s.at[step, joined], i_r.at[slot, joined], dev(x, y, to_z, cc))

    for step in range(4):
        stage(f"out{step}", image_out, step)
    stage("project_x", project_x)

    @pl.when(unaligned)
    def _():
        for step in (0, 2, 1, 3):
            stage(f"join{step}", image_join, step)

    stage("project", project_done)

    def images_done():
        for slot in (1, 2):
            for q in range(2):
                arrived(RI.at[slot, q], i_r.at[slot, q])

        @pl.when(unaligned)
        def _():
            arrived(RI.at[0], i_r.at[0, 0])

    stage("images", images_done)

    def drain():
        for copy in pending:
            copy.wait_send()

        @pl.when(unaligned)
        def _():
            sent(xin, v_s.at[0, 0])
            for q in range(2):
                for cc in range(2):
                    sent(vector_piece(q, z - 1 - 2 * q, cc), t_s.at[q, cc])
            for step in range(4):
                for q in range(2):
                    sent(SB.at[step, q], i_s.at[step, q])
            for k in range(2):
                sent(SZ.at[z], u_s.at[k])

        @pl.when(aligned)
        def _():
            for step in range(2):
                for q in range(2):
                    sent(SB.at[step, q], i_s.at[step, q])
            sent(SB.at[2], i_s.at[2, 0])
            sent(SZ.at[z], u_s.at[0])
            for e in (1, 3, 2):
                for cc in range(2):
                    sent(SO.at[x], w_s.at[e, cc])
            sent(SO.at[x], w_s.at[0, 0])

    stage("drain", drain)


def finish(parts, so, img, sub):
    for f in range(4):
        total = parts[0, f].astype(jnp.float32) + parts[1, f].astype(jnp.float32)
        img[f] = total + parts[2, f].astype(jnp.float32)
        sub[f, 0] = so[f, :, 0:64]
        sub[f, 1] = so[f, :, 64:128]


def shards(pair_density, trial_vectors, frequency, val_energy, cond_energy, pair_index):
    groups = lax.axis_size("freq")
    members = lax.axis_size("band")
    pair_count = pair_density.shape[0] * groups * members
    grid_count = trial_vectors.shape[3] * members
    prefactor = 1.0 / math.sqrt(2.0 * grid_count * pair_count)
    pieces = jnp.transpose(pair_density, (1, 0, 2))
    bf, f32 = jnp.bfloat16, jnp.float32
    vmem = pl.BlockSpec(memory_space=pltpu.VMEM)
    smem = pl.BlockSpec(memory_space=pltpu.SMEM)
    dma = pltpu.SemaphoreType.DMA
    parts, subspace = pl.pallas_call(
        functools.partial(kernel, (prefactor, grid_count)),
        name="response",
        out_shape=(
            jax.ShapeDtypeStruct((3, 2, 2, 2, 64, 512), bf),
            jax.ShapeDtypeStruct((4, 64, 128), f32),
        ),
        in_specs=[vmem, vmem, smem, smem, smem, smem],
        out_specs=(vmem, vmem),
        scratch_shapes=[
            pltpu.VMEM((2, 4, 2, 4, 2, 16, 2048), bf),
            pltpu.VMEM((4, 2, 64, 2048), bf),
            pltpu.VMEM((512, 2048), f32),
            pltpu.VMEM((2, 4, 4, 2, 64, 128), f32),
            pltpu.VMEM((2, 4, 4, 2, 64, 128), bf),
            pltpu.VMEM((2, 4, 4, 2, 64, 128), bf),
            pltpu.VMEM((2, 4, 4, 2, 64, 128), bf),
            pltpu.VMEM((4, 2, 64, 768), bf),
            pltpu.VMEM((4, 2, 2, 2, 64, 512), bf),
            pltpu.VMEM((2, 2, 2, 2, 64, 512), bf),
            pltpu.VMEM((32, 8, 128), f32),
            pltpu.VMEM((4, 64, 128), f32),
            pltpu.VMEM((256, 128), f32),
            pltpu.VMEM((2, 4, 8, 128), f32),
            dma((2, 4)), dma((2, 4)),
            dma((2, 2, 4)), dma((2, 2, 4)),
            dma((2, 2, 4)), dma((2, 2, 4)),
            dma((2, 4, 4)), dma((2, 4, 4)),
            dma((4, 2)), dma((4, 2, 2)), dma((2, 2)),
            dma((2, 4, 4)), dma((2, 4, 4)),
            dma((2, 4, 4)), dma((2, 4, 4)),
            dma((4, 2)), dma((4, 2)), dma((2, 2)),
            dma((2, 4)), dma((2, 4)),
            dma((2,)), dma((4,)),
            dma((4, 2)), dma((4,)),
            dma, dma,
        ],
        compiler_params=pltpu.CompilerParams(
            collective_id=0, has_side_effects=True, vmem_limit_bytes=36 * 2**20
        ),
    )(pieces, trial_vectors, pair_index, cond_energy, val_energy, frequency)
    return pl.pallas_call(
        finish,
        name="finish",
        out_shape=(
            jax.ShapeDtypeStruct((4, 2, 64, 512), f32),
            jax.ShapeDtypeStruct((4, 2, 64, 64), f32),
        ),
        in_specs=[vmem, vmem],
        out_specs=(vmem, vmem),
        compiler_params=pltpu.CompilerParams(vmem_limit_bytes=8 * 2**20),
    )(parts.reshape(3, 4, 2, 64, 512), subspace)


def solution(mesh):
    return jax.shard_map(
        shards,
        mesh=mesh,
        in_specs=(
            P(("freq", "band"), None, None),
            P("freq", None, None, "band"),
            P("freq"),
            P(),
            P(),
            P(("freq", "band")),
        ),
        out_specs=(P("freq", None, None, "band"), P("freq", None, None, None)),
        check_vma=False,
    )
```

```python
import functools
import math

import jax
import jax.numpy as jnp
from jax import lax
from jax.experimental import pallas as pl
from jax.experimental.pallas import tpu as pltpu
from jax.sharding import PartitionSpec as P

MESH = pl.DeviceIdType.MESH
ORDER = (0, 1, 3, 2)


def wrap(v, n=4):
    return lax.rem(v + n, n)


def dev(x, y, z, c):
    x, y, z, c = wrap(x), wrap(y), wrap(z), wrap(c, 2)
    return (lax.rem(z, 2) * 4 + y, x * 4 + (z // 2) * 2 + c)


def dot_nt(a, b):
    return lax.dot_general(a, b, (((1,), (1,)), ((), ())), preferred_element_type=jnp.float32)


def kernel(
    consts,
    rho, xin, idx, cond, val, freq,
    RI, SO,
    R, XF, acc, C32, CB, CR, SF, L, SB, RC, D, SZ, SA, FQ,
    x_s, x_r, y_s, y_r, f_s, f_r, p_s, p_r, v_s, v_r, t_s, c_s, c_r, g_s, g_r,
    i_s, i_r, k_r, d_s, d_r, u_s, u_r, w_s, w_r, q_s, q_r,
):
    prefactor, grid_count = consts
    fi, bi = lax.axis_index("freq"), lax.axis_index("band")
    zl, y = fi // 4, lax.rem(fi, 4)
    x, zh, c = bi // 4, lax.rem(bi // 2, 2), lax.rem(bi, 2)
    z = zh * 2 + zl
    me = (fi, bi)
    partner = dev(x, y, z, 1 - c)
    aligned = zl == c
    unaligned = jnp.logical_not(aligned)
    pending = []

    def send(src, dst, ss, rs, to):
        copy = pltpu.make_async_remote_copy(
            src_ref=src, dst_ref=dst, send_sem=ss, recv_sem=rs, device_id=to, device_id_type=MESH
        )
        copy.start()
        return copy

    def keep(copy):
        pending.append(copy)

    def arrived(dst, rs):
        pltpu.make_async_remote_copy(
            src_ref=dst, dst_ref=dst, send_sem=rs, recv_sem=rs, device_id=me, device_id_type=MESH
        ).wait_recv()

    def sent(src, ss):
        pltpu.make_async_remote_copy(
            src_ref=src, dst_ref=src, send_sem=ss, recv_sem=ss, device_id=me, device_id_type=MESH
        ).wait_send()

    lines = [dev(x + e, y, z, cc) for e in (1, 2, 3) for cc in range(2)]
    lines += [dev(x, y + dy, z, c) for dy in (1, 2, 3)]
    lines += [dev(x, y, z + dz, cc) for dz in (1, 2, 3) for cc in range(2)]
    lines.append(partner)
    barrier = pltpu.get_barrier_semaphore()
    for other in lines:
        pl.semaphore_signal(barrier, inc=1, device_id=other, device_id_type=MESH)
    with jax.named_scope("entry"):
        pl.semaphore_wait(barrier, len(lines))

    def lanes(block):
        return pl.ds(pl.multiple_of(block * 512, 512), 512)

    def stage(name, fn, *args):
        with jax.named_scope(name):
            fn(*args)

    def at(e):
        return wrap(x - e)

    def columns(block):
        return pl.ds(pl.multiple_of(block * 2048, 2048), 2048)

    def own_piece(h, block):
        return rho.at[:, pl.ds(16 * h, 16), columns(block)]

    def spread(h, e):
        src = own_piece(h, x) if e == 0 else R.at[h, 0, :, at(e), c]
        keep(send(src, R.at[h, 1, :, at(e), c], y_s.at[h, 0, e], y_r.at[h, 0, e], dev(x, y + 1, z, c)))
        keep(send(src, R.at[h, 2, :, at(e), c], y_s.at[h, 1, e], y_r.at[h, 1, e], dev(x, y - 1, z, c)))
        keep(send(src, R.at[h, 0, :, at(e), c], p_s.at[h, 0, e], p_r.at[h, 0, e], partner))

    def pass_on(h, e):
        for side in range(2):
            to = dev(x, y + 1 - 2 * side, z, c)
            piece = R.at[h, 1 + side, :, at(e), c]
            arrived(piece, y_r.at[h, side, e])
            part = R.at[h, 1 + side, side, at(e), c]
            keep(send(part, R.at[h, 3, side, at(e), c], f_s.at[h, side, e], f_r.at[h, side, e], to))
            keep(send(piece, piece, p_s.at[h, 1 + side, e], p_r.at[h, 1 + side, e], partner))

    def pass_far(h, e):
        for side in range(2):
            arrived(R.at[h, 3, side, at(e), c], f_r.at[h, side, e])
        piece = R.at[h, 3, :, at(e), c]
        keep(send(piece, piece, p_s.at[h, 3, e], p_r.at[h, 3, e], partner))

    def partner_done(h, pos):
        for e in ORDER:
            arrived(R.at[h, pos, :, at(e), 1 - c], p_r.at[h, pos, e])

    def from_x(h, e):
        arrived(R.at[h, 0, :, at(e), c], x_r.at[h, e])
        spread(h, e)

    my_lanes = lanes(zh * 2 + c)

    def vector_piece(q, zz, cc):
        return XF.at[pl.ds(2 * q, 2), :, :, lanes((wrap(zz) // 2) * 2 + cc)]

    def begin():
        spread(0, 0)
        def to_x(h):
            for e in (1, 3, 2):
                keep(send(own_piece(h, wrap(x + e)), R.at[h, 0, :, x, c], x_s.at[h, e], x_r.at[h, e], dev(x + e, y, z, c)))

        to_x(0)
        for k in range(2):
            for side in range(2):
                q = (k + side) % 2
                dz = 1 + 2 * side
                keep(send(xin.at[pl.ds(2 * q, 2)], vector_piece(q, z, c), v_s.at[dz, q], v_r.at[dz, c, q], dev(x, y, z + dz, zl)))
        spread(1, 0)

        @pl.when(unaligned)
        def _():
            send(xin, XF.at[:, :, :, my_lanes], v_s.at[0, 0], v_r.at[0, c, 0], partner)

        for f in range(4):
            FQ[0, f] = jnp.full((8, 128), freq[f], jnp.float32)

        lane = lax.broadcasted_iota(jnp.int32, (8, 128), 1)
        row = lax.broadcasted_iota(jnp.int32, (8, 128), 0)
        place = jnp.bitwise_and(row, 1) * 16 + jnp.bitwise_and(lane, 15)
        number = jnp.zeros((8, 128), jnp.int32)
        for i in range(32):
            number = jnp.where(place == i, idx[i], number)
        cond_no = jnp.bitwise_and(number, 127)
        val_no = jnp.right_shift(number, 7)
        zero = jnp.zeros((8, 128), jnp.float32)
        cond_pick = lax.fori_loop(0, 128, lambda j, a: jnp.where(cond_no == j, cond[j], a), zero)
        val_pick = lax.fori_loop(0, 32, lambda j, a: jnp.where(val_no == j, val[j], a), zero)
        D[c * 16 + x] = jnp.where(jnp.right_shift(lane, 4) == x * 2 + c, cond_pick - val_pick, 0.0)
        for h in range(2):
            R[h, 0, :, x, c] = rho[:, 16 * h : 16 * h + 16, columns(x)]

        @pl.when(aligned)
        def _():
            XF[:, :, :, my_lanes] = xin[...]
            FQ[1] = FQ[0]

        @pl.when(aligned)
        def _():
            send(FQ.at[0], FQ.at[1], q_s, q_r, dev(x, y, z - 1, c))

        for e in (1, 3, 2):
            keep(send(D.at[c * 16 + x], D.at[c * 16 + x], d_s.at[0, e], d_r.at[0, e], dev(x + e, y, z, c)))
        to_x(1)

    def energies_y():
        for e in (1, 3, 2):
            arrived(D.at[c * 16 + at(e)], d_r.at[0, e])
        row = D.at[pl.ds(c * 16, 4)]
        for dy, pos in ((1, 1), (3, 2), (2, 3)):
            keep(send(row, D.at[pl.ds(c * 16 + pos * 4, 4)], d_s.at[1, dy], d_r.at[1, dy], dev(x, y + dy, z, c)))

    def energies_core():
        for dy, pos in ((1, 1), (3, 2), (2, 3)):
            arrived(D.at[pl.ds(c * 16 + pos * 4, 4)], d_r.at[1, dy])
        keep(send(D.at[pl.ds(c * 16, 16)], D.at[pl.ds(c * 16, 16)], d_s.at[0, 0], d_r.at[0, 0], partner))

    def vectors_pass():
        @pl.when(unaligned)
        def _():
            for q in range(2):
                dz = 1 + 2 * q
                for cc in range(2):
                    piece = vector_piece(q, z - dz, cc)
                    arrived(piece, v_r.at[dz, cc, q])
                    send(piece, piece, t_s.at[q, cc], v_r.at[2, cc, q], dev(x, y, z + dz, c))

    def vectors_done():
        @pl.when(aligned)
        def _():
            arrived(XF.at[:, :, :, lanes(zh * 2 + 1 - c)], v_r.at[0, 1 - c, 0])
            for q in range(2):
                for cc in range(2):
                    arrived(vector_piece(q, z + 2, cc), v_r.at[2, cc, q])

        @pl.when(unaligned)
        def _():
            for q in range(2):
                dz = 3 - 2 * q
                for cc in range(2):
                    arrived(vector_piece(q, z - dz, cc), v_r.at[dz, cc, q])

    A, FAR, B, LAST = (0, 0, 3), (0, 3, 4), (1, 0, 2), (1, 2, 4)

    def cross(h, pos):
        t = dot_nt(XF[...].reshape(512, 2048), R[h, pos].reshape(256, 2048)).reshape(4, 2, 64, 256)
        re = t[:, 0, :, 0:128] + t[:, 1, :, 128:256]
        im = t[:, 1, :, 0:128] - t[:, 0, :, 128:256]
        C32[h, :, pos, 0] = re
        C32[h, :, pos, 1] = im
        CB[h, :, pos, 0] = re.astype(jnp.bfloat16)
        CB[h, :, pos, 1] = im.astype(jnp.bfloat16)

    def cross_out(h, pos):
        for e in (2, 1, 3):
            keep(send(CB.at[h, wrap(x + e), pos], CR.at[h, e, pos], c_s.at[h, pos, e], c_r.at[h, pos, e], dev(x + e, y, z, c)))

    def scale(h, pos):
        for e in (1, 3, 2):
            arrived(CR.at[h, e, pos], c_r.at[h, pos, e])
        own = FQ[1, x][0:1, 0:1]
        total = C32[h, x, pos]
        for e in (1, 2, 3):
            total = total + CR[h, e, pos].astype(jnp.float32)
        delta = D[pos * 4]
        for k in range(1, 8):
            delta = delta + D[(k // 4) * 16 + pos * 4 + k % 4]
        delta = delta[h : h + 1]
        ratio = delta / (delta * delta + own * own)
        weight = (-4.0 * prefactor * ratio).astype(jnp.bfloat16).astype(jnp.float32)
        SF[h, x, pos] = (weight[None] * total).astype(jnp.bfloat16)
        C32[h, x, pos] = total
        for e in (2, 1, 3):
            keep(send(SF.at[h, x, pos], SF.at[h, x, pos], g_s.at[h, pos, e], g_r.at[h, pos, e], dev(x + e, y, z, c)))

    def project_add(group):
        h = group[0]
        for pos in range(group[1], group[2]):
            flat = C32[h, x, pos].reshape(128, 128)
            high = flat.astype(jnp.bfloat16)
            low = (flat - high.astype(jnp.float32)).astype(jnp.bfloat16)
            part = dot_nt(jnp.concatenate([high, low], axis=0), SF[h, x, pos].reshape(128, 128))
            if h == 0 and pos == 0:
                SA[...] = part
            else:
                SA[...] += part

    def gathered(group):
        h = group[0]
        for pos in range(group[1], group[2]):
            for e in (1, 3, 2):
                arrived(SF.at[h, at(e), pos], g_r.at[h, pos, e])
        for pos in range(group[1], group[2]):
            base = (pos - group[1]) * 256
            re, im = SF[h, :, pos, 0], SF[h, :, pos, 1]
            L[:, 0, :, base : base + 128] = re
            L[:, 0, :, base + 128 : base + 256] = -im
            L[:, 1, :, base : base + 128] = im
            L[:, 1, :, base + 128 : base + 256] = re

    def image_tile(group, block):
        h, some = group[0], pl.ds(group[1], group[2] - group[1])
        depth = (group[2] - group[1]) * 256
        return jnp.dot(
            L[:, :, :, 0:depth].reshape(512, depth),
            R[h, some, :, :, :, :, lanes(block)].reshape(depth, 512),
            preferred_element_type=jnp.float32,
        )

    def image(group):
        gathered(group)
        for block in range(4):
            part = image_tile(group, block)
            if group == A:
                acc[:, block * 512 : block * 512 + 512] = part
            else:
                acc[:, block * 512 : block * 512 + 512] += part

    def energies_done():
        arrived(D.at[pl.ds((1 - c) * 16, 16)], d_r.at[0, 0])

        @pl.when(aligned)
        def _():
            sent(FQ.at[0], q_s)

        @pl.when(unaligned)
        def _():
            arrived(FQ.at[1], q_r)

    stage("begin", begin)
    stage("xA1", from_x, 0, 1)
    stage("xA3", from_x, 0, 3)
    stage("passA0", pass_on, 0, 0)
    stage("xA2", from_x, 0, 2)
    stage("relay", vectors_pass)
    stage("energies_y", energies_y)
    stage("passA1", pass_on, 0, 1)
    stage("passA3", pass_on, 0, 3)
    stage("xB1", from_x, 1, 1)
    stage("xB3", from_x, 1, 3)
    stage("farA0", pass_far, 0, 0)
    stage("passA2", pass_on, 0, 2)
    stage("passB0", pass_on, 1, 0)
    stage("xB2", from_x, 1, 2)
    stage("energies_core", energies_core)
    stage("vectors", vectors_done)
    stage("partA0", partner_done, 0, 0)
    stage("crossA0", cross, 0, 0)
    stage("outA0", cross_out, 0, 0)
    stage("farA1", pass_far, 0, 1)
    stage("partA1", partner_done, 0, 1)
    stage("crossA1", cross, 0, 1)
    stage("outA1", cross_out, 0, 1)
    stage("farA3", pass_far, 0, 3)
    stage("partA2", partner_done, 0, 2)
    stage("crossA2", cross, 0, 2)
    stage("outA2", cross_out, 0, 2)
    stage("partB0", partner_done, 1, 0)
    stage("crossB0", cross, 1, 0)
    stage("outB0", cross_out, 1, 0)
    stage("passB1", pass_on, 1, 1)
    stage("energies", energies_done)
    stage("scaleA0", scale, 0, 0)
    stage("scaleA1", scale, 0, 1)
    stage("passB3", pass_on, 1, 3)
    stage("farA2", pass_far, 0, 2)
    stage("partA3", partner_done, 0, 3)
    stage("crossA3", cross, 0, 3)
    stage("outA3", cross_out, 0, 3)
    stage("scaleA2", scale, 0, 2)
    stage("scaleB0", scale, 1, 0)
    stage("passB2", pass_on, 1, 2)
    stage("farB0", pass_far, 1, 0)
    stage("partB1", partner_done, 1, 1)
    stage("crossB1", cross, 1, 1)
    stage("outB1", cross_out, 1, 1)
    stage("farB1", pass_far, 1, 1)
    stage("partB2", partner_done, 1, 2)
    stage("crossB2", cross, 1, 2)
    stage("outB2", cross_out, 1, 2)
    stage("farB3", pass_far, 1, 3)
    stage("farB2", pass_far, 1, 2)
    stage("scaleA3", scale, 0, 3)
    stage("partB3", partner_done, 1, 3)
    stage("crossB3", cross, 1, 3)
    stage("outB3", cross_out, 1, 3)
    stage("imageA", image, A)
    stage("scaleB1", scale, 1, 1)
    stage("scaleB2", scale, 1, 2)
    stage("imageF", image, FAR)
    stage("scaleB3", scale, 1, 3)
    stage("addA", project_add, A)
    stage("addF", project_add, FAR)
    stage("addB", project_add, B)
    stage("addL", project_add, LAST)

    def project_z():
        both = SA[0:128] + SA[128:256]
        re = both[0:64, 0:64] + both[64:128, 64:128]
        im = both[0:64, 64:128] - both[64:128, 0:64]
        SZ[z] = jnp.concatenate([re, im], axis=1) / grid_count

        @pl.when(aligned)
        def _():
            send(SZ.at[z], SZ.at[z], u_s.at[0], u_r.at[2], dev(x, y, z + 2, c))

        @pl.when(unaligned)
        def _():
            for k, dz in enumerate((1, 3)):
                send(SZ.at[z], SZ.at[z], u_s.at[k], u_r.at[dz], dev(x, y, z + dz, c))

    def project_x():
        @pl.when(aligned)
        def _():
            for dz in (1, 3, 2):
                arrived(SZ.at[wrap(z - dz)], u_r.at[dz])
            SO[x] = SZ[0] + SZ[1] + SZ[2] + SZ[3]
            for e in (1, 3, 2):
                for cc in range(2):
                    send(SO.at[x], SO.at[x], w_s.at[e, cc], w_r.at[e], dev(x + e, y, z, cc))
            send(SO.at[x], SO.at[x], w_s.at[0, 0], w_r.at[0], dev(x, y, z, 1 - c))

    def project_done():
        @pl.when(unaligned)
        def _():
            arrived(SO.at[x], w_r.at[0])

        for e in (1, 3, 2):
            arrived(SO.at[at(e)], w_r.at[e])

    stage("project_z", project_z)
    stage("imageB", image, B)
    stage("gatheredL", gathered, LAST)

    def target(step):
        h = 1 - zh if step < 2 else zh
        cc = 1 - c if step % 2 == 0 else c
        to_z = h * 2 + c
        dz = wrap(to_z - z)
        return h * 2 + cc, cc, to_z, (dz + 1) // 2, (3 - dz) // 2

    def image_out(step):
        block, cc, to_z, slot, direct = target(step)
        total = acc[:, lanes(block)] + image_tile(LAST, block)
        half = total.astype(jnp.bfloat16).reshape(2, 2, 2, 64, 512)
        SB[step] = half

        @pl.when(unaligned)
        def _():
            acc[:, lanes(block)] = total
            send(SB.at[step, direct], RI.at[slot, direct], i_s.at[step, direct], i_r.at[slot, direct], dev(x, y, to_z, cc))

        @pl.when(aligned)
        def _():
            if step < 2:
                send(SB.at[step, 0], RC.at[0, cc], i_s.at[step, 0], k_r.at[0, cc], dev(x, y, z + 1, c))
                send(SB.at[step, 1], RC.at[1, cc], i_s.at[step, 1], k_r.at[1, cc], dev(x, y, z - 1, c))
            elif step == 2:
                send(SB.at[step], RI.at[0], i_s.at[step, 0], i_r.at[0, 0], partner)
            else:
                RI[0] = half

    def image_join(step):
        block, cc, to_z, slot, direct = target(step)
        joined = 1 - direct
        arrived(RC.at[joined, cc], k_r.at[joined, cc])
        rows = pl.ds(pl.multiple_of(joined * 256, 256), 256)
        total = acc[rows, lanes(block)].reshape(2, 2, 64, 512) + RC[joined, cc].astype(jnp.float32)
        SB[step, joined] = total.astype(jnp.bfloat16)
        send(SB.at[step, joined], RI.at[slot, joined], i_s.at[step, joined], i_r.at[slot, joined], dev(x, y, to_z, cc))

    for step in range(4):
        stage(f"out{step}", image_out, step)
    stage("project_x", project_x)

    @pl.when(unaligned)
    def _():
        for step in (0, 2, 1, 3):
            stage(f"join{step}", image_join, step)

    stage("project", project_done)

    def images_done():
        for slot in (1, 2):
            for q in range(2):
                arrived(RI.at[slot, q], i_r.at[slot, q])

        @pl.when(unaligned)
        def _():
            arrived(RI.at[0], i_r.at[0, 0])

    stage("images", images_done)

    def drain():
        for copy in pending:
            copy.wait_send()

        @pl.when(unaligned)
        def _():
            sent(xin, v_s.at[0, 0])
            for q in range(2):
                for cc in range(2):
                    sent(vector_piece(q, z - 1 - 2 * q, cc), t_s.at[q, cc])
            for step in range(4):
                for q in range(2):
                    sent(SB.at[step, q], i_s.at[step, q])
            for k in range(2):
                sent(SZ.at[z], u_s.at[k])

        @pl.when(aligned)
        def _():
            for step in range(2):
                for q in range(2):
                    sent(SB.at[step, q], i_s.at[step, q])
            sent(SB.at[2], i_s.at[2, 0])
            sent(SZ.at[z], u_s.at[0])
            for e in (1, 3, 2):
                for cc in range(2):
                    sent(SO.at[x], w_s.at[e, cc])
            sent(SO.at[x], w_s.at[0, 0])

    stage("drain", drain)


def finish(parts, so, img, sub, images, matrix, i_sem, m_sem):
    for f in range(4):
        matrix[f, 0] = so[f, :, 0:64]
        matrix[f, 1] = so[f, :, 64:128]
    copies = [pltpu.make_async_copy(matrix, sub, m_sem)]
    copies[0].start()
    for f in range(4):
        total = parts[0, f].astype(jnp.float32) + parts[1, f].astype(jnp.float32)
        images[f] = total + parts[2, f].astype(jnp.float32)
        copies.append(pltpu.make_async_copy(images.at[f], img.at[f], i_sem.at[f]))
        copies[-1].start()
    for copy in copies:
        copy.wait()


def shards(pair_density, trial_vectors, frequency, val_energy, cond_energy, pair_index):
    groups = lax.axis_size("freq")
    members = lax.axis_size("band")
    pair_count = pair_density.shape[0] * groups * members
    grid_count = trial_vectors.shape[3] * members
    prefactor = 1.0 / math.sqrt(2.0 * grid_count * pair_count)
    pieces = jnp.transpose(pair_density, (1, 0, 2))
    bf, f32 = jnp.bfloat16, jnp.float32
    vmem = pl.BlockSpec(memory_space=pltpu.VMEM)
    smem = pl.BlockSpec(memory_space=pltpu.SMEM)
    hbm = pl.BlockSpec(memory_space=pltpu.HBM)
    dma = pltpu.SemaphoreType.DMA
    parts, subspace = pl.pallas_call(
        functools.partial(kernel, (prefactor, grid_count)),
        name="response",
        out_shape=(
            jax.ShapeDtypeStruct((3, 2, 2, 2, 64, 512), bf),
            jax.ShapeDtypeStruct((4, 64, 128), f32),
        ),
        in_specs=[vmem, vmem, smem, smem, smem, smem],
        out_specs=(vmem, vmem),
        scratch_shapes=[
            pltpu.VMEM((2, 4, 2, 4, 2, 16, 2048), bf),
            pltpu.VMEM((4, 2, 64, 2048), bf),
            pltpu.VMEM((512, 2048), f32),
            pltpu.VMEM((2, 4, 4, 2, 64, 128), f32),
            pltpu.VMEM((2, 4, 4, 2, 64, 128), bf),
            pltpu.VMEM((2, 4, 4, 2, 64, 128), bf),
            pltpu.VMEM((2, 4, 4, 2, 64, 128), bf),
            pltpu.VMEM((4, 2, 64, 768), bf),
            pltpu.VMEM((4, 2, 2, 2, 64, 512), bf),
            pltpu.VMEM((2, 2, 2, 2, 64, 512), bf),
            pltpu.VMEM((32, 8, 128), f32),
            pltpu.VMEM((4, 64, 128), f32),
            pltpu.VMEM((256, 128), f32),
            pltpu.VMEM((2, 4, 8, 128), f32),
            dma((2, 4)), dma((2, 4)),
            dma((2, 2, 4)), dma((2, 2, 4)),
            dma((2, 2, 4)), dma((2, 2, 4)),
            dma((2, 4, 4)), dma((2, 4, 4)),
            dma((4, 2)), dma((4, 2, 2)), dma((2, 2)),
            dma((2, 4, 4)), dma((2, 4, 4)),
            dma((2, 4, 4)), dma((2, 4, 4)),
            dma((4, 2)), dma((4, 2)), dma((2, 2)),
            dma((2, 4)), dma((2, 4)),
            dma((2,)), dma((4,)),
            dma((4, 2)), dma((4,)),
            dma, dma,
        ],
        compiler_params=pltpu.CompilerParams(
            collective_id=0, has_side_effects=True, vmem_limit_bytes=36 * 2**20
        ),
    )(pieces, trial_vectors, pair_index, cond_energy, val_energy, frequency)
    return pl.pallas_call(
        finish,
        name="finish",
        out_shape=(
            jax.ShapeDtypeStruct((4, 2, 64, 512), f32),
            jax.ShapeDtypeStruct((4, 2, 64, 64), f32),
        ),
        in_specs=[vmem, vmem],
        out_specs=(hbm, hbm),
        scratch_shapes=[
            pltpu.VMEM((4, 2, 64, 512), f32),
            pltpu.VMEM((4, 2, 64, 64), f32),
            dma((4,)), dma,
        ],
        compiler_params=pltpu.CompilerParams(vmem_limit_bytes=8 * 2**20),
    )(parts.reshape(3, 4, 2, 64, 512), subspace)


def solution(mesh):
    return jax.shard_map(
        shards,
        mesh=mesh,
        in_specs=(
            P(("freq", "band"), None, None),
            P("freq", None, None, "band"),
            P("freq"),
            P(),
            P(),
            P(("freq", "band")),
        ),
        out_specs=(P("freq", None, None, "band"), P("freq", None, None, None)),
        check_vma=False,
    )
```

```python
import functools
import math

import jax
import jax.numpy as jnp
from jax import lax
from jax.experimental import pallas as pl
from jax.experimental.pallas import tpu as pltpu
from jax.sharding import PartitionSpec as P

MESH = pl.DeviceIdType.MESH
ORDER = (0, 1, 3, 2)


def wrap(v, n=4):
    return lax.rem(v + n, n)


def dev(x, y, z, c):
    x, y, z, c = wrap(x), wrap(y), wrap(z), wrap(c, 2)
    return (lax.rem(z, 2) * 4 + y, x * 4 + (z // 2) * 2 + c)


def dot_nt(a, b):
    return lax.dot_general(a, b, (((1,), (1,)), ((), ())), preferred_element_type=jnp.float32)


def kernel(
    consts,
    rho, xin, idx, cond, val, freq,
    RI, SO,
    R, XF, acc, C32, CB, CR, SF, L, SB, RC, D, SZ, SA, FQ,
    x_s, x_r, y_s, y_r, f_s, f_r, p_s, p_r, v_s, v_r, t_s, c_s, c_r, g_s, g_r,
    i_s, i_r, k_r, d_s, d_r, u_s, u_r, w_s, w_r, q_s, q_r,
):
    prefactor, grid_count = consts
    fi, bi = lax.axis_index("freq"), lax.axis_index("band")
    zl, y = fi // 4, lax.rem(fi, 4)
    x, zh, c = bi // 4, lax.rem(bi // 2, 2), lax.rem(bi, 2)
    z = zh * 2 + zl
    me = (fi, bi)
    partner = dev(x, y, z, 1 - c)
    aligned = zl == c
    unaligned = jnp.logical_not(aligned)
    pending = []

    def send(src, dst, ss, rs, to):
        copy = pltpu.make_async_remote_copy(
            src_ref=src, dst_ref=dst, send_sem=ss, recv_sem=rs, device_id=to, device_id_type=MESH
        )
        copy.start()
        return copy

    def keep(copy):
        pending.append(copy)

    def arrived(dst, rs):
        pltpu.make_async_remote_copy(
            src_ref=dst, dst_ref=dst, send_sem=rs, recv_sem=rs, device_id=me, device_id_type=MESH
        ).wait_recv()

    def sent(src, ss):
        pltpu.make_async_remote_copy(
            src_ref=src, dst_ref=src, send_sem=ss, recv_sem=ss, device_id=me, device_id_type=MESH
        ).wait_send()

    lines = [dev(x + e, y, z, cc) for e in (1, 2, 3) for cc in range(2)]
    lines += [dev(x, y + dy, z, c) for dy in (1, 2, 3)]
    lines += [dev(x, y, z + dz, cc) for dz in (1, 2, 3) for cc in range(2)]
    lines.append(partner)
    barrier = pltpu.get_barrier_semaphore()
    for other in lines:
        pl.semaphore_signal(barrier, inc=1, device_id=other, device_id_type=MESH)
    with jax.named_scope("entry"):
        pl.semaphore_wait(barrier, len(lines))

    def lanes(block):
        return pl.ds(pl.multiple_of(block * 512, 512), 512)

    def stage(name, fn, *args):
        with jax.named_scope(name):
            fn(*args)

    def at(e):
        return wrap(x - e)

    def columns(block):
        return pl.ds(pl.multiple_of(block * 2048, 2048), 2048)

    def own_piece(h, block):
        return rho.at[:, pl.ds(16 * h, 16), columns(block)]

    def spread(h, e):
        src = own_piece(h, x) if e == 0 else R.at[h, 0, :, at(e), c]
        keep(send(src, R.at[h, 1, :, at(e), c], y_s.at[h, 0, e], y_r.at[h, 0, e], dev(x, y + 1, z, c)))
        keep(send(src, R.at[h, 2, :, at(e), c], y_s.at[h, 1, e], y_r.at[h, 1, e], dev(x, y - 1, z, c)))
        keep(send(src, R.at[h, 0, :, at(e), c], p_s.at[h, 0, e], p_r.at[h, 0, e], partner))

    def pass_on(h, e):
        for side in range(2):
            to = dev(x, y + 1 - 2 * side, z, c)
            piece = R.at[h, 1 + side, :, at(e), c]
            arrived(piece, y_r.at[h, side, e])
            part = R.at[h, 1 + side, side, at(e), c]
            keep(send(part, R.at[h, 3, side, at(e), c], f_s.at[h, side, e], f_r.at[h, side, e], to))
            keep(send(piece, piece, p_s.at[h, 1 + side, e], p_r.at[h, 1 + side, e], partner))

    def pass_far(h, e):
        for side in range(2):
            arrived(R.at[h, 3, side, at(e), c], f_r.at[h, side, e])
        piece = R.at[h, 3, :, at(e), c]
        keep(send(piece, piece, p_s.at[h, 3, e], p_r.at[h, 3, e], partner))

    def partner_done(h, pos):
        for e in ORDER:
            arrived(R.at[h, pos, :, at(e), 1 - c], p_r.at[h, pos, e])

    def from_x(h, e):
        arrived(R.at[h, 0, :, at(e), c], x_r.at[h, e])
        spread(h, e)

    my_lanes = lanes(zh * 2 + c)

    def vector_piece(q, zz, cc):
        return XF.at[pl.ds(2 * q, 2), :, :, lanes((wrap(zz) // 2) * 2 + cc)]

    def begin():
        spread(0, 0)
        def to_x(h):
            for e in (1, 3, 2):
                keep(send(own_piece(h, wrap(x + e)), R.at[h, 0, :, x, c], x_s.at[h, e], x_r.at[h, e], dev(x + e, y, z, c)))

        to_x(0)
        for k in range(2):
            for side in range(2):
                q = (k + side) % 2
                dz = 1 + 2 * side
                keep(send(xin.at[pl.ds(2 * q, 2)], vector_piece(q, z, c), v_s.at[dz, q], v_r.at[dz, c, q], dev(x, y, z + dz, zl)))
        spread(1, 0)

        @pl.when(unaligned)
        def _():
            send(xin, XF.at[:, :, :, my_lanes], v_s.at[0, 0], v_r.at[0, c, 0], partner)

        for f in range(4):
            FQ[0, f] = jnp.full((8, 128), freq[f], jnp.float32)

        lane = lax.broadcasted_iota(jnp.int32, (8, 128), 1)
        row = lax.broadcasted_iota(jnp.int32, (8, 128), 0)
        place = jnp.bitwise_and(row, 1) * 16 + jnp.bitwise_and(lane, 15)
        number = jnp.zeros((8, 128), jnp.int32)
        for i in range(32):
            number = jnp.where(place == i, idx[i], number)
        cond_no = jnp.bitwise_and(number, 127)
        val_no = jnp.right_shift(number, 7)
        zero = jnp.zeros((8, 128), jnp.float32)
        cond_pick = lax.fori_loop(0, 128, lambda j, a: jnp.where(cond_no == j, cond[j], a), zero)
        val_pick = lax.fori_loop(0, 32, lambda j, a: jnp.where(val_no == j, val[j], a), zero)
        D[c * 16 + x] = jnp.where(jnp.right_shift(lane, 4) == x * 2 + c, cond_pick - val_pick, 0.0)
        for h in range(2):
            R[h, 0, :, x, c] = rho[:, 16 * h : 16 * h + 16, columns(x)]

        @pl.when(aligned)
        def _():
            XF[:, :, :, my_lanes] = xin[...]
            FQ[1] = FQ[0]

        @pl.when(aligned)
        def _():
            send(FQ.at[0], FQ.at[1], q_s, q_r, dev(x, y, z - 1, c))

        for e in (1, 3, 2):
            keep(send(D.at[c * 16 + x], D.at[c * 16 + x], d_s.at[0, e], d_r.at[0, e], dev(x + e, y, z, c)))
        to_x(1)

    def energies_y():
        for e in (1, 3, 2):
            arrived(D.at[c * 16 + at(e)], d_r.at[0, e])
        row = D.at[pl.ds(c * 16, 4)]
        for dy, pos in ((1, 1), (3, 2), (2, 3)):
            keep(send(row, D.at[pl.ds(c * 16 + pos * 4, 4)], d_s.at[1, dy], d_r.at[1, dy], dev(x, y + dy, z, c)))

    def energies_core():
        for dy, pos in ((1, 1), (3, 2), (2, 3)):
            arrived(D.at[pl.ds(c * 16 + pos * 4, 4)], d_r.at[1, dy])
        keep(send(D.at[pl.ds(c * 16, 16)], D.at[pl.ds(c * 16, 16)], d_s.at[0, 0], d_r.at[0, 0], partner))

    def vectors_pass():
        @pl.when(unaligned)
        def _():
            for q in range(2):
                dz = 1 + 2 * q
                for cc in range(2):
                    piece = vector_piece(q, z - dz, cc)
                    arrived(piece, v_r.at[dz, cc, q])
                    send(piece, piece, t_s.at[q, cc], v_r.at[2, cc, q], dev(x, y, z + dz, c))

    def vectors_done():
        @pl.when(aligned)
        def _():
            arrived(XF.at[:, :, :, lanes(zh * 2 + 1 - c)], v_r.at[0, 1 - c, 0])
            for q in range(2):
                for cc in range(2):
                    arrived(vector_piece(q, z + 2, cc), v_r.at[2, cc, q])

        @pl.when(unaligned)
        def _():
            for q in range(2):
                dz = 3 - 2 * q
                for cc in range(2):
                    arrived(vector_piece(q, z - dz, cc), v_r.at[dz, cc, q])

    A, FAR, B, LAST = (0, 0, 3), (0, 3, 4), (1, 0, 2), (1, 2, 4)

    def cross(h, pos):
        t = dot_nt(XF[...].reshape(512, 2048), R[h, pos].reshape(256, 2048)).reshape(4, 2, 64, 256)
        re = t[:, 0, :, 0:128] + t[:, 1, :, 128:256]
        im = t[:, 1, :, 0:128] - t[:, 0, :, 128:256]
        C32[h, :, pos, 0] = re
        C32[h, :, pos, 1] = im
        CB[h, :, pos, 0] = re.astype(jnp.bfloat16)
        CB[h, :, pos, 1] = im.astype(jnp.bfloat16)

    def cross_out(h, pos):
        for e in (2, 1, 3):
            keep(send(CB.at[h, wrap(x + e), pos], CR.at[h, e, pos], c_s.at[h, pos, e], c_r.at[h, pos, e], dev(x + e, y, z, c)))

    def scale(h, pos):
        for e in (1, 3, 2):
            arrived(CR.at[h, e, pos], c_r.at[h, pos, e])
        own = FQ[1, x][0:1, 0:1]
        total = C32[h, x, pos]
        for e in (1, 2, 3):
            total = total + CR[h, e, pos].astype(jnp.float32)
        delta = D[pos * 4]
        for k in range(1, 8):
            delta = delta + D[(k // 4) * 16 + pos * 4 + k % 4]
        delta = delta[h : h + 1]
        ratio = delta / (delta * delta + own * own)
        weight = (-4.0 * prefactor * ratio).astype(jnp.bfloat16).astype(jnp.float32)
        SF[h, x, pos] = (weight[None] * total).astype(jnp.bfloat16)
        C32[h, x, pos] = total
        for e in (2, 1, 3):
            keep(send(SF.at[h, x, pos], SF.at[h, x, pos], g_s.at[h, pos, e], g_r.at[h, pos, e], dev(x + e, y, z, c)))

    def project_add(group):
        h = group[0]
        for pos in range(group[1], group[2]):
            flat = C32[h, x, pos].reshape(128, 128)
            high = flat.astype(jnp.bfloat16)
            low = (flat - high.astype(jnp.float32)).astype(jnp.bfloat16)
            part = dot_nt(jnp.concatenate([high, low], axis=0), SF[h, x, pos].reshape(128, 128))
            if h == 0 and pos == 0:
                SA[...] = part
            else:
                SA[...] += part

    def gathered(group):
        h = group[0]
        for pos in range(group[1], group[2]):
            for e in (1, 3, 2):
                arrived(SF.at[h, at(e), pos], g_r.at[h, pos, e])
        for pos in range(group[1], group[2]):
            base = (pos - group[1]) * 256
            re, im = SF[h, :, pos, 0], SF[h, :, pos, 1]
            L[:, 0, :, base : base + 128] = re
            L[:, 0, :, base + 128 : base + 256] = -im
            L[:, 1, :, base : base + 128] = im
            L[:, 1, :, base + 128 : base + 256] = re

    def image_tile(group, block):
        h, some = group[0], pl.ds(group[1], group[2] - group[1])
        depth = (group[2] - group[1]) * 256
        return jnp.dot(
            L[:, :, :, 0:depth].reshape(512, depth),
            R[h, some, :, :, :, :, lanes(block)].reshape(depth, 512),
            preferred_element_type=jnp.float32,
        )

    def image(group):
        gathered(group)
        for block in range(4):
            part = image_tile(group, block)
            if group == A:
                acc[:, block * 512 : block * 512 + 512] = part
            else:
                acc[:, block * 512 : block * 512 + 512] += part

    def energies_done():
        arrived(D.at[pl.ds((1 - c) * 16, 16)], d_r.at[0, 0])

        @pl.when(aligned)
        def _():
            sent(FQ.at[0], q_s)

        @pl.when(unaligned)
        def _():
            arrived(FQ.at[1], q_r)

    stage("begin", begin)
    stage("xA1", from_x, 0, 1)
    stage("xA3", from_x, 0, 3)
    stage("passA0", pass_on, 0, 0)
    stage("xA2", from_x, 0, 2)
    stage("relay", vectors_pass)
    stage("energies_y", energies_y)
    stage("passA1", pass_on, 0, 1)
    stage("passA3", pass_on, 0, 3)
    stage("xB1", from_x, 1, 1)
    stage("xB3", from_x, 1, 3)
    stage("farA0", pass_far, 0, 0)
    stage("passA2", pass_on, 0, 2)
    stage("passB0", pass_on, 1, 0)
    stage("xB2", from_x, 1, 2)
    stage("energies_core", energies_core)
    stage("vectors", vectors_done)
    stage("partA0", partner_done, 0, 0)
    stage("crossA0", cross, 0, 0)
    stage("outA0", cross_out, 0, 0)
    stage("farA1", pass_far, 0, 1)
    stage("partA1", partner_done, 0, 1)
    stage("crossA1", cross, 0, 1)
    stage("outA1", cross_out, 0, 1)
    stage("farA3", pass_far, 0, 3)
    stage("partA2", partner_done, 0, 2)
    stage("crossA2", cross, 0, 2)
    stage("outA2", cross_out, 0, 2)
    stage("partB0", partner_done, 1, 0)
    stage("crossB0", cross, 1, 0)
    stage("outB0", cross_out, 1, 0)
    stage("passB1", pass_on, 1, 1)
    stage("energies", energies_done)
    stage("scaleA0", scale, 0, 0)
    stage("scaleA1", scale, 0, 1)
    stage("passB3", pass_on, 1, 3)
    stage("farA2", pass_far, 0, 2)
    stage("partA3", partner_done, 0, 3)
    stage("crossA3", cross, 0, 3)
    stage("outA3", cross_out, 0, 3)
    stage("scaleA2", scale, 0, 2)
    stage("scaleB0", scale, 1, 0)
    stage("passB2", pass_on, 1, 2)
    stage("farB0", pass_far, 1, 0)
    stage("partB1", partner_done, 1, 1)
    stage("crossB1", cross, 1, 1)
    stage("outB1", cross_out, 1, 1)
    stage("farB1", pass_far, 1, 1)
    stage("partB2", partner_done, 1, 2)
    stage("crossB2", cross, 1, 2)
    stage("outB2", cross_out, 1, 2)
    stage("farB3", pass_far, 1, 3)
    stage("farB2", pass_far, 1, 2)
    stage("scaleA3", scale, 0, 3)
    stage("partB3", partner_done, 1, 3)
    stage("crossB3", cross, 1, 3)
    stage("outB3", cross_out, 1, 3)
    stage("scaleB1", scale, 1, 1)
    stage("imageA", image, A)
    stage("scaleB2", scale, 1, 2)
    stage("scaleB3", scale, 1, 3)
    stage("imageF", image, FAR)
    stage("addA", project_add, A)
    stage("addF", project_add, FAR)
    stage("addB", project_add, B)
    stage("addL", project_add, LAST)

    def project_z():
        both = SA[0:128] + SA[128:256]
        re = both[0:64, 0:64] + both[64:128, 64:128]
        im = both[0:64, 64:128] - both[64:128, 0:64]
        SZ[z] = jnp.concatenate([re, im], axis=1) / grid_count

        @pl.when(aligned)
        def _():
            send(SZ.at[z], SZ.at[z], u_s.at[0], u_r.at[2], dev(x, y, z + 2, c))

        @pl.when(unaligned)
        def _():
            for k, dz in enumerate((1, 3)):
                send(SZ.at[z], SZ.at[z], u_s.at[k], u_r.at[dz], dev(x, y, z + dz, c))

    def project_x():
        @pl.when(aligned)
        def _():
            for dz in (1, 3, 2):
                arrived(SZ.at[wrap(z - dz)], u_r.at[dz])
            SO[x] = SZ[0] + SZ[1] + SZ[2] + SZ[3]
            for e in (1, 3, 2):
                for cc in range(2):
                    send(SO.at[x], SO.at[x], w_s.at[e, cc], w_r.at[e], dev(x + e, y, z, cc))
            send(SO.at[x], SO.at[x], w_s.at[0, 0], w_r.at[0], dev(x, y, z, 1 - c))

    def project_done():
        @pl.when(unaligned)
        def _():
            arrived(SO.at[x], w_r.at[0])

        for e in (1, 3, 2):
            arrived(SO.at[at(e)], w_r.at[e])

    stage("project_z", project_z)
    stage("imageB", image, B)
    stage("gatheredL", gathered, LAST)

    def target(step):
        h = 1 - zh if step < 2 else zh
        cc = 1 - c if step % 2 == 0 else c
        to_z = h * 2 + c
        dz = wrap(to_z - z)
        return h * 2 + cc, cc, to_z, (dz + 1) // 2, (3 - dz) // 2

    def image_out(step):
        block, cc, to_z, slot, direct = target(step)
        total = acc[:, lanes(block)] + image_tile(LAST, block)
        half = total.astype(jnp.bfloat16).reshape(2, 2, 2, 64, 512)
        SB[step] = half

        @pl.when(unaligned)
        def _():
            acc[:, lanes(block)] = total
            send(SB.at[step, direct], RI.at[slot, direct], i_s.at[step, direct], i_r.at[slot, direct], dev(x, y, to_z, cc))

        @pl.when(aligned)
        def _():
            if step < 2:
                send(SB.at[step, 0], RC.at[0, cc], i_s.at[step, 0], k_r.at[0, cc], dev(x, y, z + 1, c))
                send(SB.at[step, 1], RC.at[1, cc], i_s.at[step, 1], k_r.at[1, cc], dev(x, y, z - 1, c))
            elif step == 2:
                send(SB.at[step], RI.at[0], i_s.at[step, 0], i_r.at[0, 0], partner)
            else:
                RI[0] = half

    def image_join(step):
        block, cc, to_z, slot, direct = target(step)
        joined = 1 - direct
        arrived(RC.at[joined, cc], k_r.at[joined, cc])
        rows = pl.ds(pl.multiple_of(joined * 256, 256), 256)
        total = acc[rows, lanes(block)].reshape(2, 2, 64, 512) + RC[joined, cc].astype(jnp.float32)
        SB[step, joined] = total.astype(jnp.bfloat16)
        send(SB.at[step, joined], RI.at[slot, joined], i_s.at[step, joined], i_r.at[slot, joined], dev(x, y, to_z, cc))

    for step in range(4):
        stage(f"out{step}", image_out, step)
    stage("project_x", project_x)

    @pl.when(unaligned)
    def _():
        for step in (0, 2, 1, 3):
            stage(f"join{step}", image_join, step)

    stage("project", project_done)

    def images_done():
        for slot in (1, 2):
            for q in range(2):
                arrived(RI.at[slot, q], i_r.at[slot, q])

        @pl.when(unaligned)
        def _():
            arrived(RI.at[0], i_r.at[0, 0])

    stage("images", images_done)

    def drain():
        for copy in pending:
            copy.wait_send()

        @pl.when(unaligned)
        def _():
            sent(xin, v_s.at[0, 0])
            for q in range(2):
                for cc in range(2):
                    sent(vector_piece(q, z - 1 - 2 * q, cc), t_s.at[q, cc])
            for step in range(4):
                for q in range(2):
                    sent(SB.at[step, q], i_s.at[step, q])
            for k in range(2):
                sent(SZ.at[z], u_s.at[k])

        @pl.when(aligned)
        def _():
            for step in range(2):
                for q in range(2):
                    sent(SB.at[step, q], i_s.at[step, q])
            sent(SB.at[2], i_s.at[2, 0])
            sent(SZ.at[z], u_s.at[0])
            for e in (1, 3, 2):
                for cc in range(2):
                    sent(SO.at[x], w_s.at[e, cc])
            sent(SO.at[x], w_s.at[0, 0])

    stage("drain", drain)


def finish(parts, so, img, sub, images, matrix, i_sem, m_sem):
    for f in range(4):
        matrix[f, 0] = so[f, :, 0:64]
        matrix[f, 1] = so[f, :, 64:128]
    copies = [pltpu.make_async_copy(matrix, sub, m_sem)]
    copies[0].start()
    for f in range(4):
        total = parts[0, f].astype(jnp.float32) + parts[1, f].astype(jnp.float32)
        images[f] = total + parts[2, f].astype(jnp.float32)
        copies.append(pltpu.make_async_copy(images.at[f], img.at[f], i_sem.at[f]))
        copies[-1].start()
    for copy in copies:
        copy.wait()


def shards(pair_density, trial_vectors, frequency, val_energy, cond_energy, pair_index):
    groups = lax.axis_size("freq")
    members = lax.axis_size("band")
    pair_count = pair_density.shape[0] * groups * members
    grid_count = trial_vectors.shape[3] * members
    prefactor = 1.0 / math.sqrt(2.0 * grid_count * pair_count)
    pieces = jnp.transpose(pair_density, (1, 0, 2))
    bf, f32 = jnp.bfloat16, jnp.float32
    vmem = pl.BlockSpec(memory_space=pltpu.VMEM)
    smem = pl.BlockSpec(memory_space=pltpu.SMEM)
    hbm = pl.BlockSpec(memory_space=pltpu.HBM)
    dma = pltpu.SemaphoreType.DMA
    parts, subspace = pl.pallas_call(
        functools.partial(kernel, (prefactor, grid_count)),
        name="response",
        out_shape=(
            jax.ShapeDtypeStruct((3, 2, 2, 2, 64, 512), bf),
            jax.ShapeDtypeStruct((4, 64, 128), f32),
        ),
        in_specs=[vmem, vmem, smem, smem, smem, smem],
        out_specs=(vmem, vmem),
        scratch_shapes=[
            pltpu.VMEM((2, 4, 2, 4, 2, 16, 2048), bf),
            pltpu.VMEM((4, 2, 64, 2048), bf),
            pltpu.VMEM((512, 2048), f32),
            pltpu.VMEM((2, 4, 4, 2, 64, 128), f32),
            pltpu.VMEM((2, 4, 4, 2, 64, 128), bf),
            pltpu.VMEM((2, 4, 4, 2, 64, 128), bf),
            pltpu.VMEM((2, 4, 4, 2, 64, 128), bf),
            pltpu.VMEM((4, 2, 64, 768), bf),
            pltpu.VMEM((4, 2, 2, 2, 64, 512), bf),
            pltpu.VMEM((2, 2, 2, 2, 64, 512), bf),
            pltpu.VMEM((32, 8, 128), f32),
            pltpu.VMEM((4, 64, 128), f32),
            pltpu.VMEM((256, 128), f32),
            pltpu.VMEM((2, 4, 8, 128), f32),
            dma((2, 4)), dma((2, 4)),
            dma((2, 2, 4)), dma((2, 2, 4)),
            dma((2, 2, 4)), dma((2, 2, 4)),
            dma((2, 4, 4)), dma((2, 4, 4)),
            dma((4, 2)), dma((4, 2, 2)), dma((2, 2)),
            dma((2, 4, 4)), dma((2, 4, 4)),
            dma((2, 4, 4)), dma((2, 4, 4)),
            dma((4, 2)), dma((4, 2)), dma((2, 2)),
            dma((2, 4)), dma((2, 4)),
            dma((2,)), dma((4,)),
            dma((4, 2)), dma((4,)),
            dma, dma,
        ],
        compiler_params=pltpu.CompilerParams(
            collective_id=0, has_side_effects=True, vmem_limit_bytes=36 * 2**20
        ),
    )(pieces, trial_vectors, pair_index, cond_energy, val_energy, frequency)
    return pl.pallas_call(
        finish,
        name="finish",
        out_shape=(
            jax.ShapeDtypeStruct((4, 2, 64, 512), f32),
            jax.ShapeDtypeStruct((4, 2, 64, 64), f32),
        ),
        in_specs=[vmem, vmem],
        out_specs=(hbm, hbm),
        scratch_shapes=[
            pltpu.VMEM((4, 2, 64, 512), f32),
            pltpu.VMEM((4, 2, 64, 64), f32),
            dma((4,)), dma,
        ],
        compiler_params=pltpu.CompilerParams(vmem_limit_bytes=8 * 2**20),
    )(parts.reshape(3, 4, 2, 64, 512), subspace)


def solution(mesh):
    return jax.shard_map(
        shards,
        mesh=mesh,
        in_specs=(
            P(("freq", "band"), None, None),
            P("freq", None, None, "band"),
            P("freq"),
            P(),
            P(),
            P(("freq", "band")),
        ),
        out_specs=(P("freq", None, None, "band"), P("freq", None, None, None)),
        check_vma=False,
    )
```
